32 devices in a mesh: part: 1 (over z), row: 4 (over y), col: 4 (over x), dep: 2 (over core).
Axes of the slice: x: 4, y: 4, z: 1, core: 2. Of those that a mesh axis runs over, the one named last changes fastest.
The devices are a block of a 4x4x8 slice.
Arguments:
- x_in: bfloat16 [8192, 4096], P(('part', 'row', 'col'), 'dep')
- ln_scale: float32 [4096], P('dep')
- ln_shift: float32 [4096], P('dep')
- w_up: bfloat16 [4096, 16384], P(('dep', 'row'), 'col')
- b_up: bfloat16 [16384], P('col')
- w_down: bfloat16 [16384, 4096], P(('col', 'row'), 'dep')
- b_down: bfloat16 [4096], P('dep')
- y_grad: bfloat16 [8192, 4096], P(('part', 'row', 'col'), 'dep')
Outputs:
- output 1: bfloat16 [8192, 4096], P(('part', 'row', 'col'), 'dep')
- output 2: bfloat16 [8192, 4096], P(('part', 'row', 'col'), 'dep')
- output 3: bfloat16 [4096, 16384], P(('part', 'dep', 'row'), 'col')
- output 4: float32 [16384], P(('part', 'col'))
- output 5: bfloat16 [16384, 4096], P(('part', 'col', 'row'), 'dep')
- output 6: float32 [4096], P(('part', 'dep'))
- output 7: float32 [4096], P(('part', 'dep'))
- output 8: float32 [4096], P(('part', 'dep'))
All inputs are finite; a program needn't handle non-finite values.
Results may differ from the reference program's by a relative error of at most 0.00166166.
Values are sent between devices in bfloat16 or wider.
A program may use at most 768 MiB of HBM per device.

```python
import jax
import jax.numpy as jnp
from jax import lax

TOKENS = 8192
D_MODEL = 4096
D_FF = 16384

BLOCK_ROWS = min(TOKENS, 512)
N_BLOCKS = TOKENS // BLOCK_ROWS
LN_EPS = 1e-5
GELU_K = 0.7978845608028654
GELU_C = 0.044715
TWO_PI = 6.283185307179586


def setup_inputs(seed: int = 0, part: int = 0) -> dict:
    shared_root, part_root = jax.random.split(jax.random.key(seed))
    part_keys = jax.random.split(jax.random.fold_in(part_root, part), 4)
    shared_keys = jax.random.split(shared_root, 6)
    col_pos = jnp.arange(D_MODEL, dtype=jnp.float32) / D_MODEL
    col_phase = jax.random.uniform(part_keys[0], (), jnp.float32, 0.0, TWO_PI)
    col_mean = 1.5 * jnp.sin(TWO_PI * col_pos + col_phase) + 0.5 * jax.random.normal(part_keys[1], (D_MODEL,), jnp.float32)
    x_vals = jax.random.normal(part_keys[2], (TOKENS, D_MODEL), jnp.float32) + col_mean
    g_vals = jax.random.normal(part_keys[3], (TOKENS, D_MODEL), jnp.float32)
    return {
        "x_in": x_vals.astype(jnp.bfloat16),
        "ln_scale": 1.0 + 0.3 * jax.random.normal(shared_keys[0], (D_MODEL,), jnp.float32),
        "ln_shift": 0.5 * jax.random.normal(shared_keys[1], (D_MODEL,), jnp.float32),
        "w_up": (jax.random.normal(shared_keys[2], (D_MODEL, D_FF), jnp.float32) * D_MODEL ** -0.5).astype(jnp.bfloat16),
        "b_up": (0.5 * jax.random.normal(shared_keys[3], (D_FF,), jnp.float32)).astype(jnp.bfloat16),
        "w_down": (jax.random.normal(shared_keys[4], (D_FF, D_MODEL), jnp.float32) * D_FF ** -0.5).astype(jnp.bfloat16),
        "b_down": (0.5 * jax.random.normal(shared_keys[5], (D_MODEL,), jnp.float32)).astype(jnp.bfloat16),
        "y_grad": g_vals.astype(jnp.bfloat16),
    }


def gelu_tanh(pre_act):
    inner_arg = GELU_K * (pre_act + GELU_C * pre_act * (pre_act * pre_act))
    return 0.5 * pre_act * (1.0 + jnp.tanh(inner_arg))


def gelu_slope(pre_act):
    squared = pre_act * pre_act
    tanh_val = jnp.tanh(GELU_K * (pre_act + GELU_C * pre_act * squared))
    return 0.5 * (1.0 + tanh_val) + 0.5 * pre_act * (1.0 - tanh_val * tanh_val) * GELU_K * (1.0 + 3.0 * GELU_C * squared)


def block_pass(x_blk, g_blk, ln_scale, ln_shift, w_up, b_up, w_down, b_down):
    x_float = x_blk.astype(jnp.float32)
    mean_row = jnp.sum(x_float, axis=1, keepdims=True) / D_MODEL
    var_row = jnp.sum(x_float * x_float, axis=1, keepdims=True) / D_MODEL - mean_row * mean_row
    inv_std = lax.rsqrt(var_row + LN_EPS)
    x_hat = (x_float - mean_row) * inv_std
    normed = (x_hat * ln_scale + ln_shift).astype(jnp.bfloat16)
    pre_act = jnp.dot(normed, w_up, preferred_element_type=jnp.float32) + b_up.astype(jnp.float32)
    hidden = gelu_tanh(pre_act).astype(jnp.bfloat16)
    out_sum = jnp.dot(hidden, w_down, preferred_element_type=jnp.float32)
    y_blk = (x_float + out_sum + b_down.astype(jnp.float32)).astype(jnp.bfloat16)
    g_float = g_blk.astype(jnp.float32)
    w_down_part = jnp.dot(hidden.T, g_blk, preferred_element_type=jnp.float32)
    hid_grad = jnp.dot(g_blk, w_down.T, preferred_element_type=jnp.float32)
    pre_grad = hid_grad * gelu_slope(pre_act)
    pre_lowp = pre_grad.astype(jnp.bfloat16)
    w_up_part = jnp.dot(normed.T, pre_lowp, preferred_element_type=jnp.float32)
    norm_grad = jnp.dot(pre_lowp, w_up.T, preferred_element_type=jnp.float32)
    xhat_grad = norm_grad * ln_scale
    mean_one = jnp.sum(xhat_grad, axis=1, keepdims=True) / D_MODEL
    mean_two = jnp.sum(xhat_grad * x_hat, axis=1, keepdims=True) / D_MODEL
    dx_blk = (g_float + inv_std * (xhat_grad - mean_one - x_hat * mean_two)).astype(jnp.bfloat16)
    part_sums = (w_up_part, jnp.sum(pre_grad, axis=0), w_down_part, jnp.sum(g_float, axis=0), jnp.sum(norm_grad * x_hat, axis=0), jnp.sum(norm_grad, axis=0))
    return y_blk, dx_blk, part_sums


def reference(x_in, ln_scale, ln_shift, w_up, b_up, w_down, b_down, y_grad):
    x_blocks = x_in.reshape(N_BLOCKS, BLOCK_ROWS, D_MODEL)
    g_blocks = y_grad.reshape(N_BLOCKS, BLOCK_ROWS, D_MODEL)

    def scan_step(acc_sums, blk_pair):
        y_blk, dx_blk, part_sums = block_pass(blk_pair[0], blk_pair[1], ln_scale, ln_shift, w_up, b_up, w_down, b_down)
        new_sums = tuple(acc_val + add_val for acc_val, add_val in zip(acc_sums, part_sums))
        return new_sums, (y_blk, dx_blk)

    zero_sums = (jnp.zeros((D_MODEL, D_FF), jnp.float32), jnp.zeros((D_FF,), jnp.float32), jnp.zeros((D_FF, D_MODEL), jnp.float32), jnp.zeros((D_MODEL,), jnp.float32), jnp.zeros((D_MODEL,), jnp.float32), jnp.zeros((D_MODEL,), jnp.float32))
    total_sums, out_blocks = lax.scan(scan_step, zero_sums, (x_blocks, g_blocks))
    return (out_blocks[0].reshape(TOKENS, D_MODEL), out_blocks[1].reshape(TOKENS, D_MODEL), total_sums[0].astype(jnp.bfloat16), total_sums[1], total_sums[2].astype(jnp.bfloat16), total_sums[3], total_sums[4], total_sums[5])
```

```python
import functools

import jax
import jax.numpy as jnp
from jax import lax
from jax.experimental import pallas as pl
from jax.experimental.pallas import tpu as pltpu
from jax.sharding import PartitionSpec as P

LN_EPS = 1e-5
GELU_K = 0.7978845608028654
GELU_C = 0.044715
F32 = jnp.float32
BF16 = jnp.bfloat16
MESH = pl.DeviceIdType.MESH

NAMES = ("A", "G", "W1", "W2", "HP", "HQ", "CP", "CQ", "DB",
         "PY", "RY", "YQ1", "YQ2", "YRF", "YRX", "PD", "RD", "DQ1", "DQ2", "DRF", "DRX",
         "S1", "R1", "S2", "R2", "K1", "K2", "OUT1", "OUT2")


def buffers(TH, DM, DS, FB):
    F2, FC = 2 * FB, 4 * FB
    shapes = {
        "A": ((2, 4, 2 * TH, DM), BF16), "G": ((2, 4, 2 * TH, DM), BF16),
        "W1": ((DM, FC), BF16), "W2": ((FC, DM), BF16),
        "HP": ((2, 2, 2, 2 * TH, F2), BF16), "CP": ((2, 2, 2, 2 * TH, F2), BF16),
        "HQ": ((2, 2, 2 * TH, F2), BF16), "CQ": ((2, 2, 2 * TH, F2), BF16),
        "DB": ((8, FC), F32),
        "S1": ((4, DS, F2), F32), "R1": ((4, DS, F2), F32), "S2": ((FB, DM), F32), "R2": ((FB, DM), F32),
        "K1": ((4, DS, F2), BF16), "K2": ((4, FB, DM // 4), BF16),
        "OUT1": ((DS, 8 * FB), BF16), "OUT2": ((2 * FB, DM // 2), BF16),
    }
    for p, rr, s in (("PY", "RY", "Y"), ("PD", "RD", "D")):
        shapes[p] = shapes[rr] = ((2, 2, TH, DM), F32)
        shapes[s + "Q1"] = shapes[s + "Q2"] = shapes[s + "RX"] = ((2, TH, DM), F32)
        shapes[s + "RF"] = ((2, TH // 2, DM), F32)
    return [jax.ShapeDtypeStruct(*shapes[n]) for n in NAMES]


def mul(x, n):
    return x * n if isinstance(x, int) else pl.multiple_of(x * n, n)


def cp(src, dst, sem):
    return pltpu.make_async_copy(src, dst, sem)


def start(*copies):
    for t in copies:
        t.start()


def wait(*copies):
    for t in copies:
        t.wait()


def kernel(cfg, a_own, g_own, w1, w2, bup, *refs):
    TH, DM, DS, FB = cfg
    o = dict(zip(NAMES, refs[:len(NAMES)]))
    ssem, rsem = refs[len(NAMES):]
    DH, F2, FC, BN, HT, T2 = DM // 2, 2 * FB, 4 * FB, DM // 4, TH // 2, 2 * TH
    A, G, W1, W2 = o["A"], o["G"], o["W1"], o["W2"]
    r, c, d = lax.axis_index("row"), lax.axis_index("col"), lax.axis_index("dep")
    hp, hi = r % 2, r // 2
    g = (r + hi) % 2
    u, v, q = r + 1 - 2 * hp, 3 - r, (r + 2) % 4
    R, L, far = (c + 1) % 4, (c + 3) % 4, (c + 2) % 4
    e = 1 - d
    pos_r, pos_v = 2 * g + hi, 2 * g + 1 - hi
    pos_u, pos_q = 2 * (1 - g) + hi, 2 * (1 - g) + 1 - hi
    half_g, half_n = pl.ds(mul(g, F2), F2), pl.ds(mul(1 - g, F2), F2)
    c_lo, c_hi = c % 2, c // 2

    ids, counts = {}, [0, 0]

    def rid(name, n=1):
        if name not in ids:
            ids[name] = counts[0]
            counts[0] += n
        return ids[name]

    for nm in ("A", "G"):
        for w in ("xr0", "xl0", "u", "xr1", "xl1", "fr0", "fl0", "fr1", "fl1"):
            rid(nm + w)
        for t in ("0", "1"):
            for w in ("c", "L", "R", "x", "y"):
                rid(nm + "d" + t + w)
    rid("w1d", 4)
    for s in ("u", "v"):
        rid("w1" + s, 8)
        rid("w2" + s, 2)
        rid("f1" + s, 2)
        rid("f2" + s)
    rid("w2d")
    for s in ("s1", "s2", "k1u"):
        rid(s, 4)
    rid("k1d", 2)
    rid("k2", 2)
    for s in ("Y", "D"):
        for w in ("p", "r", "l", "pr", "pl"):
            rid(s + w, 4)

    pending = []
    dev_e, dev_R, dev_L = {"dep": e}, {"col": R}, {"col": L}

    def dev(row, core):
        return {"row": row, "dep": core}

    class Send:
        def __init__(self, fn, n=1):
            self.fn, self.sid = fn, counts[1]
            counts[1] += n
            for j in range(n):
                pending.append((self, j))

        def desc(self, j=0):
            src, dst, rsid, device = self.fn(j)
            return pltpu.make_async_remote_copy(src_ref=src, dst_ref=dst, send_sem=ssem.at[self.sid + j], recv_sem=rsem.at[rsid],
                                                device_id=device, device_id_type=MESH)

        def start(self, j=0):
            self.desc(j).start()

    def same(ref, rsid, device):
        return Send(lambda j: (ref, ref, rsid, device))

    def arrived(dst, rsid):
        pltpu.make_async_remote_copy(src_ref=dst, dst_ref=dst, send_sem=ssem.at[0], recv_sem=rsem.at[rsid],
                                     device_id=dev_e, device_id_type=MESH).wait_recv()

    barrier = pltpu.get_barrier_semaphore()
    peers = [dev_e, dev_R, dev_L] + [dev(t, k) for t in (u, v) for k in (0, 1)]
    for p in peers:
        pl.semaphore_signal(barrier, inc=1, device_id=p, device_id_type=MESH)
    pl.semaphore_wait(barrier, len(peers))

    ARR = (("A", A, a_own), ("G", G, g_own))
    ROW = (hp, 1 - hp)

    def ch(X, t, col, core, part=None):
        if part is None:
            return X.at[ROW[t], col, pl.ds(mul(core, TH), TH)]
        return X.at[ROW[t], col, pl.ds(pl.multiple_of(core * TH + part * HT, HT), HT)]

    def w1_src(pos, core):
        gg, ii = pos // 2, pos % 2
        return w1.at[:, pl.ds(mul(((1 - gg) * 3 * ii + gg * (1 + ii)) * 2 + core, FB), FB)]

    def w1_rows(dd, row):
        return pl.ds(mul(dd * 4 + row, DS), DS)

    def w1_dst(dd, row, pos):
        return W1.at[w1_rows(dd, row), pl.ds(mul(pos, FB), FB)]

    def send_w1(tag, row, half):
        for core in (0, 1):
            for ii in (0, 1):
                pos = 2 * half + ii
                Send(lambda j, pos=pos, core=core: (w1_src(pos, core), w1_dst(d, r, pos), rid("w1" + tag) + d * 4 + pos, dev(row, core))).start()

    def wait_w1(tag, row, half):
        for dd in (0, 1):
            for ii in (0, 1):
                pos = 2 * half + ii
                arrived(w1_dst(dd, row, pos), rid("w1" + tag) + dd * 4 + pos)

    def w2_part(pos, half):
        return W2.at[pl.ds(mul(pos, FB), FB), pl.ds(mul(half, DH), DH)]

    def send_w2(tag, row):
        for core in (0, 1):
            Send(lambda j, core=core: (w2.at[pl.ds(core * FB, FB), :], w2_part(pos_r, d), rid("w2" + tag) + d, dev(row, core))).start()

    def wait_w2(tag, pos):
        for dd in (0, 1):
            arrived(w2_part(pos, dd), rid("w2" + tag) + dd)

    for nm, X, own in ARR:
        for w, dv in (("u", dev(u, d)), ("xr0", dev_R), ("xl0", dev_L)):
            Send(lambda j, X=X, own=own, nm=nm, w=w, dv=dv: (own, ch(X, 0, c, d), rid(nm + w), dv)).start()
    send_w1("v", v, g)
    send_w1("u", u, 1 - g)
    send_w2("v", v)
    send_w2("u", u)
    send_w1("u", u, g)
    for nm, X, own in ARR:
        Send(lambda j, X=X, own=own, nm=nm: (own, ch(X, 0, c, d), rid(nm + "d0c"), dev_e)).start()
    for pos in range(4):
        Send(lambda j, pos=pos: (w1_src(pos, e), w1_dst(d, r, pos), rid("w1d") + pos, dev_e)).start()
    Send(lambda j: (w2.at[pl.ds(mul(e, FB), FB), :], w2_part(pos_r, d), rid("w2d"), dev_e)).start()

    def own_copies(b0, b1, b2, b3, sems):
        ld = [cp(a_own, b0, sems.at[0]), cp(g_own, b1, sems.at[1]), cp(w2.at[pl.ds(mul(d, FB), FB), :], b3, sems.at[2])]
        ld += [cp(w1_src(pos, d), b2.at[:, pl.ds(pos * FB, FB)], sems.at[3 + pos]) for pos in range(4)]
        st = [cp(b0, ch(A, 0, c, d), sems.at[7]), cp(b1, ch(G, 0, c, d), sems.at[8]), cp(b3, w2_part(pos_r, d), sems.at[9]),
              cp(b2, W1.at[w1_rows(d, r), :], sems.at[10])]
        start(*ld)
        for i in range(3):
            wait(ld[i])
            start(st[i])
        wait(*ld[3:])
        start(st[3])
        wait(*st)

    pl.run_scoped(own_copies, pltpu.VMEM((TH, DM), BF16), pltpu.VMEM((TH, DM), BF16), pltpu.VMEM((DS, FC), BF16),
                  pltpu.VMEM((FB, DH), BF16), pltpu.SemaphoreType.DMA((11,)))

    fwd = {}
    for nm, X, _ in ARR:
        for t in (0, 1):
            k = nm + str(t)
            fwd[k] = [same(ch(X, t, L, d, 0), rid(nm + "fr" + str(t)), dev_R), same(ch(X, t, R, d, 1), rid(nm + "fl" + str(t)), dev_L),
                      same(ch(X, t, L, d), rid(nm + "d" + str(t) + "L"), dev_e), same(ch(X, t, R, d), rid(nm + "d" + str(t) + "R"), dev_e),
                      same(ch(X, t, far, d, 0), rid(nm + "d" + str(t) + "x"), dev_e), same(ch(X, t, far, d, 1), rid(nm + "d" + str(t) + "y"), dev_e)]
        fwd[nm + "p"] = [same(ch(X, 1, c, d), rid(nm + "xr1"), dev_R), same(ch(X, 1, c, d), rid(nm + "xl1"), dev_L),
                         same(ch(X, 1, c, d), rid(nm + "d1c"), dev_e)]

    def pass_on(nm, X, t):
        f, t_ = fwd[nm + str(t)], str(t)
        arrived(ch(X, t, L, d), rid(nm + "xr" + t_))
        f[0].start()
        arrived(ch(X, t, R, d), rid(nm + "xl" + t_))
        f[1].start()
        f[2].start()
        f[3].start()

    def far_in(nm, X, t):
        f, t_ = fwd[nm + str(t)], str(t)
        arrived(ch(X, t, far, d, 0), rid(nm + "fr" + t_))
        f[4].start()
        arrived(ch(X, t, far, d, 1), rid(nm + "fl" + t_))
        f[5].start()

    def other_core(t, which):
        for nm, X, _ in ARR:
            b = nm + "d" + str(t)
            if which == "far":
                arrived(ch(X, t, far, e, 0), rid(b + "x"))
                arrived(ch(X, t, far, e, 1), rid(b + "y"))
            else:
                arrived(ch(X, t, {"c": c, "L": L, "R": R}[which], e), rid(b + which))

    f1u = Send(lambda j: (W1.at[w1_rows(j, v), half_g], W1.at[w1_rows(j, v), half_g], rid("f1u") + j, dev(u, d)), 2)
    f1v = Send(lambda j: (W1.at[w1_rows(j, u), half_g], W1.at[w1_rows(j, u), half_g], rid("f1v") + j, dev(v, d)), 2)
    q0, q1 = pl.ds(0, BN), pl.ds(BN, DM - BN)

    def w2_rows(pos, cols):
        return W2.at[pl.ds(mul(pos, FB), FB), cols]

    f2u = same(w2_rows(pos_v, q0), rid("f2u"), dev(u, d))
    f2v = same(w2_rows(pos_u, q1), rid("f2v"), dev(v, d))

    pass_on("A", A, 0)
    wait_w1("v", v, g)
    for j in (0, 1):
        f1u.start(j)
    pass_on("G", G, 0)
    for nm, X, _ in ARR:
        arrived(ch(X, 1, c, d), rid(nm + "u"))
        for t in fwd[nm + "p"]:
            t.start()
    wait_w1("u", u, g)
    for j in (0, 1):
        f1v.start(j)
    send_w1("v", v, 1 - g)
    for nm, X, _ in ARR:
        far_in(nm, X, 0)
    wait_w2("v", pos_v)
    f2u.start()
    for which in ("c", "L", "R", "far"):
        other_core(0, which)
    for ii in (0, 1):
        arrived(w1_dst(e, r, 2 * g + ii), rid("w1d") + 2 * g + ii)
    arrived(w2_part(pos_r, e), rid("w2d"))
    for j in (0, 1):
        arrived(W1.at[w1_rows(j, q), half_g], rid("f1v") + j)

    RC = min(32, TH)

    def cd_block(a, gr, w1b, w2b, bias, cbuf, gbuf, put, dbs, count_db):
        cbuf[...] = jnp.dot(a, w1b, preferred_element_type=F32)
        gbuf[...] = lax.dot_general(gr, w2b, (((1,), (1,)), ((), ())), preferred_element_type=F32)

        def rows(m, acc):
            sl = pl.ds(mul(m, RC), RC)
            pre = cbuf[sl, :] + bias
            sq = pre * pre
            th = jnp.tanh(GELU_K * (pre + GELU_C * pre * sq))
            half = 0.5 * (1.0 + th)
            slope = half + 0.5 * pre * (1.0 - th * th) * GELU_K * (1.0 + 3.0 * GELU_C * sq)
            dc = gbuf[sl, :] * slope
            put(sl, (pre * half).astype(BF16), dc.astype(BF16))
            return acc + jnp.sum(dc.reshape(RC // 8, 8, FB), axis=0)

        acc = lax.fori_loop(0, T2 // RC, rows, jnp.zeros((8, FB), F32))

        @pl.when(count_db)
        def _():
            dbs[...] += acc

    def order(k):
        k = k % 4
        return (c + k + k // 2 * (5 - 2 * k)) % 4

    def phase1(ab, gb, w1b, w2b, cbuf, gbuf, hb, cb, dbs, isem, osem, wsem):
        wl = [cp(W1.at[:, half_g], w1b, wsem.at[0]), cp(W2.at[half_g, :], w2b, wsem.at[1])]
        start(*wl)
        dbs[...] = jnp.zeros_like(dbs)

        def row_of(k):
            return jnp.where(k < 4, hp, 1 - hp)

        def ins(k, s):
            return [cp(A.at[row_of(k), order(k)], ab.at[s], isem.at[s]), cp(G.at[row_of(k), order(k)], gb.at[s], isem.at[2 + s])]

        def outs(k, s):
            at = (row_of(k), order(k) // 2, order(k) % 2)
            return [cp(hb.at[s], o["HP"].at[at], osem.at[s]), cp(cb.at[s], o["CP"].at[at], osem.at[2 + s])]

        start(*ins(0, 0))
        wait(*wl)

        def fetch(k):
            @pl.when(k == 0)
            def _():
                pass_on("A", A, 1)

            @pl.when(k == 3)
            def _():
                other_core(1, "c")

            @pl.when(k == 4)
            def _():
                pass_on("G", G, 1)
                wait_w2("u", pos_u)
                f2v.start()
                other_core(1, "R")

            @pl.when(k == 5)
            def _():
                other_core(1, "L")

            @pl.when(k == 6)
            def _():
                for nm, X, _ in ARR:
                    far_in(nm, X, 1)
                other_core(1, "far")

            @pl.when(k < 7)
            def _():
                start(*ins(k + 1, 1 - k % 2))

        def it(k, _):
            s = k % 2
            wait(*ins(k, s))

            @pl.when(k >= 2)
            def _():
                wait(*outs(k - 2, s))

            for ii in (0, 1):
                cols = slice(ii * FB, (ii + 1) * FB)

                def put(sl, h, dc, cols=cols):
                    hb[s, sl, cols] = h
                    cb[s, sl, cols] = dc

                cd_block(ab[s], gb[s], w1b[:, cols], w2b[cols, :], bup[:, pl.ds(mul(2 * g + ii, FB), FB)], cbuf, gbuf, put,
                         dbs.at[:, cols], k < 4)

                @pl.when((k == 6) == (ii == 1))
                def _():
                    fetch(k)
            start(*outs(k, s))
            return 0

        lax.fori_loop(0, 8, it, 0)
        for k in (6, 7):
            wait(*outs(k, k % 2))
        t = cp(dbs, o["DB"].at[:, half_g], wsem.at[0])
        start(t)
        wait(t)

    pl.run_scoped(phase1, pltpu.VMEM((2, T2, DM), BF16), pltpu.VMEM((2, T2, DM), BF16), pltpu.VMEM((DM, F2), BF16),
                  pltpu.VMEM((F2, DM), BF16), pltpu.VMEM((T2, FB), F32), pltpu.VMEM((T2, FB), F32),
                  pltpu.VMEM((2, T2, F2), BF16), pltpu.VMEM((2, T2, F2), BF16), pltpu.VMEM((8, F2), F32),
                  pltpu.SemaphoreType.DMA((4,)), pltpu.SemaphoreType.DMA((4,)), pltpu.SemaphoreType.DMA((2,)))

    TN = (((0,), (0,)), ((), ()))
    ALLT = 8 * T2

    s1 = Send(lambda j: (o["S1"].at[j], o["R1"].at[j], rid("s1") + j, dev(v, d)), 4)
    s2 = Send(lambda j: (o["S2"].at[:, pl.ds(mul(j, BN), BN)], o["R2"].at[:, pl.ds(mul(j, BN), BN)], rid("s2") + j, dev(v, d)), 4)

    def run(n, ins, outs, work, done):
        start(*ins(0, 0))

        def it(k, _):
            s = k % 2
            wait(*ins(k, s))

            @pl.when(k < n - 1)
            def _():
                start(*ins(k + 1, 1 - s))
            work(k, s)
            start(*outs(k, s))

            @pl.when(k >= 1)
            def _():
                wait(*outs(k - 1, 1 - s))
                done(k - 1, 1 - s)
            return 0

        lax.fori_loop(0, n, it, 0)
        wait(*outs(n - 1, (n - 1) % 2))
        done(n - 1, (n - 1) % 2)

    def dw1_cols(k, pair, first):
        j = first + (1 - 2 * first) * (k // 2)
        return pl.ds(mul((k % 2) * 4 + 2 * pair + j, DS), DS)

    def dw1_send(dcb, ab, ob, isem, osem, wsem):
        t = cp(o["CP"], dcb, wsem.at[0])
        start(t)
        wait(t)

        def work(k, s):
            ob[s] = lax.dot_general(ab[s].reshape(ALLT, DS), dcb[...].reshape(ALLT, F2), TN, preferred_element_type=F32)

        run(4, lambda k, s: [cp(A.at[:, :, :, dw1_cols(k, 1 - hi, hp)], ab.at[s], isem.at[s])],
            lambda k, s: [cp(ob.at[s], o["S1"].at[k], osem.at[s])], work, lambda k, s: s1.start(k))

    pl.run_scoped(dw1_send, pltpu.VMEM((2, 2, 2, T2, F2), BF16), pltpu.VMEM((2, 2, 4, T2, DS), BF16), pltpu.VMEM((2, DS, F2), F32),
                  pltpu.SemaphoreType.DMA((2,)), pltpu.SemaphoreType.DMA((2,)), pltpu.SemaphoreType.DMA((1,)))

    def block_of(j):
        return pl.ds(mul(j, BN), BN)

    def h_cols(pair):
        return pl.ds(mul(pair, FB), FB)

    def dw2_send(hb, gb, ob, isem, osem, wsem):
        t = cp(o["HP"].at[:, :, :, :, h_cols(1 - hi)], hb, wsem.at[0])
        start(t)
        wait(t)

        def work(k, s):
            ob[s] = lax.dot_general(hb[...].reshape(ALLT, FB), gb[s].reshape(ALLT, BN), TN, preferred_element_type=F32)

        run(4, lambda k, s: [cp(G.at[:, :, :, block_of(k)], gb.at[s], isem.at[s])],
            lambda k, s: [cp(ob.at[s], o["S2"].at[:, block_of(k)], osem.at[s])], work, lambda k, s: s2.start(k))

    pl.run_scoped(dw2_send, pltpu.VMEM((2, 2, 2, T2, FB), BF16), pltpu.VMEM((2, 2, 4, T2, BN), BF16), pltpu.VMEM((2, FB, BN), F32),
                  pltpu.SemaphoreType.DMA((2,)), pltpu.SemaphoreType.DMA((2,)), pltpu.SemaphoreType.DMA((1,)))

    for ii in (0, 1):
        pos = 2 * (1 - g) + ii
        arrived(w1_dst(e, r, pos), rid("w1d") + pos)
    wait_w1("u", u, 1 - g)
    wait_w1("v", v, 1 - g)
    for j in (0, 1):
        arrived(W1.at[w1_rows(j, q), half_n], rid("f1u") + j)

    def phase2(ab, gb, w1b, w2b, cbuf, gbuf, hb, cb, dbs, isem, osem, wsem):
        def pos_of(b):
            return jnp.where(b == 0, pos_u, pos_q)

        def wl(b):
            cols = pl.ds(mul(pos_of(b), FB), FB)
            return [cp(W1.at[:, cols], w1b.at[b], wsem.at[b]), cp(W2.at[cols, :], w2b.at[b], wsem.at[2 + b])]

        start(*wl(0))
        dbs[...] = jnp.zeros_like(dbs)

        def ins(k, s):
            return [cp(A.at[hp, k % 4], ab.at[s], isem.at[s]), cp(G.at[hp, k % 4], gb.at[s], isem.at[2 + s])]

        def outs(k, s):
            at = (k % 4 // 2, k % 2, slice(None), pl.ds(mul(pos_of(k // 4) % 2, FB), FB))
            return [cp(hb.at[s], o["HQ"].at[at], osem.at[s]), cp(cb.at[s], o["CQ"].at[at], osem.at[2 + s])]

        start(*ins(0, 0))

        def it(k, _):
            s, b = k % 2, k // 4

            @pl.when(k % 4 == 0)
            def _():
                wait(*wl(b))
            wait(*ins(k, s))

            @pl.when(k < 7)
            def _():
                start(*ins(k + 1, 1 - s))

            @pl.when(k >= 2)
            def _():
                wait(*outs(k - 2, s))

            def put(sl, h, dc):
                hb[s, sl, :] = h
                cb[s, sl, :] = dc

            cd_block(ab[s], gb[s], w1b[b], w2b[b], bup[:, pl.ds(mul(pos_of(b), FB), FB)], cbuf, gbuf, put, dbs.at[b], k >= 0)
            start(*outs(k, s))

            @pl.when(k == 2)
            def _():
                arrived(w2_rows(pos_q, q1), rid("f2v"))
                arrived(w2_rows(pos_q, q0), rid("f2u"))
                start(*wl(1))
            return 0

        lax.fori_loop(0, 8, it, 0)
        for k in (6, 7):
            wait(*outs(k, k % 2))
        ts = [cp(dbs.at[b], o["DB"].at[:, pl.ds(mul(pos_of(b), FB), FB)], wsem.at[b]) for b in (0, 1)]
        start(*ts)
        wait(*ts)

    pl.run_scoped(phase2, pltpu.VMEM((2, T2, DM), BF16), pltpu.VMEM((2, T2, DM), BF16), pltpu.VMEM((2, DM, FB), BF16),
                  pltpu.VMEM((2, FB, DM), BF16), pltpu.VMEM((T2, FB), F32), pltpu.VMEM((T2, FB), F32),
                  pltpu.VMEM((2, T2, FB), BF16), pltpu.VMEM((2, T2, FB), BF16), pltpu.VMEM((2, 8, FB), F32),
                  pltpu.SemaphoreType.DMA((4,)), pltpu.SemaphoreType.DMA((4,)), pltpu.SemaphoreType.DMA((4,)))

    def wdot(lhs, wref, s, first, nt):
        sel = pl.ds(mul(g if first else 1 - g, F2), F2)
        x = lhs[...].reshape(-1, F2)
        if nt:
            return lax.dot_general(x, wref[s, :, sel], (((1,), (1,)), ((), ())), preferred_element_type=F32)
        return jnp.dot(x, wref[s, sel, :], preferred_element_type=F32)

    def region(s, nt, XP, XQ, PX, RX):
        Q1, Q2, RF, RR = o[s + "Q1"], o[s + "Q2"], o[s + "RF"], o[s + "RX"]
        ex = Send(lambda j: (PX.at[:, :, :, block_of(j)], RX.at[:, :, :, block_of(j)], rid(s + "p") + j, dev_e), 4)
        rows_r, rows_l = pl.ds(0, HT), pl.ds(HT, HT)
        far_r = Send(lambda j: (Q1.at[1 - c_hi, rows_r, block_of(j)], RF.at[1 - c_hi, :, block_of(j)], rid(s + "r") + j, dev_R), 4)
        far_l = Send(lambda j: (Q1.at[1 - c_hi, rows_l, block_of(j)], RF.at[1 - c_hi, :, block_of(j)], rid(s + "l") + j, dev_L), 4)
        pm_r = Send(lambda j: (Q2.at[R // 2, :, block_of(j)], RR.at[0, :, block_of(j)], rid(s + "pr") + j, dev_R), 4)
        pm_l = Send(lambda j: (Q2.at[L // 2, :, block_of(j)], RR.at[1, :, block_of(j)], rid(s + "pl") + j, dev_L), 4)
        wshape = (BN, FC) if nt else (FC, BN)

        def wblk(j, wb, slot, sem):
            src = W1.at[block_of(j), :] if nt else W2.at[:, block_of(j)]
            return cp(src, wb.at[slot], sem.at[slot])

        mine, other = pl.ds(mul(d, TH), TH), pl.ds(mul(e, TH), TH)

        def first(lop, loq, lfp, lfq, wb, ob, ab, qb, wsem, lsem, osem):
            lds = [cp(XP.at[hp, :, :, other], lop, lsem.at[0]), cp(XQ.at[:, :, other], loq, lsem.at[1]),
                   cp(XP.at[hp, :, c_lo, mine], lfp, lsem.at[2]), cp(XQ.at[:, c_lo, mine], lfq, lsem.at[3])]
            start(wblk(0, wb, 0, wsem), *lds)
            wait(*lds)

            def it(j, _):
                slot, prev = j % 3, (j + 2) % 3
                o1 = cp(ob, PX.at[:, :, :, block_of(j)], osem.at[0])

                @pl.when(j < 4)
                def _():
                    wait(wblk(j, wb, slot, wsem))

                    @pl.when(j < 3)
                    def _():
                        start(wblk(j + 1, wb, (j + 1) % 3, wsem))
                    ob[...] = (wdot(lop, wb, slot, True, nt) + wdot(loq, wb, slot, False, nt)).reshape(2, 2, TH, BN)
                    start(o1)

                @pl.when(j >= 1)
                def _():
                    k = j - 1
                    arrived(RX.at[:, :, :, block_of(k)], rid(s + "p") + k)
                    add = cp(RX.at[:, c_lo, :, block_of(k)], ab, osem.at[1])
                    start(add)
                    qb[...] = (wdot(lfp, wb, prev, True, nt) + wdot(lfq, wb, prev, False, nt)).reshape(2, TH, BN)
                    wait(add)
                    qb[...] += ab[...]
                    o2 = cp(qb, Q1.at[:, :, block_of(k)], osem.at[2])
                    start(o2)
                    wait(o2)
                    far_r.start(k)
                    far_l.start(k)

                @pl.when(j < 4)
                def _():
                    wait(o1)
                    ex.start(j)
                return 0

            lax.fori_loop(0, 5, it, 0)

        def second(lp, lq, wb, ab, fb, ob, wsem, lsem, isem, osem):
            lds = [cp(XP.at[hp, :, 1 - c_lo, mine], lp, lsem.at[0]), cp(XQ.at[:, 1 - c_lo, mine], lq, lsem.at[1])]
            start(*lds)

            def ins(k, sl):
                return [wblk(k, wb, sl, wsem), cp(RX.at[:, 1 - c_lo, :, block_of(k)], ab.at[sl], isem.at[sl]),
                        cp(RF.at[:, :, block_of(k)], fb.at[sl], isem.at[2 + sl])]

            def need(k):
                arrived(RF.at[R // 2, :, block_of(k)], rid(s + "r") + k)
                arrived(RF.at[L // 2, :, block_of(k)], rid(s + "l") + k)

            need(0)
            start(*ins(0, 0))
            wait(*lds)

            def outs(k, sl):
                return cp(ob.at[sl], Q2.at[:, :, block_of(k)], osem.at[sl])

            def it(k, _):
                sl = k % 2
                wait(*ins(k, sl))
                ob[sl] = (wdot(lp, wb, sl, True, nt) + wdot(lq, wb, sl, False, nt)).reshape(2, TH, BN) + ab[sl]
                ob[sl, R // 2, 0:HT, :] += fb[sl, R // 2]
                ob[sl, L // 2, HT:TH, :] += fb[sl, L // 2]
                start(outs(k, sl))

                @pl.when(k < 3)
                def _():
                    need(k + 1)
                    start(*ins(k + 1, 1 - sl))
                wait(outs(k, sl))
                pm_r.start(k)
                pm_l.start(k)
                return 0

            lax.fori_loop(0, 4, it, 0)

        def run_first():
            pl.run_scoped(first, pltpu.VMEM((2, 2, TH, F2), BF16), pltpu.VMEM((2, 2, TH, F2), BF16), pltpu.VMEM((2, TH, F2), BF16),
                          pltpu.VMEM((2, TH, F2), BF16), pltpu.VMEM((3,) + wshape, BF16), pltpu.VMEM((2, 2, TH, BN), F32),
                          pltpu.VMEM((2, TH, BN), F32), pltpu.VMEM((2, TH, BN), F32), pltpu.SemaphoreType.DMA((3,)),
                          pltpu.SemaphoreType.DMA((4,)), pltpu.SemaphoreType.DMA((3,)))

        def run_second():
            pl.run_scoped(second, pltpu.VMEM((2, TH, F2), BF16), pltpu.VMEM((2, TH, F2), BF16), pltpu.VMEM((2,) + wshape, BF16),
                          pltpu.VMEM((2, 2, TH, BN), F32), pltpu.VMEM((2, 2, HT, BN), F32), pltpu.VMEM((2, 2, TH, BN), F32),
                          pltpu.SemaphoreType.DMA((2,)), pltpu.SemaphoreType.DMA((2,)), pltpu.SemaphoreType.DMA((4,)),
                          pltpu.SemaphoreType.DMA((2,)))

        def finish():
            for j in range(4):
                arrived(RR.at[0, :, block_of(j)], rid(s + "pr") + j)
                arrived(RR.at[1, :, block_of(j)], rid(s + "pl") + j)
        return run_first, run_second, finish

    y1, y2, y3 = region("Y", False, o["HP"], o["HQ"], o["PY"], o["RY"])
    d1, d2, d3 = region("D", True, o["CP"], o["CQ"], o["PD"], o["RD"])
    y1()
    d1()
    y2()
    d2()

    def out1_cols(ii):
        return pl.ds(mul(((1 - g) * 3 * ii + g * (1 + ii)) * 2 + d, FB), FB)

    K1, K2, OUT1, OUT2 = o["K1"], o["K2"], o["OUT1"], o["OUT2"]

    def piece(ii):
        return slice(ii * FB, (ii + 1) * FB)

    k1u = [Send(lambda m, ii=ii: (K1.at[m, :, piece(ii)], OUT1.at[:, out1_cols(ii)], rid("k1u") + d * 2 + ii, dev(u, m)), 2) for ii in (0, 1)]
    k1d = [Send(lambda m, ii=ii: (K1.at[2 + e, :, piece(ii)], OUT1.at[:, out1_cols(ii)], rid("k1d") + ii, dev_e)) for ii in (0, 1)]

    def out2_at(core, jj):
        return OUT2.at[pl.ds(mul(core, FB), FB), pl.ds(mul(jj, BN), BN)]

    k2 = Send(lambda jj: (K2.at[2 * e + jj], out2_at(d, jj), rid("k2") + jj, dev_e), 2)

    def dw1_keep(dcb, ab, rb, ob, isem, osem, wsem):
        t = cp(o["CP"], dcb, wsem.at[0])
        start(t)

        def ins(k, s):
            return [cp(A.at[:, :, :, dw1_cols(k, hi, 1 - hp)], ab.at[s], isem.at[s]), cp(o["R1"].at[k], rb.at[s], isem.at[2 + s])]

        def outs(k, s):
            return cp(ob.at[s], K1.at[k], osem.at[s])

        arrived(o["R1"].at[0], rid("s1"))
        start(*ins(0, 0))
        wait(t)

        def it(k, _):
            s = k % 2
            wait(*ins(k, s))

            @pl.when(k < 3)
            def _():
                arrived(o["R1"].at[k + 1], rid("s1") + k + 1)
                start(*ins(k + 1, 1 - s))
            acc = lax.dot_general(ab[s].reshape(ALLT, DS), dcb[...].reshape(ALLT, F2), TN, preferred_element_type=F32)
            ob[s] = (acc + rb[s]).astype(BF16)
            start(outs(k, s))
            wait(outs(k, s))

            @pl.when(k < 2)
            def _():
                k1u[0].start(k)
                k1u[1].start(k)

            @pl.when(k == 2 + e)
            def _():
                k1d[0].start()
                k1d[1].start()

            @pl.when(k == 2 + d)
            def _():
                ts = [cp(ob.at[s, :, piece(ii)], OUT1.at[:, out1_cols(ii)], wsem.at[ii]) for ii in (0, 1)]
                start(*ts)
                wait(*ts)
            return 0

        lax.fori_loop(0, 4, it, 0)

    pl.run_scoped(dw1_keep, pltpu.VMEM((2, 2, 2, T2, F2), BF16), pltpu.VMEM((2, 2, 4, T2, DS), BF16), pltpu.VMEM((2, DS, F2), F32),
                  pltpu.VMEM((2, DS, F2), BF16), pltpu.SemaphoreType.DMA((4,)), pltpu.SemaphoreType.DMA((2,)), pltpu.SemaphoreType.DMA((2,)))

    def dw2_keep(hb, gb, rb, ob, isem, osem, wsem):
        t = cp(o["HP"].at[:, :, :, :, h_cols(hi)], hb, wsem.at[0])
        start(t)

        def ins(k, s):
            return cp(G.at[:, :, :, block_of(k)], gb.at[s], isem.at[s])

        start(ins(0, 0))
        wait(t)

        def it(k, _):
            s = k % 2
            wait(ins(k, s))

            @pl.when(k < 3)
            def _():
                start(ins(k + 1, 1 - s))
            acc = lax.dot_general(hb[...].reshape(ALLT, FB), gb[s].reshape(ALLT, BN), TN, preferred_element_type=F32)
            arrived(o["R2"].at[:, block_of(k)], rid("s2") + k)
            t = cp(o["R2"].at[:, block_of(k)], rb, osem.at[0])
            start(t)
            wait(t)
            ob[...] = (acc + rb[...]).astype(BF16)

            @pl.when(k // 2 == d)
            def _():
                t = cp(ob, out2_at(d, k % 2), osem.at[1])
                start(t)
                wait(t)

            @pl.when(k // 2 == e)
            def _():
                t = cp(ob, K2.at[k], osem.at[1])
                start(t)
                wait(t)
                k2.start(k % 2)
            return 0

        lax.fori_loop(0, 4, it, 0)

    pl.run_scoped(dw2_keep, pltpu.VMEM((2, 2, 2, T2, FB), BF16), pltpu.VMEM((2, 2, 4, T2, BN), BF16), pltpu.VMEM((FB, BN), F32),
                  pltpu.VMEM((FB, BN), BF16), pltpu.SemaphoreType.DMA((2,)), pltpu.SemaphoreType.DMA((2,)), pltpu.SemaphoreType.DMA((1,)))

    y3()
    d3()
    for ii in (0, 1):
        for dd in (0, 1):
            arrived(OUT1.at[:, pl.ds(mul((g * 3 * ii + (1 - g) * (1 + ii)) * 2 + dd, FB), FB)], rid("k1u") + dd * 2 + ii)
        arrived(OUT1.at[:, pl.ds(mul(((1 - g) * 3 * ii + g * (1 + ii)) * 2 + e, FB), FB)], rid("k1d") + ii)
    for jj in (0, 1):
        arrived(out2_at(e, jj), rid("k2") + jj)
    for s, j in pending:
        s.desc(j).wait_send()


SEMS = (125, 125)


def solution(mesh):
    nr, nc, nd = mesh.shape["row"], mesh.shape["col"], mesh.shape["dep"]
    assert nr == 4 and nc == 4 and nd == 2
    tok_spec = P(("part", "row", "col"), "dep")
    vec_dep = P("dep")
    part_dep = P(("part", "dep"))
    in_specs = (tok_spec, vec_dep, vec_dep, P(("dep", "row"), "col"), P("col"), P(("col", "row"), "dep"), vec_dep, tok_spec)
    out_specs = (tok_spec, tok_spec, P(("part", "dep", "row"), "col"), P(("part", "col")), P(("part", "col", "row"), "dep"), part_dep, part_dep, part_dep)

    def swap(t):
        return lax.ppermute(t, "dep", [(0, 1), (1, 0)])

    def xor(t, axis, m):
        return lax.ppermute(t, axis, [(i, i ^ m) for i in range(4)])

    def local_step(x_in, ln_scale, ln_shift, w_up, b_up, w_down, b_down, y_grad):
        d, c = lax.axis_index("dep"), lax.axis_index("col")
        th, dhalf = x_in.shape[0] // 2, x_in.shape[1]
        dm, ds_, fb = 2 * dhalf, w_up.shape[0], w_up.shape[1] // 8
        lo = d == 0

        def merge_last(mine, other):
            return jnp.where(lo, jnp.concatenate([mine, other], axis=-1), jnp.concatenate([other, mine], axis=-1))

        def tok_half(t, which):
            return lax.dynamic_slice_in_dim(t, which * th, th, 0)

        xo = merge_last(tok_half(x_in, d), swap(tok_half(x_in, 1 - d)))
        go = merge_last(tok_half(y_grad, d), swap(tok_half(y_grad, 1 - d)))
        vecs = jnp.stack([ln_scale, ln_shift, b_down.astype(F32)])
        vecs = merge_last(vecs, swap(vecs))
        gamma, beta, bdn = vecs[0], vecs[1], vecs[2]
        x_float = xo.astype(F32)
        mean_row = jnp.sum(x_float, axis=1, keepdims=True) / dm
        var_row = jnp.sum(x_float * x_float, axis=1, keepdims=True) / dm - mean_row * mean_row
        inv_std = lax.rsqrt(var_row + LN_EPS)
        x_hat = (x_float - mean_row) * inv_std
        ao = (x_hat * gamma + beta).astype(BF16)
        b3 = lax.dynamic_index_in_dim(b_up.reshape(4, 2, fb), d, 1, keepdims=False).astype(F32)
        bup = jnp.concatenate([b3[k] for k in (0, 3, 1, 2)]).reshape(1, 4 * fb)

        cfg = (th, dm, ds_, fb)
        outs = pl.pallas_call(
            functools.partial(kernel, cfg),
            name="mlp_layer",
            out_shape=buffers(*cfg),
            in_specs=[pl.BlockSpec(memory_space=pl.ANY)] * 4 + [pl.BlockSpec(memory_space=pltpu.VMEM)],
            out_specs=[pl.BlockSpec(memory_space=pl.ANY)] * len(NAMES),
            scratch_shapes=[pltpu.SemaphoreType.DMA((SEMS[0],)), pltpu.SemaphoreType.DMA((SEMS[1],))],
            compiler_params=pltpu.CompilerParams(collective_id=0, has_side_effects=True, vmem_limit_bytes=62 * 1024 * 1024),
        )(ao, go, w_up, w_down, bup)
        o = dict(zip(NAMES, outs))

        def total(s):
            own = lax.dynamic_index_in_dim(o[s + "Q1"], c // 2, 0, keepdims=False)
            return own + o[s + "RX"][0] + o[s + "RX"][1]

        def to_out(t):
            mine = lax.dynamic_slice_in_dim(t, d * dhalf, dhalf, 1)
            oth = swap(lax.dynamic_slice_in_dim(t, (1 - d) * dhalf, dhalf, 1))
            return jnp.where(lo, jnp.concatenate([mine, oth], axis=0), jnp.concatenate([oth, mine], axis=0))

        y_out = to_out((x_float + total("Y") + bdn).astype(BF16))
        norm_grad = total("D")
        g_float = go.astype(F32)
        val = norm_grad * gamma
        m1 = jnp.sum(val, axis=1, keepdims=True) / dm
        m2 = jnp.sum(val * x_hat, axis=1, keepdims=True) / dm
        x_grad = to_out((g_float + inv_std * (val - m1 - x_hat * m2)).astype(BF16))

        sums = jnp.stack([jnp.sum(norm_grad * x_hat, axis=0), jnp.sum(norm_grad, axis=0), jnp.sum(g_float, axis=0)])
        s_m = lax.dynamic_slice_in_dim(sums, d * dhalf, dhalf, 1)
        sums = s_m + swap(lax.dynamic_slice_in_dim(sums, (1 - d) * dhalf, dhalf, 1))
        for axis, m in (("row", 1), ("row", 3), ("col", 1), ("col", 3)):
            sums = sums + xor(sums, axis, m)

        db4 = jnp.sum(o["DB"], axis=0).reshape(4, fb)
        db = jnp.stack([db4[k] for k in (0, 2, 3, 1)])
        for m in (1, 3):
            db = db + xor(db, "row", m)
        db_o = swap(db)
        b_up_grad = jnp.where(lo, jnp.stack([db, db_o], axis=1), jnp.stack([db_o, db], axis=1)).reshape(8 * fb)
        return (y_out, x_grad, o["OUT1"], b_up_grad, o["OUT2"], sums[2], sums[0], sums[1])

    return jax.shard_map(local_step, mesh=mesh, in_specs=in_specs, out_specs=out_specs, check_vma=False)
```

```python
import functools

import jax
import jax.numpy as jnp
from jax import lax
from jax.experimental import pallas as pl
from jax.experimental.pallas import tpu as pltpu
from jax.sharding import PartitionSpec as P

LN_EPS = 1e-5
GELU_K = 0.7978845608028654
GELU_C = 0.044715
F32 = jnp.float32
BF16 = jnp.bfloat16
MESH = pl.DeviceIdType.MESH

NAMES = ("A", "G", "W1", "W2", "HP", "HQ", "CP", "CQ", "DB",
         "PY", "RY", "YQ1", "YQ2", "YRF", "YRX", "PD", "RD", "DQ1", "DQ2", "DRF", "DRX",
         "S1", "R1", "S2", "R2", "K1", "K2", "OUT1", "OUT2")
TWO, RING = 2, 4
BOTH, SLOTS = (0, 1), (2,)
NT = (((1,), (1,)), ((), ()))
TN = (((0,), (0,)), ((), ()))


def flip(x):
    return 1 - x


def low(x):
    return x % 2


def high(x):
    return x // 2


def buffers(TH, DM, DS, FB):
    F2, FC, T2 = 2 * FB, 4 * FB, 2 * TH
    pair = (TWO, TWO)
    shapes = {
        "A": ((TWO, RING, T2, DM), BF16), "W1": ((DM, FC), BF16), "W2": ((FC, DM), BF16),
        "HP": (SLOTS + pair + (T2, F2), BF16), "HQ": (pair + (T2, F2), BF16), "DB": ((8, FC), F32),
        "S1": ((RING, DS, F2), F32), "S2": ((FB, DM), F32),
        "K1": ((RING, DS, F2), BF16), "K2": ((RING, FB, high(DM) // TWO), BF16),
        "OUT1": ((DS, 8 * FB), BF16), "OUT2": ((F2, high(DM)), BF16),
    }
    for new, old in (("G", "A"), ("CP", "HP"), ("CQ", "HQ"), ("R1", "S1"), ("R2", "S2")):
        shapes[new] = shapes[old]
    for p, s in (("PY", "Y"), ("PD", "D")):
        shapes[p] = shapes["R" + s] = (pair + (TH, DM), F32)
        for q in ("Q1", "Q2", "RX"):
            shapes[s + q] = (SLOTS + (TH, DM), F32)
        shapes[s + "RF"] = (SLOTS + (high(TH), DM), F32)
    return [jax.ShapeDtypeStruct(*shapes[n]) for n in NAMES]


def mul(x, n):
    return x * n if isinstance(x, int) else pl.multiple_of(x * n, n)


def cp(src, dst, sem):
    return pltpu.make_async_copy(src, dst, sem)


def batch(sem, *pairs):
    return [cp(src, dst, sem.at[i]) for i, (src, dst) in enumerate(pairs)]


def start(copies):
    for t in copies:
        t.start()


def wait(copies):
    for t in copies:
        t.wait()


def move(copies):
    start(copies)
    wait(copies)


def dma(*shape):
    return pltpu.SemaphoreType.DMA(shape)


def bf(*shape):
    return pltpu.VMEM(shape, BF16)


def fl(*shape):
    return pltpu.VMEM(shape, F32)


def when(cond):
    def deco(fn):
        pl.when(cond)(fn)
    return deco


def run(n, ins, outs, isem, osem, work, done=None, posts=None, late=()):
    posts = posts or {}

    def fetch(k, s):
        return batch(isem.at[s], *ins(k, s))

    def back(k, s):
        return batch(osem.at[s], *outs(k, s))

    start(fetch(0, 0))

    def step(k, _):
        s, nxt = low(k), k + 1
        is_late = functools.reduce(jnp.logical_or, [nxt == t for t in late], False)
        more = nxt < n
        wait(fetch(k, s))

        @when(jnp.logical_and(more, jnp.logical_not(is_late)))
        def _():
            start(fetch(nxt, flip(s)))
        if done is None:
            @when(k >= TWO)
            def _():
                wait(back(k, s))
        work(k, s)
        start(back(k, s))
        for t, fn in posts.items():
            when(k == t)(fn)
        if late:
            @when(is_late)
            def _():
                start(fetch(nxt, flip(s)))
        if done is not None:
            wait(back(k, s))
            done(k, s)
        return 0

    lax.fori_loop(0, n, step, 0)
    if done is None:
        for s in BOTH:
            wait(back(s, s))


def kernel(cfg, a_own, g_own, w1, w2, bup, *refs):
    TH, DM, DS, FB = cfg
    o = dict(zip(NAMES, refs[:len(NAMES)]))
    ssem, rsem = refs[len(NAMES):]
    DH, F2, FC, HT, T2 = high(DM), TWO * FB, RING * FB, high(TH), TWO * TH
    BN, ALLT = high(DH), TWO * RING * T2
    A, G, W1, W2 = o["A"], o["G"], o["W1"], o["W2"]
    r, c, d = lax.axis_index("row"), lax.axis_index("col"), lax.axis_index("dep")
    hp, hi = low(r), high(r)
    hn, e = flip(hi), flip(d)
    g = low(r + hi)
    gn = flip(g)
    u, v, q = r + 1 - TWO * hp, RING - 1 - r, (r + TWO) % RING
    R, L, far = (c + 1) % RING, (c + RING - 1) % RING, (c + TWO) % RING
    pos_r, pos_v, pos_u, pos_q = TWO * g + hi, TWO * g + hn, TWO * gn + hi, TWO * gn + hn
    c_lo, c_hi = low(c), high(c)

    ids, counts = {}, [0, 0]

    def name(key, n=1):
        ids[key] = counts[0]
        counts[0] += n

    def rid(key):
        return ids[key]

    for nm in "AG":
        for w in ("xr0", "xl0", "u", "xr1", "xl1", "fr0", "fl0", "fr1", "fl1"):
            name(nm + w)
        for t in "01":
            for w in "cLRxy":
                name(nm + "d" + t + w)
    for s in "uv":
        name("w1" + s, TWO * RING)
        name("w2" + s, TWO)
        name("f1" + s, RING)
        name("f2" + s)
    name("w2d")
    for s in ("w1d", "s1", "s2", "k1u"):
        name(s, RING)
    name("k1d", TWO)
    name("k2", TWO)
    for s in "YD":
        for w in ("p", "r", "l", "pr", "pl"):
            name(s + w, RING)

    pending = []
    dev_e, dev_R, dev_L = {"dep": e}, {"col": R}, {"col": L}

    def dev(row, core):
        return {"row": row, "dep": core}

    class Send:
        def __init__(self, fn, n=1):
            self.fn, self.n, self.sid = fn, n, counts[1]
            counts[1] += n
            pending.append(self)

        def desc(self, j=0):
            src, dst, rsid, device = self.fn(j)
            return pltpu.make_async_remote_copy(src_ref=src, dst_ref=dst, send_sem=ssem.at[self.sid + j], recv_sem=rsem.at[rsid],
                                                device_id=device, device_id_type=MESH)

        def start(self, j=0):
            self.desc(j).start()

        def all(self):
            for j in range(self.n):
                self.start(j)

    def same(ref, rsid, device):
        return Send(lambda j: (ref, ref, rsid, device))

    def arrived(dst, rsid):
        pltpu.make_async_remote_copy(src_ref=dst, dst_ref=dst, send_sem=ssem.at[0], recv_sem=rsem.at[rsid],
                                     device_id=dev_e, device_id_type=MESH).wait_recv()

    barrier = pltpu.get_barrier_semaphore()
    peers = [dev_e, dev_R, dev_L] + [dev(t, k) for t in (u, v) for k in BOTH]
    for p in peers:
        pl.semaphore_signal(barrier, inc=1, device_id=p, device_id_type=MESH)
    pl.semaphore_wait(barrier, len(peers))

    ARR = (("A", A, a_own), ("G", G, g_own))
    ROW = (hp, flip(hp))

    def ch(X, t, col, core, part=None):
        if part is None:
            return X.at[ROW[t], col, pl.ds(mul(core, TH), TH)]
        return X.at[ROW[t], col, pl.ds(pl.multiple_of(core * TH + part * HT, HT), HT)]

    def blk(k, n):
        return pl.ds(mul(k, n), n)

    def f_block(pos, core):
        gg, ii = high(pos), low(pos)
        return blk((flip(gg) * (RING - 1) * ii + gg * (1 + ii)) * TWO + core, FB)

    def w1_src(pos, core):
        return w1.at[:, f_block(pos, core)]

    def w1_dst(dd, row, pos):
        return W1.at[blk(dd * RING + row, DS), blk(pos, FB)]

    def send_w1(tag, row, *positions):
        for pos in positions:
            for core in BOTH:
                Send(lambda j, pos=pos, core=core: (w1_src(pos, core), w1_dst(d, r, pos), rid("w1" + tag) + d * RING + pos, dev(row, core))).start()

    def w2_part(pos, half):
        return W2.at[blk(pos, FB), blk(half, DH)]

    def send_w2(tag, row):
        for core in BOTH:
            Send(lambda j, core=core: (w2.at[blk(core, FB), :], w2_part(pos_r, d), rid("w2" + tag) + d, dev(row, core))).start()

    def wait_w2(tag, pos):
        for dd in BOTH:
            arrived(w2_part(pos, dd), rid("w2" + tag) + dd)

    send_w1("v", v, pos_v, pos_r)
    send_w1("u", u, pos_u, pos_q)
    for nm, X, own in ARR:
        for w, dv in (("u", dev(u, d)), ("xr0", dev_R), ("xl0", dev_L)):
            Send(lambda j, nm=nm, X=X, own=own, w=w, dv=dv: (own, ch(X, 0, c, d), rid(nm + w), dv)).start()
    send_w2("u", u)
    send_w1("u", u, pos_r, pos_v)
    for pos in range(RING):
        Send(lambda j, pos=pos: (w1_src(pos, e), w1_dst(d, r, pos), rid("w1d") + pos, dev_e)).start()
    Send(lambda j: (w2.at[blk(e, FB), :], w2_part(pos_r, d), rid("w2d"), dev_e)).start()
    for nm, X, own in ARR:
        Send(lambda j, nm=nm, X=X, own=own: (own, ch(X, 0, c, d), rid(nm + "d0c"), dev_e)).start()

    def own_copies(b0, b1, b2, b3, sems, sems2):
        ld = batch(sems, (a_own, b0), (g_own, b1), (w2.at[blk(d, FB), :], b3),
                   *[(w1_src(pos, d), b2.at[:, blk(pos, FB)]) for pos in range(RING)])
        st = batch(sems2, (b0, ch(A, 0, c, d)), (b1, ch(G, 0, c, d)), (b3, w2_part(pos_r, d)), (b2, W1.at[blk(d * RING + r, DS), :]))
        start(ld)
        for i, t in enumerate(st):
            wait(ld[i:] if t is st[-1] else ld[i:i + 1])
            t.start()
        wait(st)

    pl.run_scoped(own_copies, bf(TH, DM), bf(TH, DM), bf(DS, FC), bf(FB, DH), dma(RING + RING), dma(RING))

    fwd, par = {}, {}
    for nm, X, _ in ARR:
        for t in BOTH:
            b = nm + "d" + str(t)
            fwd[nm, t] = [same(ch(X, t, L, d, 0), rid(nm + "fr" + str(t)), dev_R), same(ch(X, t, R, d, 1), rid(nm + "fl" + str(t)), dev_L),
                          same(ch(X, t, L, d), rid(b + "L"), dev_e), same(ch(X, t, R, d), rid(b + "R"), dev_e),
                          same(ch(X, t, far, d, 0), rid(b + "x"), dev_e), same(ch(X, t, far, d, 1), rid(b + "y"), dev_e)]
        par[nm] = [same(ch(X, 1, c, d), rid(nm + w), dv) for w, dv in (("xr1", dev_R), ("xl1", dev_L), ("d1c", dev_e))]

    def pass_on(nm, X, t):
        to_r, to_l, d_l, d_r = fwd[nm, t][:RING]
        arrived(ch(X, t, L, d), rid(nm + "xr" + str(t)))
        to_r.start()
        arrived(ch(X, t, R, d), rid(nm + "xl" + str(t)))
        to_l.start()
        d_l.start()
        d_r.start()

    def from_u(nm, X):
        arrived(ch(X, 1, c, d), rid(nm + "u"))
        for t in par[nm]:
            t.start()

    def far_in(nm, X, t):
        for part, w in zip(BOTH, ("fr", "fl")):
            arrived(ch(X, t, far, d, part), rid(nm + w + str(t)))
            fwd[nm, t][RING + part].start()

    def other_core(t, *which):
        for nm, X, _ in ARR:
            b = nm + "d" + str(t)
            for w in which:
                if w == "far":
                    for part, z in zip(BOTH, "xy"):
                        arrived(ch(X, t, far, e, part), rid(b + z))
                else:
                    arrived(ch(X, t, {"c": c, "L": L, "R": R}[w], e), rid(b + w))

    def hop(tag, row, device, *positions):
        out = []
        for pos in positions:
            out.append(Send(lambda j, pos=pos: (w1_dst(j, row, pos), w1_dst(j, row, pos), rid(tag) + low(pos) * TWO + j, device), TWO))
        return out

    f1v = hop("f1v", u, dev(v, d), pos_v, pos_r)
    f1u = hop("f1u", v, dev(u, d), pos_r, pos_v)
    q0, q1 = pl.ds(0, BN), pl.ds(BN, DM - BN)
    f2u = same(W2.at[blk(pos_v, FB), q0], rid("f2u"), dev(u, d))
    f2v = same(W2.at[blk(pos_u, FB), q1], rid("f2v"), dev(v, d))

    def w1_in(tag, row, pos):
        for dd in BOTH:
            arrived(w1_dst(dd, row, pos), rid("w1" + tag) + dd * RING + pos)

    def w1_rest(pos, tag):
        arrived(w1_dst(e, r, pos), rid("w1d") + pos)
        for j in BOTH:
            arrived(w1_dst(j, q, pos), rid(tag) + low(pos) * TWO + j)

    for pos in (pos_r, pos_v):
        w1_in("u", u, pos)
    for t in f1v:
        t.all()
    send_w2("v", v)
    send_w1("v", v, pos_q, pos_u)
    pass_on("A", A, 0)
    for pos in (pos_r, pos_v):
        w1_in("v", v, pos)
    for t in f1u:
        t.all()
    other_core(0, "c")
    arrived(w2_part(pos_r, e), rid("w2d"))
    w1_rest(pos_r, "f1v")

    RC = min(8 * RING, TH)

    def cd_block(a, gr, w1b, w2b, bias, cbuf, gbuf, h_out, dc_out, db, count_db):
        cbuf[:] = jnp.dot(a, w1b, preferred_element_type=F32)
        gbuf[:] = lax.dot_general(gr, w2b, NT, preferred_element_type=F32)

        def rows(m, acc):
            sl = blk(m, RC)
            pre = cbuf[sl, :] + bias
            sq = pre * pre
            th = jnp.tanh(GELU_K * (pre + GELU_C * pre * sq))
            half = 0.5 * (1.0 + th)
            slope = half + 0.5 * pre * (1.0 - th * th) * GELU_K * (1.0 + 3.0 * GELU_C * sq)
            dc = gbuf[sl, :] * slope
            h_out[sl, :] = (pre * half).astype(BF16)
            dc_out[sl, :] = dc.astype(BF16)
            return acc + jnp.sum(dc.reshape(RC // 8, 8, FB), axis=0)

        acc = lax.fori_loop(0, T2 // RC, rows, jnp.zeros((8, FB), F32))

        @when(count_db)
        def _():
            db[:] += acc

    def hidden(n, place, block, need, first, posts, late):
        def body(ab, gb, w1b, w2b, cbuf, gbuf, hb, cb, dbs, isem, osem, wsem):
            def weights(b):
                pos = block(b * first)[1]
                return batch(wsem.at[b], (W1.at[:, blk(pos, FB)], w1b.at[b]), (W2.at[blk(pos, FB), :], w2b.at[b]))

            def load(b):
                need(b)
                start(weights(b))

            load(0)
            dbs[:] = jnp.zeros_like(dbs)

            def ins(k, s):
                row, col, _ = place(k)
                return (A.at[row, col], ab.at[s]), (G.at[row, col], gb.at[s])

            def outs(k, s):
                row, col, _ = place(k)
                to_p, cols = block(k)[TWO:]
                at = (high(col), low(col), slice(None), cols)
                H, C = (o["HP"].at[row], o["CP"].at[row]) if to_p else (o["HQ"], o["CQ"])
                return (hb.at[s], H.at[at]), (cb.at[s], C.at[at])

            def work(k, s):
                b, pos = block(k)[:TWO]
                for t in BOTH:
                    @when(k == t * first)
                    def _():
                        wait(weights(t))
                cd_block(ab[s], gb[s], w1b[b], w2b[b], bup[:, blk(pos, FB)], cbuf, gbuf, hb.at[s], cb.at[s], dbs.at[b], place(k)[TWO])

            run(n, ins, outs, isem, osem, work, posts={k: functools.partial(fn, load) for k, fn in posts.items()}, late=late)
            move(batch(wsem.at[0], *[(dbs.at[b], o["DB"].at[:, blk(block(b * first)[1], FB)]) for b in BOTH]))

        pl.run_scoped(body, bf(TWO, T2, DM), bf(TWO, T2, DM), bf(TWO, DM, FB), bf(TWO, FB, DM), fl(T2, FB), fl(T2, FB),
                      bf(TWO, T2, FB), bf(TWO, T2, FB), fl(TWO, 8, FB), dma(TWO, TWO), dma(TWO, TWO), dma(TWO, TWO))

    five, ten = RING + 1, TWO * RING + TWO

    def place1(k):
        early = k < ten
        k5, k2 = k % five, high(k - ten) + 1
        mine = jnp.logical_and(early, k5 < RING)
        m = jnp.where(early, k5 % RING, k2)
        return jnp.where(mine, hp, flip(hp)), (c + m + high(m) * (five - TWO * m)) % RING, mine

    def block1(k):
        b = jnp.where(k < ten, k // five % TWO, low(k))
        ii = jnp.where(b == 0, hi, hn)
        return b, TWO * g + ii, True, blk(ii, FB)

    def need1(b):
        if b:
            wait_w2("v", pos_v)
            f2u.start()
            w1_rest(pos_v, "f1v")

    def post0(load):
        pass_on("G", G, 0)
        from_u("A", A)
        other_core(0, "L", "R")

    def post2(load):
        far_in("A", A, 0)
        from_u("G", G)
        far_in("G", G, 0)
        other_core(0, "far")

    def post9(load):
        pass_on("G", G, 1)
        wait_w2("u", pos_u)
        f2v.start()
        other_core(1, "L", "R")

    def post13(load):
        for nm, X, _ in ARR:
            far_in(nm, X, 1)
        other_core(1, "far")

    posts1 = {0: post0, TWO: post2, RING - 1: lambda load: other_core(1, "c"), RING: lambda load: load(1),
              five: lambda load: pass_on("A", A, 1), ten - 1: post9, ten + RING - 1: post13}
    hidden(ten + RING + TWO, place1, block1, need1, five, posts1, (1, RING - 1, RING, ten, ten + RING))

    S1, R1, S2, R2, K1, K2, OUT1, OUT2 = [o[t] for t in ("S1", "R1", "S2", "R2", "K1", "K2", "OUT1", "OUT2")]
    s1 = Send(lambda j: (S1.at[j], R1.at[j], rid("s1") + j, dev(v, d)), RING)
    s2 = Send(lambda j: (S2.at[:, blk(j, BN)], R2.at[:, blk(j, BN)], rid("s2") + j, dev(v, d)), RING)

    def dw1_cols(k, pair, first):
        j = first + (1 - TWO * first) * high(k)
        return blk(low(k) * RING + TWO * pair + j, DS)

    def grad(left, right, left_shape, right_shape, resident, out_shape, outs, done, recv=None):
        rows, width = out_shape

        def body(lb, rb, acc, ob, nb, isem, osem, wsem):
            stay = batch(wsem, resident((lb, rb)))
            start(stay)

            def ins(k, s):
                return (left(k), lb.at[s]) if right is None else (right(k), rb.at[s]),

            def work(k, s):
                @when(k == 0)
                def _():
                    wait(stay)
                x, y = (lb[s], rb[:]) if right is None else (lb[:], rb[s])
                val = lax.dot_general(x.reshape(ALLT, rows), y.reshape(ALLT, width), TN, preferred_element_type=F32)
                if recv is None:
                    ob[s] = val
                else:
                    acc[:] = val
                    ref, rsid = recv(k)
                    arrived(ref, rsid)
                    move(batch(wsem, (ref, nb)))
                    ob[s] = (acc[:] + nb[:]).astype(BF16)

            run(RING, ins, lambda k, s: ((ob.at[s], outs(k)),), isem, osem, work, done=lambda k, s: done(k, ob.at[s], wsem))

        extra = out_shape if recv else (8, BN)
        pl.run_scoped(body, bf(*left_shape), bf(*right_shape), fl(*extra), pltpu.VMEM(SLOTS + out_shape, BF16 if recv else F32), fl(*extra),
                      dma(TWO, 1), dma(TWO, 1), dma(TWO))

    PT, PTS = (TWO, RING, T2), (TWO, TWO, TWO, T2)

    def grad1(pair, first, outs, done, recv=None):
        grad(lambda k: A.at[:, :, :, dw1_cols(k, pair, first)], None, SLOTS + PT + (DS,), PTS + (F2,), lambda b: (o["CP"], b[1]),
             (DS, F2), outs, done, recv)

    def grad2(pair, outs, done, recv=None):
        grad(None, lambda k: G.at[:, :, :, blk(k, BN)], PTS + (FB,), SLOTS + PT + (BN,), lambda b: (o["HP"].at[:, :, :, :, blk(pair, FB)], b[0]),
             (FB, BN), outs, done, recv)

    grad1(hn, hp, lambda k: S1.at[k], lambda k, ob, sem: s1.start(k))

    def block2(k):
        b = k // RING
        ii = jnp.where(b == 0, hi, hn)
        return b, TWO * gn + ii, False, blk(ii, FB)

    def need2(b):
        pos = pos_q if b else pos_u
        w1_in("u", u, pos)
        w1_in("v", v, pos)
        w1_rest(pos, "f1u")
        if b:
            arrived(W2.at[blk(pos_q, FB), q1], rid("f2v"))
            arrived(W2.at[blk(pos_q, FB), q0], rid("f2u"))

    hidden(TWO * RING, lambda k: (hp, k % RING, k >= 0), block2, need2, RING, {TWO: lambda load: load(1)}, ())

    LAG = 2

    def region(s, nt, XP, XQ, PX, RX):
        Q1, Q2, RF, RR = [o[s + t] for t in ("Q1", "Q2", "RF", "RX")]
        ex = Send(lambda j: (PX.at[:, :, :, blk(j, BN)], RX.at[:, :, :, blk(j, BN)], rid(s + "p") + j, dev_e), RING)
        away = flip(c_hi)
        far_r = Send(lambda j: (Q1.at[away, blk(0, HT), blk(j, BN)], RF.at[away, :, blk(j, BN)], rid(s + "r") + j, dev_R), RING)
        far_l = Send(lambda j: (Q1.at[away, blk(1, HT), blk(j, BN)], RF.at[away, :, blk(j, BN)], rid(s + "l") + j, dev_L), RING)
        pm_r = Send(lambda j: (Q2.at[high(R), :, blk(j, BN)], RR.at[0, :, blk(j, BN)], rid(s + "pr") + j, dev_R), RING)
        pm_l = Send(lambda j: (Q2.at[high(L), :, blk(j, BN)], RR.at[1, :, blk(j, BN)], rid(s + "pl") + j, dev_L), RING)
        wshape = (BN, FC) if nt else (FC, BN)
        mine, other = blk(d, TH), blk(e, TH)

        def wsrc(j):
            return W1.at[blk(j, BN), :] if nt else W2.at[:, blk(j, BN)]

        def wdot(p_ref, q_ref, wref, shape):
            total = 0.0
            for ref, half in ((p_ref, g), (q_ref, gn)):
                x, sel = ref[:].reshape(-1, F2), blk(half, F2)
                if nt:
                    total += lax.dot_general(x, wref[:, sel], NT, preferred_element_type=F32)
                else:
                    total += jnp.dot(x, wref[sel, :], preferred_element_type=F32)
            return total.reshape(shape)

        def first(lop, loq, lfp, lfq, wb, ob, ab, qb, wsem, lsem, osem):
            lds = batch(lsem, (XP.at[hp, :, :, other], lop), (XQ.at[:, :, other], loq), (XP.at[hp, :, c_lo, mine], lfp), (XQ.at[:, c_lo, mine], lfq))

            def wcp(j):
                return batch(wsem.at[j % RING], (wsrc(j), wb.at[j % RING]))

            start(wcp(0) + lds)
            wait(lds)

            def step(j, _):
                o1 = batch(osem, (ob, PX.at[:, :, :, blk(j, BN)]))

                @when(j < RING)
                def _():
                    wait(wcp(j))

                    @when(j < RING - 1)
                    def _():
                        start(wcp(j + 1))
                    ob[:] = wdot(lop, loq, wb.at[j % RING], (TWO, TWO, TH, BN))
                    start(o1)

                @when(j >= LAG)
                def _():
                    k = j - LAG
                    arrived(RX.at[:, :, :, blk(k, BN)], rid(s + "p") + k)
                    add = batch(lsem, (RX.at[:, c_lo, :, blk(k, BN)], ab))
                    start(add)
                    qb[:] = wdot(lfp, lfq, wb.at[k % RING], (TWO, TH, BN))
                    wait(add)
                    qb[:] += ab[:]

                @when(j < RING)
                def _():
                    wait(o1)
                    ex.start(j)

                @when(j >= LAG)
                def _():
                    k = j - LAG
                    move(batch(lsem, (qb, Q1.at[:, :, blk(k, BN)])))
                    far_r.start(k)
                    far_l.start(k)
                return 0

            lax.fori_loop(0, RING + LAG, step, 0)

        def second(lp, lq, wb, ab, fb, ob, lsem, isem, osem):
            lds = batch(lsem, (XP.at[hp, :, flip(c_lo), mine], lp), (XQ.at[:, flip(c_lo), mine], lq))
            start(lds)

            def need(k):
                arrived(RF.at[high(R), :, blk(k, BN)], rid(s + "r") + k)
                arrived(RF.at[high(L), :, blk(k, BN)], rid(s + "l") + k)

            for k in range(RING):
                need(k)
            wait(lds)

            def ins(k, sl):
                return (wsrc(k), wb.at[sl]), (RX.at[:, flip(c_lo), :, blk(k, BN)], ab.at[sl]), (RF.at[:, :, blk(k, BN)], fb.at[sl])

            def work(k, sl):
                ob[sl] = wdot(lp, lq, wb.at[sl], (TWO, TH, BN)) + ab[sl]
                for col, part in ((R, 0), (L, 1)):
                    ob[sl, high(col), part * HT:(part + 1) * HT, :] += fb[sl, high(col)]

            def done(k, sl):
                pm_r.start(k)
                pm_l.start(k)

            run(RING, ins, lambda k, sl: ((ob.at[sl], Q2.at[:, :, blk(k, BN)]),), isem, osem, work, done=done)

        def run_first():
            pl.run_scoped(first, bf(TWO, TWO, TH, F2), bf(TWO, TWO, TH, F2), bf(TWO, TH, F2), bf(TWO, TH, F2), bf(RING, *wshape),
                          fl(TWO, TWO, TH, BN), fl(TWO, TH, BN), fl(TWO, TH, BN), dma(RING, 1), dma(RING), dma(1))

        def run_second():
            pl.run_scoped(second, bf(TWO, TH, F2), bf(TWO, TH, F2), bf(TWO, *wshape), fl(TWO, TWO, TH, BN), fl(TWO, TWO, HT, BN),
                          fl(TWO, TWO, TH, BN), dma(TWO), dma(TWO, RING), dma(TWO, 1))

        def finish():
            for j in range(RING):
                arrived(RR.at[0, :, blk(j, BN)], rid(s + "pr") + j)
                arrived(RR.at[1, :, blk(j, BN)], rid(s + "pl") + j)
        return run_first, run_second, finish

    y1, y2, y3 = region("Y", False, o["HP"], o["HQ"], o["PY"], o["RY"])
    d1, d2, d3 = region("D", True, o["CP"], o["CQ"], o["PD"], o["RD"])
    y1()
    d1()
    y2()
    grad2(hn, lambda k: S2.at[:, blk(k, BN)], lambda k, ob, sem: s2.start(k))
    d2()

    def piece(ii):
        return slice(ii * FB, (ii + 1) * FB)

    k1u = [Send(lambda m, ii=ii: (K1.at[m, :, piece(ii)], OUT1.at[:, f_block(TWO * g + ii, d)], rid("k1u") + d * TWO + ii, dev(u, m)), TWO)
           for ii in BOTH]
    k1d = [Send(lambda m, ii=ii: (K1.at[TWO + e, :, piece(ii)], OUT1.at[:, f_block(TWO * g + ii, d)], rid("k1d") + ii, dev_e)) for ii in BOTH]

    def done1(k, ob, sem):
        @when(k < TWO)
        def _():
            for t in k1u:
                t.start(k)

        @when(k == TWO + e)
        def _():
            for t in k1d:
                t.start()

        @when(k == TWO + d)
        def _():
            move(batch(sem, *[(ob.at[:, piece(ii)], OUT1.at[:, f_block(TWO * g + ii, d)]) for ii in BOTH]))

    def out2_at(core, jj):
        return OUT2.at[blk(core, FB), blk(jj, BN)]

    k2 = Send(lambda jj: (K2.at[TWO * e + jj], out2_at(d, jj), rid("k2") + jj, dev_e), TWO)

    def done2(k, ob, sem):
        @when(high(k) == d)
        def _():
            move(batch(sem, (ob, out2_at(d, low(k)))))

        @when(high(k) == e)
        def _():
            k2.start(low(k))

    grad1(hi, flip(hp), lambda k: K1.at[k], done1, lambda k: (R1.at[k], rid("s1") + k))
    grad2(hi, lambda k: K2.at[k], done2, lambda k: (R2.at[:, blk(k, BN)], rid("s2") + k))

    y3()
    d3()
    for ii in BOTH:
        for dd in BOTH:
            arrived(OUT1.at[:, f_block(TWO * gn + ii, dd)], rid("k1u") + dd * TWO + ii)
        arrived(OUT1.at[:, f_block(TWO * g + ii, e)], rid("k1d") + ii)
        arrived(out2_at(e, ii), rid("k2") + ii)
    for t in pending:
        for j in range(t.n):
            t.desc(j).wait_send()
    assert tuple(counts) == SEMS, counts


SEMS = (129, 129)


def solution(mesh):
    nr, nc, nd = mesh.shape["row"], mesh.shape["col"], mesh.shape["dep"]
    assert nr == 4 and nc == 4 and nd == 2
    tok_spec = P(("part", "row", "col"), "dep")
    vec_dep = P("dep")
    part_dep = P(("part", "dep"))
    in_specs = (tok_spec, vec_dep, vec_dep, P(("dep", "row"), "col"), P("col"), P(("col", "row"), "dep"), vec_dep, tok_spec)
    out_specs = (tok_spec, tok_spec, P(("part", "dep", "row"), "col"), P(("part", "col")), P(("part", "col", "row"), "dep"), part_dep, part_dep, part_dep)

    def swap(t):
        return lax.ppermute(t, "dep", [(0, 1), (1, 0)])

    def xor(t, axis, m):
        return lax.ppermute(t, axis, [(i, i ^ m) for i in range(4)])

    def local_step(x_in, ln_scale, ln_shift, w_up, b_up, w_down, b_down, y_grad):
        d, c = lax.axis_index("dep"), lax.axis_index("col")
        th, dhalf = x_in.shape[0] // 2, x_in.shape[1]
        dm, ds_, fb = 2 * dhalf, w_up.shape[0], w_up.shape[1] // 8
        lo = d == 0

        def merge_last(mine, other):
            return jnp.where(lo, jnp.concatenate([mine, other], axis=-1), jnp.concatenate([other, mine], axis=-1))

        def tok_half(t, which):
            return lax.dynamic_slice_in_dim(t, which * th, th, 0)

        xo = merge_last(tok_half(x_in, d), swap(tok_half(x_in, 1 - d)))
        go = merge_last(tok_half(y_grad, d), swap(tok_half(y_grad, 1 - d)))
        vecs = jnp.stack([ln_scale, ln_shift, b_down.astype(F32)])
        vecs = merge_last(vecs, swap(vecs))
        gamma, beta, bdn = vecs[0], vecs[1], vecs[2]
        x_float = xo.astype(F32)
        mean_row = jnp.sum(x_float, axis=1, keepdims=True) / dm
        var_row = jnp.sum(x_float * x_float, axis=1, keepdims=True) / dm - mean_row * mean_row
        inv_std = lax.rsqrt(var_row + LN_EPS)
        x_hat = (x_float - mean_row) * inv_std
        ao = (x_hat * gamma + beta).astype(BF16)
        b3 = lax.dynamic_index_in_dim(b_up.reshape(4, 2, fb), d, 1, keepdims=False).astype(F32)
        bup = jnp.concatenate([b3[k] for k in (0, 3, 1, 2)]).reshape(1, 4 * fb)

        cfg = (th, dm, ds_, fb)
        outs = pl.pallas_call(
            functools.partial(kernel, cfg),
            name="mlp_layer",
            out_shape=buffers(*cfg),
            in_specs=[pl.BlockSpec(memory_space=pl.ANY)] * 4 + [pl.BlockSpec(memory_space=pltpu.VMEM)],
            out_specs=[pl.BlockSpec(memory_space=pl.ANY)] * len(NAMES),
            scratch_shapes=[dma(SEMS[0]), dma(SEMS[1])],
            compiler_params=pltpu.CompilerParams(collective_id=0, has_side_effects=True, vmem_limit_bytes=62 * 1024 * 1024),
        )(ao, go, w_up, w_down, bup)
        o = dict(zip(NAMES, outs))

        def total(s):
            own = lax.dynamic_index_in_dim(o[s + "Q1"], c // 2, 0, keepdims=False)
            return own + o[s + "RX"][0] + o[s + "RX"][1]

        def to_out(t):
            mine = lax.dynamic_slice_in_dim(t, d * dhalf, dhalf, 1)
            oth = swap(lax.dynamic_slice_in_dim(t, (1 - d) * dhalf, dhalf, 1))
            return jnp.where(lo, jnp.concatenate([mine, oth], axis=0), jnp.concatenate([oth, mine], axis=0))

        y_out = to_out((x_float + total("Y") + bdn).astype(BF16))
        norm_grad = total("D")
        g_float = go.astype(F32)
        val = norm_grad * gamma
        m1 = jnp.sum(val, axis=1, keepdims=True) / dm
        m2 = jnp.sum(val * x_hat, axis=1, keepdims=True) / dm
        x_grad = to_out((g_float + inv_std * (val - m1 - x_hat * m2)).astype(BF16))

        sums = jnp.stack([jnp.sum(norm_grad * x_hat, axis=0), jnp.sum(norm_grad, axis=0), jnp.sum(g_float, axis=0)])
        s_m = lax.dynamic_slice_in_dim(sums, d * dhalf, dhalf, 1)
        sums = s_m + swap(lax.dynamic_slice_in_dim(sums, (1 - d) * dhalf, dhalf, 1))
        for axis, m in (("row", 1), ("row", 3), ("col", 1), ("col", 3)):
            sums = sums + xor(sums, axis, m)

        db4 = jnp.sum(o["DB"], axis=0).reshape(4, fb)
        db = jnp.stack([db4[k] for k in (0, 2, 3, 1)])
        for m in (1, 3):
            db = db + xor(db, "row", m)
        db_o = swap(db)
        b_up_grad = jnp.where(lo, jnp.stack([db, db_o], axis=1), jnp.stack([db_o, db], axis=1)).reshape(8 * fb)
        return (y_out, x_grad, o["OUT1"], b_up_grad, o["OUT2"], sums[2], sums[0], sums[1])

    return jax.shard_map(local_step, mesh=mesh, in_specs=in_specs, out_specs=out_specs, check_vma=False)
```

```python
import functools

import jax
import jax.numpy as jnp
from jax import lax
from jax.experimental import pallas as pl
from jax.experimental.pallas import tpu as pltpu
from jax.sharding import PartitionSpec as P

LN_EPS = 1e-5
GELU_K = 0.7978845608028654
GELU_C = 0.044715
F32 = jnp.float32
BF16 = jnp.bfloat16
MESH = pl.DeviceIdType.MESH

NAMES = ("A", "G", "W1", "W2", "HP", "HQ", "CP", "CQ", "DB",
         "PY", "RY", "YQ1", "YQ2", "YRF", "YRX", "PD", "RD", "DQ1", "DQ2", "DRF", "DRX",
         "S1", "R1", "S2", "R2", "K1", "K2", "OUT1", "OUT2", "XF", "GF", "PV", "YO", "XO", "OUTY", "OUTX", "BG", "SO")
TWO, RING, STAGES = 2, 4, 5
BOTH, SLOTS = (0, 1), (2,)
NT = (((1,), (1,)), ((), ()))
TN = (((0,), (0,)), ((), ()))


def flip(x):
    return 1 - x


def low(x):
    return x % 2


def high(x):
    return x // 2


def buffers(TH, DM, DS, FB):
    F2, FC, T2 = 2 * FB, 4 * FB, 2 * TH
    pair = (TWO, TWO)
    shapes = {
        "A": ((TWO, RING, T2, DM), BF16), "W1": ((DM, FC), BF16), "W2": ((FC, DM), BF16),
        "HP": (SLOTS + pair + (T2, F2), BF16), "HQ": (pair + (T2, F2), BF16), "DB": ((8, FC), F32),
        "S1": ((RING, DS, F2), F32), "S2": ((FB, DM), F32),
        "K1": ((RING, DS, F2), BF16), "K2": ((RING, FB, high(DM) // TWO), BF16),
        "OUT1": ((DS, 8 * FB), BF16), "OUT2": ((F2, high(DM)), BF16),
        "XF": ((TH, DM), BF16), "GF": ((TH, DM), BF16), "PV": ((8, DM), F32), "YO": ((RING, TH, high(DM) // TWO), BF16),
        "XO": ((TH, high(DM)), BF16), "OUTY": ((T2, high(DM)), BF16), "OUTX": ((T2, high(DM)), BF16),
        "BG": (SLOTS + (8, FC), F32), "SO": ((8, high(DM)), F32),
    }
    for new, old in (("G", "A"), ("CP", "HP"), ("CQ", "HQ"), ("R1", "S1"), ("R2", "S2")):
        shapes[new] = shapes[old]
    for p, s in (("PY", "Y"), ("PD", "D")):
        shapes[p] = shapes["R" + s] = (pair + (TH, DM), F32)
        for q in ("Q1", "Q2", "RX"):
            shapes[s + q] = (SLOTS + (TH, DM), F32)
        shapes[s + "RF"] = (SLOTS + (high(TH), DM), F32)
    return [jax.ShapeDtypeStruct(*shapes[n]) for n in NAMES]


def mul(x, n):
    return x * n if isinstance(x, int) else pl.multiple_of(x * n, n)


def cp(src, dst, sem):
    return pltpu.make_async_copy(src, dst, sem)


def batch(sem, *pairs):
    return [cp(src, dst, sem.at[i]) for i, (src, dst) in enumerate(pairs)]


def start(copies):
    for t in copies:
        t.start()


def wait(copies):
    for t in copies:
        t.wait()


def move(copies):
    start(copies)
    wait(copies)


def dma(*shape):
    return pltpu.SemaphoreType.DMA(shape)


def bf(*shape):
    return pltpu.VMEM(shape, BF16)


def fl(*shape):
    return pltpu.VMEM(shape, F32)


def when(cond):
    def deco(fn):
        pl.when(cond)(fn)
    return deco


def run(n, ins, outs, isem, osem, work, done=None, posts=None, late=()):
    posts = posts or {}

    def fetch(k, s):
        return batch(isem.at[s], *ins(k, s))

    def back(k, s):
        return batch(osem.at[s], *outs(k, s))

    start(fetch(0, 0))

    def step(k, _):
        s, nxt = low(k), k + 1
        is_late = functools.reduce(jnp.logical_or, [nxt == t for t in late], False)
        more = nxt < n
        wait(fetch(k, s))

        @when(jnp.logical_and(more, jnp.logical_not(is_late)))
        def _():
            start(fetch(nxt, flip(s)))
        if done is None:
            @when(k >= TWO)
            def _():
                wait(back(k, s))
        work(k, s)
        start(back(k, s))
        for t, fn in posts.items():
            when(k == t)(fn)
        if late:
            @when(is_late)
            def _():
                start(fetch(nxt, flip(s)))
        if done is not None:
            wait(back(k, s))
            done(k, s)
        return 0

    lax.fori_loop(0, n, step, 0)
    if done is None:
        for s in BOTH:
            wait(back(s, s))


def kernel(cfg, x_in, g_in, w1, w2, vec, bup, *refs):
    TH, DM, DS, FB = cfg
    o = dict(zip(NAMES, refs[:len(NAMES)]))
    ssem, rsem, sums, sums_in, db, db_in = refs[len(NAMES):]
    DH, F2, FC, HT, T2 = high(DM), TWO * FB, RING * FB, high(TH), TWO * TH
    BN, ALLT = high(DH), TWO * RING * T2
    A, G, W1, W2 = o["A"], o["G"], o["W1"], o["W2"]
    r, c, d = lax.axis_index("row"), lax.axis_index("col"), lax.axis_index("dep")
    hp, hi = low(r), high(r)
    hn, e = flip(hi), flip(d)
    g = low(r + hi)
    gn = flip(g)
    u, v, q = r + 1 - TWO * hp, RING - 1 - r, (r + TWO) % RING
    R, L, far = (c + 1) % RING, (c + RING - 1) % RING, (c + TWO) % RING
    pos_r, pos_v, pos_u, pos_q = TWO * g + hi, TWO * g + hn, TWO * gn + hi, TWO * gn + hn
    c_lo, c_hi = low(c), high(c)

    ids, counts = {}, [0, 0]

    def name(key, n=1):
        ids[key] = counts[0]
        counts[0] += n

    def rid(key):
        return ids[key]

    for nm in "AG":
        for w in ("xr0", "xl0", "u", "xr1", "xl1", "fr0", "fl0", "fr1", "fl1"):
            name(nm + w)
        for t in "01":
            for w in "cLRxy":
                name(nm + "d" + t + w)
    for s in "uv":
        name("w1" + s, TWO * RING)
        name("w2" + s, TWO)
        name("f1" + s, RING)
        name("f2" + s)
    for s in ("w2d", "xf", "gf", "pv", "xo", "bg"):
        name(s)
    name("yo", TWO)
    name("bf", TWO)
    name("sum", STAGES)
    for s in ("w1d", "s1", "s2", "k1u"):
        name(s, RING)
    name("k1d", TWO)
    name("k2", TWO)
    for s in "YD":
        for w in ("p", "r", "l", "pr", "pl"):
            name(s + w, RING)

    pending = []
    dev_e, dev_R, dev_L = {"dep": e}, {"col": R}, {"col": L}

    def dev(row, core):
        return {"row": row, "dep": core}

    class Send:
        def __init__(self, fn, n=1):
            self.fn, self.n, self.sid = fn, n, counts[1]
            counts[1] += n
            pending.append(self)

        def desc(self, j=0):
            src, dst, rsid, device = self.fn(j)
            return pltpu.make_async_remote_copy(src_ref=src, dst_ref=dst, send_sem=ssem.at[self.sid + j], recv_sem=rsem.at[rsid],
                                                device_id=device, device_id_type=MESH)

        def start(self, j=0):
            self.desc(j).start()

        def all(self):
            for j in range(self.n):
                self.start(j)

    def same(ref, rsid, device):
        return Send(lambda j: (ref, ref, rsid, device))

    def arrived(dst, rsid):
        pltpu.make_async_remote_copy(src_ref=dst, dst_ref=dst, send_sem=ssem.at[0], recv_sem=rsem.at[rsid],
                                     device_id=dev_e, device_id_type=MESH).wait_recv()

    barrier = pltpu.get_barrier_semaphore()
    peers = [dev_e, dev_R, dev_L] + [dev(t, k) for t in (u, v) for k in BOTH]
    for p in peers:
        pl.semaphore_signal(barrier, inc=1, device_id=p, device_id_type=MESH)
    pl.semaphore_wait(barrier, len(peers))

    ARR = (("A", A), ("G", G))
    ROW = (hp, flip(hp))

    def ch(X, t, col, core, part=None):
        if part is None:
            return X.at[ROW[t], col, pl.ds(mul(core, TH), TH)]
        return X.at[ROW[t], col, pl.ds(pl.multiple_of(core * TH + part * HT, HT), HT)]

    def blk(k, n):
        return pl.ds(mul(k, n), n)

    def f_block(pos, core):
        gg, ii = high(pos), low(pos)
        return blk((flip(gg) * (RING - 1) * ii + gg * (1 + ii)) * TWO + core, FB)

    def w1_src(pos, core):
        return w1.at[:, f_block(pos, core)]

    def w1_dst(dd, row, pos):
        return W1.at[blk(dd * RING + row, DS), blk(pos, FB)]

    def send_w1(tag, row, *positions):
        for pos in positions:
            for core in BOTH:
                Send(lambda j, pos=pos, core=core: (w1_src(pos, core), w1_dst(d, r, pos), rid("w1" + tag) + d * RING + pos, dev(row, core))).start()

    def w2_part(pos, half):
        return W2.at[blk(pos, FB), blk(half, DH)]

    def send_w2(tag, row):
        for core in BOTH:
            Send(lambda j, core=core: (w2.at[blk(core, FB), :], w2_part(pos_r, d), rid("w2" + tag) + d, dev(row, core))).start()

    def wait_w2(tag, pos):
        for dd in BOTH:
            arrived(w2_part(pos, dd), rid("w2" + tag) + dd)

    XF, GF, PV = o["XF"], o["GF"], o["PV"]
    Send(lambda j: (g_in.at[blk(e, TH), :], GF.at[:, blk(d, DH)], rid("gf"), dev_e)).start()
    Send(lambda j: (x_in.at[blk(e, TH), :], XF.at[:, blk(d, DH)], rid("xf"), dev_e)).start()
    Send(lambda j: (vec, PV.at[:, blk(d, DH)], rid("pv"), dev_e)).start()
    send_w1("v", v, pos_v, pos_r)
    send_w1("u", u, pos_u, pos_q)

    RL = min(8 * RING, TH)

    def stats(x):
        mean = jnp.sum(x, axis=1, keepdims=True) / DM
        var = jnp.sum(x * x, axis=1, keepdims=True) / DM - mean * mean
        inv_std = lax.rsqrt(var + LN_EPS)
        return inv_std, (x - mean) * inv_std

    def send_own(nm, X):
        for w, dv in (("u", dev(u, d)), ("xr0", dev_R), ("xl0", dev_L), ("d0c", dev_e)):
            Send(lambda j, w=w, dv=dv: (ch(X, 0, c, d), ch(X, 0, c, d), rid(nm + w), dv)).start()

    def own_part(xb, gb, ab, vb, b2, b3, sems, sems2):
        mine, other = blk(d, DH), blk(e, DH)
        ld = batch(sems, (g_in.at[blk(d, TH), :], gb.at[:, mine]), (x_in.at[blk(d, TH), :], xb.at[:, mine]), (vec, vb.at[:, mine]))
        wl = batch(sems2, (w2.at[blk(d, FB), :], b3), *[(w1_src(pos, d), b2.at[:, blk(pos, FB)]) for pos in range(RING)])
        start(ld + wl)
        wait(ld)
        got = batch(sems, (GF.at[:, other], gb.at[:, other]), (XF.at[:, other], xb.at[:, other]), (PV.at[:, other], vb.at[:, other]))
        for t, ref, w in zip(got, (GF, XF, PV), ("gf", "xf", "pv")):
            arrived(ref.at[:, other], rid(w))
            t.start()
        wait(got[:1])
        move(batch(sems, (gb, ch(G, 0, c, d))))
        wait(got[1:])
        keep = batch(sems, (xb.at[:, mine], XF.at[:, mine]), (vb.at[:, mine], PV.at[:, mine]))
        start(keep)
        scale, shift = vb[0:1, :], vb[1:TWO, :]

        def rows(m, _):
            sl = blk(m, RL)
            ab[sl, :] = (stats(xb[sl, :].astype(F32))[1] * scale + shift).astype(BF16)
            return 0

        lax.fori_loop(0, TH // RL, rows, 0)
        wait(keep)
        send_own("G", G)
        move(batch(sems, (ab, ch(A, 0, c, d))))
        send_own("A", A)
        send_w2("u", u)
        send_w1("u", u, pos_r, pos_v)
        wait(wl)
        move(batch(sems2, (b3, w2_part(pos_r, d)), (b2, W1.at[blk(d * RING + r, DS), :])))

    pl.run_scoped(own_part, bf(TH, DM), bf(TH, DM), bf(TH, DM), fl(8, DM), bf(DS, FC), bf(FB, DH), dma(RING), dma(RING + 1))
    for pos in range(RING):
        Send(lambda j, pos=pos: (w1_src(pos, e), w1_dst(d, r, pos), rid("w1d") + pos, dev_e)).start()
    Send(lambda j: (w2.at[blk(e, FB), :], w2_part(pos_r, d), rid("w2d"), dev_e)).start()

    fwd, par = {}, {}
    for nm, X in ARR:
        for t in BOTH:
            b = nm + "d" + str(t)
            fwd[nm, t] = [same(ch(X, t, L, d, 0), rid(nm + "fr" + str(t)), dev_R), same(ch(X, t, R, d, 1), rid(nm + "fl" + str(t)), dev_L),
                          same(ch(X, t, L, d), rid(b + "L"), dev_e), same(ch(X, t, R, d), rid(b + "R"), dev_e),
                          same(ch(X, t, far, d, 0), rid(b + "x"), dev_e), same(ch(X, t, far, d, 1), rid(b + "y"), dev_e)]
        par[nm] = [same(ch(X, 1, c, d), rid(nm + w), dv) for w, dv in (("xr1", dev_R), ("xl1", dev_L), ("d1c", dev_e))]

    def pass_on(nm, X, t):
        to_r, to_l, d_l, d_r = fwd[nm, t][:RING]
        arrived(ch(X, t, L, d), rid(nm + "xr" + str(t)))
        to_r.start()
        arrived(ch(X, t, R, d), rid(nm + "xl" + str(t)))
        to_l.start()
        d_l.start()
        d_r.start()

    def from_u(nm, X):
        arrived(ch(X, 1, c, d), rid(nm + "u"))
        for t in par[nm]:
            t.start()

    def far_in(nm, X, t):
        for part, w in zip(BOTH, ("fr", "fl")):
            arrived(ch(X, t, far, d, part), rid(nm + w + str(t)))
            fwd[nm, t][RING + part].start()

    def other_core(t, *which):
        for nm, X in ARR:
            b = nm + "d" + str(t)
            for w in which:
                if w == "far":
                    for part, z in zip(BOTH, "xy"):
                        arrived(ch(X, t, far, e, part), rid(b + z))
                else:
                    arrived(ch(X, t, {"c": c, "L": L, "R": R}[w], e), rid(b + w))

    def hop(tag, row, device, *positions):
        out = []
        for pos in positions:
            out.append(Send(lambda j, pos=pos: (w1_dst(j, row, pos), w1_dst(j, row, pos), rid(tag) + low(pos) * TWO + j, device), TWO))
        return out

    f1v = hop("f1v", u, dev(v, d), pos_v, pos_r)
    f1u = hop("f1u", v, dev(u, d), pos_r, pos_v)
    q0, q1 = pl.ds(0, BN), pl.ds(BN, DM - BN)
    f2u = same(W2.at[blk(pos_v, FB), q0], rid("f2u"), dev(u, d))
    f2v = same(W2.at[blk(pos_u, FB), q1], rid("f2v"), dev(v, d))

    def w1_in(tag, row, pos):
        for dd in BOTH:
            arrived(w1_dst(dd, row, pos), rid("w1" + tag) + dd * RING + pos)

    def w1_rest(pos, tag):
        arrived(w1_dst(e, r, pos), rid("w1d") + pos)
        for j in BOTH:
            arrived(w1_dst(j, q, pos), rid(tag) + low(pos) * TWO + j)

    for pos in (pos_r, pos_v):
        w1_in("u", u, pos)
    for t in f1v:
        t.all()
    send_w2("v", v)
    send_w1("v", v, pos_q, pos_u)
    pass_on("G", G, 0)
    for pos in (pos_r, pos_v):
        w1_in("v", v, pos)
    for t in f1u:
        t.all()
    other_core(0, "c")
    arrived(w2_part(pos_r, e), rid("w2d"))
    w1_rest(pos_r, "f1v")

    RC = min(8 * RING, TH)

    def cd_block(a, gr, w1b, w2b, bias, cbuf, gbuf, h_out, dc_out, db, count_db):
        cbuf[:] = jnp.dot(a, w1b, preferred_element_type=F32)
        gbuf[:] = lax.dot_general(gr, w2b, NT, preferred_element_type=F32)

        def rows(m, acc):
            sl = blk(m, RC)
            pre = cbuf[sl, :] + bias
            sq = pre * pre
            th = jnp.tanh(GELU_K * (pre + GELU_C * pre * sq))
            half = 0.5 * (1.0 + th)
            slope = half + 0.5 * pre * (1.0 - th * th) * GELU_K * (1.0 + 3.0 * GELU_C * sq)
            dc = gbuf[sl, :] * slope
            h_out[sl, :] = (pre * half).astype(BF16)
            dc_out[sl, :] = dc.astype(BF16)
            return acc + jnp.sum(dc.reshape(RC // 8, 8, FB), axis=0)

        acc = lax.fori_loop(0, T2 // RC, rows, jnp.zeros((8, FB), F32))

        @when(count_db)
        def _():
            db[:] += acc

    def hidden(n, place, block, need, first, posts, late):
        def body(ab, gb, w1b, w2b, cbuf, gbuf, hb, cb, dbs, isem, osem, wsem):
            def weights(b):
                pos = block(b * first)[1]
                return batch(wsem.at[b], (W1.at[:, blk(pos, FB)], w1b.at[b]), (W2.at[blk(pos, FB), :], w2b.at[b]))

            def load(b):
                need(b)
                start(weights(b))

            load(0)
            dbs[:] = jnp.zeros_like(dbs)

            def ins(k, s):
                row, col, _ = place(k)
                return (A.at[row, col], ab.at[s]), (G.at[row, col], gb.at[s])

            def outs(k, s):
                row, col, _ = place(k)
                to_p, cols = block(k)[TWO:]
                at = (high(col), low(col), slice(None), cols)
                H, C = (o["HP"].at[row], o["CP"].at[row]) if to_p else (o["HQ"], o["CQ"])
                return (hb.at[s], H.at[at]), (cb.at[s], C.at[at])

            def work(k, s):
                b, pos = block(k)[:TWO]
                for t in BOTH:
                    @when(k == t * first)
                    def _():
                        wait(weights(t))
                cd_block(ab[s], gb[s], w1b[b], w2b[b], bup[:, blk(pos, FB)], cbuf, gbuf, hb.at[s], cb.at[s], dbs.at[b], place(k)[TWO])

            run(n, ins, outs, isem, osem, work, posts={k: functools.partial(fn, load) for k, fn in posts.items()}, late=late)
            move(batch(wsem.at[0], *[(dbs.at[b], o["DB"].at[:, blk(block(b * first)[1], FB)]) for b in BOTH]))

        pl.run_scoped(body, bf(TWO, T2, DM), bf(TWO, T2, DM), bf(TWO, DM, FB), bf(TWO, FB, DM), fl(T2, FB), fl(T2, FB),
                      bf(TWO, T2, FB), bf(TWO, T2, FB), fl(TWO, 8, FB), dma(TWO, TWO), dma(TWO, TWO), dma(TWO, TWO))

    five, ten = RING + 1, TWO * RING + TWO

    def place1(k):
        early = k < ten
        k5, k2 = k % five, high(k - ten) + 1
        mine = jnp.logical_and(early, k5 < RING)
        m = jnp.where(early, k5 % RING, k2)
        return jnp.where(mine, hp, flip(hp)), (c + m + high(m) * (five - TWO * m)) % RING, mine

    def block1(k):
        b = jnp.where(k < ten, k // five % TWO, low(k))
        ii = jnp.where(b == 0, hi, hn)
        return b, TWO * g + ii, True, blk(ii, FB)

    def need1(b):
        if b:
            wait_w2("v", pos_v)
            f2u.start()
            w1_rest(pos_v, "f1v")

    def post0(load):
        pass_on("A", A, 0)
        from_u("G", G)
        other_core(0, "L", "R")

    def post2(load):
        far_in("G", G, 0)
        from_u("A", A)
        far_in("A", A, 0)
        other_core(0, "far")

    def post9(load):
        pass_on("A", A, 1)
        wait_w2("u", pos_u)
        f2v.start()
        other_core(1, "L", "R")

    def post13(load):
        far_in("G", G, 1)
        far_in("A", A, 1)
        other_core(1, "far")

    posts1 = {0: post0, TWO: post2, RING - 1: lambda load: other_core(1, "c"), RING: lambda load: load(1),
              five: lambda load: pass_on("G", G, 1), ten - 1: post9, ten + RING - 1: post13}
    hidden(ten + RING + TWO, place1, block1, need1, five, posts1, (1, RING - 1, RING, ten, ten + RING))

    S1, R1, S2, R2, K1, K2, OUT1, OUT2 = [o[t] for t in ("S1", "R1", "S2", "R2", "K1", "K2", "OUT1", "OUT2")]
    s1 = Send(lambda j: (S1.at[j], R1.at[j], rid("s1") + j, dev(v, d)), RING)
    s2 = Send(lambda j: (S2.at[:, blk(j, BN)], R2.at[:, blk(j, BN)], rid("s2") + j, dev(v, d)), RING)

    def dw1_cols(k, pair, first):
        j = first + (1 - TWO * first) * high(k)
        return blk(low(k) * RING + TWO * pair + j, DS)

    def grad(left, right, left_shape, right_shape, resident, out_shape, outs, done, recv=None):
        rows, width = out_shape

        def body(lb, rb, acc, ob, nb, isem, osem, wsem):
            stay = batch(wsem, resident((lb, rb)))
            start(stay)

            def ins(k, s):
                return (left(k), lb.at[s]) if right is None else (right(k), rb.at[s]),

            def work(k, s):
                @when(k == 0)
                def _():
                    wait(stay)
                x, y = (lb[s], rb[:]) if right is None else (lb[:], rb[s])
                val = lax.dot_general(x.reshape(ALLT, rows), y.reshape(ALLT, width), TN, preferred_element_type=F32)
                if recv is None:
                    ob[s] = val
                else:
                    acc[:] = val
                    ref, rsid = recv(k)
                    arrived(ref, rsid)
                    move(batch(wsem, (ref, nb)))
                    ob[s] = (acc[:] + nb[:]).astype(BF16)

            run(RING, ins, lambda k, s: ((ob.at[s], outs(k)),), isem, osem, work, done=lambda k, s: done(k, ob.at[s], wsem))

        extra = out_shape if recv else (8, BN)
        pl.run_scoped(body, bf(*left_shape), bf(*right_shape), fl(*extra), pltpu.VMEM(SLOTS + out_shape, BF16 if recv else F32), fl(*extra),
                      dma(TWO, 1), dma(TWO, 1), dma(TWO))

    PT, PTS = (TWO, RING, T2), (TWO, TWO, TWO, T2)

    def grad1(pair, first, outs, done, recv=None):
        grad(lambda k: A.at[:, :, :, dw1_cols(k, pair, first)], None, SLOTS + PT + (DS,), PTS + (F2,), lambda b: (o["CP"], b[1]),
             (DS, F2), outs, done, recv)

    def grad2(pair, outs, done, recv=None):
        grad(None, lambda k: G.at[:, :, :, blk(k, BN)], PTS + (FB,), SLOTS + PT + (BN,), lambda b: (o["HP"].at[:, :, :, :, blk(pair, FB)], b[0]),
             (FB, BN), outs, done, recv)

    grad1(hn, hp, lambda k: S1.at[k], lambda k, ob, sem: s1.start(k))

    def block2(k):
        b = k // RING
        ii = jnp.where(b == 0, hi, hn)
        return b, TWO * gn + ii, False, blk(ii, FB)

    def need2(b):
        pos = pos_q if b else pos_u
        w1_in("u", u, pos)
        w1_in("v", v, pos)
        w1_rest(pos, "f1u")
        if b:
            arrived(W2.at[blk(pos_q, FB), q1], rid("f2v"))
            arrived(W2.at[blk(pos_q, FB), q0], rid("f2u"))

    hidden(TWO * RING, lambda k: (hp, k % RING, k >= 0), block2, need2, RING, {TWO: lambda load: load(1)}, ())

    LAG = 2

    def region(s, nt, XP, XQ, PX, RX):
        Q1, Q2, RF, RR = [o[s + t] for t in ("Q1", "Q2", "RF", "RX")]
        ex = Send(lambda j: (PX.at[:, :, :, blk(j, BN)], RX.at[:, :, :, blk(j, BN)], rid(s + "p") + j, dev_e), RING)
        away = flip(c_hi)
        far_r = Send(lambda j: (Q1.at[away, blk(0, HT), blk(j, BN)], RF.at[away, :, blk(j, BN)], rid(s + "r") + j, dev_R), RING)
        far_l = Send(lambda j: (Q1.at[away, blk(1, HT), blk(j, BN)], RF.at[away, :, blk(j, BN)], rid(s + "l") + j, dev_L), RING)
        pm_r = Send(lambda j: (Q2.at[high(R), :, blk(j, BN)], RR.at[0, :, blk(j, BN)], rid(s + "pr") + j, dev_R), RING)
        pm_l = Send(lambda j: (Q2.at[high(L), :, blk(j, BN)], RR.at[1, :, blk(j, BN)], rid(s + "pl") + j, dev_L), RING)
        wshape = (BN, FC) if nt else (FC, BN)
        mine, other = blk(d, TH), blk(e, TH)

        def wsrc(j):
            return W1.at[blk(j, BN), :] if nt else W2.at[:, blk(j, BN)]

        def wdot(p_ref, q_ref, wref, shape):
            total = 0.0
            for ref, half in ((p_ref, g), (q_ref, gn)):
                x, sel = ref[:].reshape(-1, F2), blk(half, F2)
                if nt:
                    total += lax.dot_general(x, wref[:, sel], NT, preferred_element_type=F32)
                else:
                    total += jnp.dot(x, wref[sel, :], preferred_element_type=F32)
            return total.reshape(shape)

        def first(lop, loq, lfp, lfq, wb, ob, ab, qb, wsem, lsem, osem):
            lds = batch(lsem, (XP.at[hp, :, :, other], lop), (XQ.at[:, :, other], loq), (XP.at[hp, :, c_lo, mine], lfp), (XQ.at[:, c_lo, mine], lfq))

            def wcp(j):
                return batch(wsem.at[j % RING], (wsrc(j), wb.at[j % RING]))

            start(wcp(0) + lds)
            wait(lds)

            def step(j, _):
                o1 = batch(osem, (ob, PX.at[:, :, :, blk(j, BN)]))

                @when(j < RING)
                def _():
                    wait(wcp(j))

                    @when(j < RING - 1)
                    def _():
                        start(wcp(j + 1))
                    ob[:] = wdot(lop, loq, wb.at[j % RING], (TWO, TWO, TH, BN))
                    start(o1)

                @when(j >= LAG)
                def _():
                    k = j - LAG
                    arrived(RX.at[:, :, :, blk(k, BN)], rid(s + "p") + k)
                    add = batch(lsem, (RX.at[:, c_lo, :, blk(k, BN)], ab))
                    start(add)
                    qb[:] = wdot(lfp, lfq, wb.at[k % RING], (TWO, TH, BN))
                    wait(add)
                    qb[:] += ab[:]

                @when(j < RING)
                def _():
                    wait(o1)
                    ex.start(j)

                @when(j >= LAG)
                def _():
                    k = j - LAG
                    move(batch(lsem, (qb, Q1.at[:, :, blk(k, BN)])))
                    far_r.start(k)
                    far_l.start(k)
                return 0

            lax.fori_loop(0, RING + LAG, step, 0)

        def second(lp, lq, wb, ab, fb, ob, lsem, isem, osem):
            lds = batch(lsem, (XP.at[hp, :, flip(c_lo), mine], lp), (XQ.at[:, flip(c_lo), mine], lq))
            start(lds)

            def need(k):
                arrived(RF.at[high(R), :, blk(k, BN)], rid(s + "r") + k)
                arrived(RF.at[high(L), :, blk(k, BN)], rid(s + "l") + k)

            for k in range(RING):
                need(k)
            wait(lds)

            def ins(k, sl):
                return (wsrc(k), wb.at[sl]), (RX.at[:, flip(c_lo), :, blk(k, BN)], ab.at[sl]), (RF.at[:, :, blk(k, BN)], fb.at[sl])

            def work(k, sl):
                ob[sl] = wdot(lp, lq, wb.at[sl], (TWO, TH, BN)) + ab[sl]
                for col, part in ((R, 0), (L, 1)):
                    ob[sl, high(col), part * HT:(part + 1) * HT, :] += fb[sl, high(col)]

            def done(k, sl):
                pm_r.start(k)
                pm_l.start(k)

            run(RING, ins, lambda k, sl: ((ob.at[sl], Q2.at[:, :, blk(k, BN)]),), isem, osem, work, done=done)

        def run_first():
            pl.run_scoped(first, bf(TWO, TWO, TH, F2), bf(TWO, TWO, TH, F2), bf(TWO, TH, F2), bf(TWO, TH, F2), bf(RING, *wshape),
                          fl(TWO, TWO, TH, BN), fl(TWO, TH, BN), fl(TWO, TH, BN), dma(RING, 1), dma(RING), dma(1))

        def run_second():
            pl.run_scoped(second, bf(TWO, TH, F2), bf(TWO, TH, F2), bf(TWO, *wshape), fl(TWO, TWO, TH, BN), fl(TWO, TWO, HT, BN),
                          fl(TWO, TWO, TH, BN), dma(TWO), dma(TWO, RING), dma(TWO, 1))

        def come(j):
            arrived(RR.at[0, :, blk(j, BN)], rid(s + "pr") + j)
            arrived(RR.at[1, :, blk(j, BN)], rid(s + "pl") + j)
        return run_first, run_second, come

    y1, y2, y_come = region("Y", False, o["HP"], o["HQ"], o["PY"], o["RY"])
    d1, d2, d_come = region("D", True, o["CP"], o["CQ"], o["PD"], o["RD"])
    d1()
    y1()
    d2()
    grad2(hn, lambda k: S2.at[:, blk(k, BN)], lambda k, ob, sem: s2.start(k))
    y2()

    def piece(ii):
        return slice(ii * FB, (ii + 1) * FB)

    k1u = [Send(lambda m, ii=ii: (K1.at[m, :, piece(ii)], OUT1.at[:, f_block(TWO * g + ii, d)], rid("k1u") + d * TWO + ii, dev(u, m)), TWO)
           for ii in BOTH]
    k1d = [Send(lambda m, ii=ii: (K1.at[TWO + e, :, piece(ii)], OUT1.at[:, f_block(TWO * g + ii, d)], rid("k1d") + ii, dev_e)) for ii in BOTH]

    def done1(k, ob, sem):
        @when(k < TWO)
        def _():
            for t in k1u:
                t.start(k)

        @when(k == TWO + e)
        def _():
            for t in k1d:
                t.start()

        @when(k == TWO + d)
        def _():
            move(batch(sem, *[(ob.at[:, piece(ii)], OUT1.at[:, f_block(TWO * g + ii, d)]) for ii in BOTH]))

    def out2_at(core, jj):
        return OUT2.at[blk(core, FB), blk(jj, BN)]

    k2 = Send(lambda jj: (K2.at[TWO * e + jj], out2_at(d, jj), rid("k2") + jj, dev_e), TWO)

    def done2(k, ob, sem):
        @when(high(k) == d)
        def _():
            move(batch(sem, (ob, out2_at(d, low(k)))))

        @when(high(k) == e)
        def _():
            k2.start(low(k))

    grad1(hi, flip(hp), lambda k: K1.at[k], done1, lambda k: (R1.at[k], rid("s1") + k))

    RX_, OUTX, XO, OUTY, YO, BG, SO = [o[t] for t in ("DRX", "OUTX", "XO", "OUTY", "YO", "BG", "SO")]
    xo = Send(lambda j: (XO, OUTX.at[blk(d, TH), :], rid("xo"), dev_e))
    stages = [dev_e, dev(u, d), dev(v, d), {"col": c + 1 - TWO * c_lo}, {"col": RING - 1 - c}]
    assert len(stages) == STAGES
    sum_send = [Send(lambda j, k=k, dv=dv: (sums.at[k], sums_in.at[k], rid("sum") + k, dv))
                for k, dv in enumerate(stages)]
    bsend = [Send(lambda j, k=k, dv=dv: (db.at[k], db_in.at[k], rid("bf") + k, dv)) for k, dv in enumerate((dev(u, d), dev(v, d)))]
    bg = Send(lambda j: (BG.at[d], BG.at[d], rid("bg"), dev_e))

    def finish_dx(q1b, rlb, rrb, xb, gb, vb, xob, acc, dbb, isem, osem, wsem):
        RB = min(8 * RING, high(TH))
        par_ = batch(wsem, (PV, vb), (o["DB"], dbb))
        start(par_)
        for j in range(RING):
            d_come(j)
        acc[:] = jnp.zeros_like(acc)

        def ins(k, s):
            rows = blk(k, RB)
            return ((o["DQ1"].at[c_hi, rows], q1b.at[s]), (RX_.at[0, rows], rlb.at[s]), (RX_.at[1, rows], rrb.at[s]), (XF.at[rows, :], xb.at[s]),
                    (G.at[hp, c, pl.ds(pl.multiple_of(d * TH + k * RB, RB), RB), :], gb.at[s]))

        def outs(k, s):
            return ((xob.at[s, :, blk(d, DH)], OUTX.at[pl.ds(pl.multiple_of(d * TH + k * RB, RB), RB), :]),
                    (xob.at[s, :, blk(e, DH)], XO.at[blk(k, RB), :]))

        def fold(x):
            return jnp.sum(x.reshape(RB // 8, 8, DM), axis=0)

        def work(k, s):
            @when(k == 0)
            def _():
                wait(par_)
            da = q1b[s] + rlb[s] + rrb[s]
            inv_std, xhat = stats(xb[s].astype(F32))
            gr = gb[s].astype(F32)
            val = da * vb[0:1, :]
            m1 = jnp.sum(val, axis=1, keepdims=True) / DM
            m2 = jnp.sum(val * xhat, axis=1, keepdims=True) / DM
            xob[s] = (gr + inv_std * (val - m1 - xhat * m2)).astype(BF16)
            for i, t in enumerate((da * xhat, da, gr)):
                acc[i] += fold(t)

        run(TH // RB, ins, outs, isem, osem, work)
        xo.start()
        for i in range(RING - 1):
            row = jnp.sum(acc[i], axis=0, keepdims=True)
            acc[i, 0:1, :] = row
        for i in range(RING - 1):
            sums[STAGES, i:i + 1, :] = acc[i, 0:1, blk(d, DH)]
            sums[0, i:i + 1, :] = acc[i, 0:1, blk(e, DH)]
        db[0, 0:1, :] = jnp.sum(dbb[:], axis=0, keepdims=True)
        cur = sums[STAGES]
        cur_b = db[0]
        for k in range(STAGES):
            if k:
                sums[k] = cur
            sum_send[k].start()
            if k in (1, TWO):
                db[k - 1] = cur_b
                bsend[k - 1].start()
            arrived(sums_in.at[k], rid("sum") + k)
            cur = cur + sums_in[k]
            if k in (1, TWO):
                arrived(db_in.at[k - 1], rid("bf") + k - 1)
                cur_b = cur_b + db_in[k - 1]
        sums[STAGES] = cur
        db[TWO] = cur_b
        move(batch(wsem, (sums.at[STAGES], SO), (db.at[TWO], BG.at[d])))
        bg.start()

    def dx_all():
        RB = min(8 * RING, high(TH))
        pl.run_scoped(finish_dx, fl(TWO, RB, DM), fl(TWO, RB, DM), fl(TWO, RB, DM), bf(TWO, RB, DM), bf(TWO, RB, DM), fl(8, DM),
                      bf(TWO, RB, DM), fl(RING - 1, 8, DM), fl(8, FC), dma(TWO, RING + 1), dma(TWO, TWO), dma(TWO))

    dx_all()
    grad2(hi, lambda k: K2.at[k], done2, lambda k: (R2.at[:, blk(k, BN)], rid("s2") + k))

    def outy_at(core, jj):
        return OUTY.at[blk(core, TH), blk(jj, BN)]

    yo = Send(lambda jj: (YO.at[TWO * e + jj], outy_at(d, jj), rid("yo") + jj, dev_e), TWO)

    def finish_y(q1b, xb, vb, rxb, yb, isem, osem, wsem):
        def ins(k, s):
            cols = blk(k, BN)
            return (o["YQ1"].at[c_hi, :, cols], q1b.at[s]), (XF.at[:, cols], xb.at[s]), (PV.at[:, cols], vb.at[s])

        def work(k, s):
            arr = batch(wsem, (o["YRX"].at[:, :, blk(k, BN)], rxb))
            for j in range(RING):
                @when(k == j)
                def _():
                    y_come(j)
            move(arr)
            yb[s] = (xb[s].astype(F32) + (q1b[s] + rxb[0] + rxb[1]) + vb[s, TWO:TWO + 1, :]).astype(BF16)

        def done(k, s):
            @when(high(k) == d)
            def _():
                move(batch(wsem, (yb.at[s], outy_at(d, low(k)))))

            @when(high(k) == e)
            def _():
                yo.start(low(k))

        run(RING, ins, lambda k, s: ((yb.at[s], YO.at[k]),), isem, osem, work, done=done)

    pl.run_scoped(finish_y, fl(TWO, TH, BN), bf(TWO, TH, BN), fl(TWO, 8, BN), fl(TWO, TH, BN), bf(TWO, TH, BN), dma(TWO, RING), dma(TWO, 1), dma(1))

    arrived(OUTX.at[blk(e, TH), :], rid("xo"))
    arrived(BG.at[e], rid("bg"))
    for ii in BOTH:
        arrived(outy_at(e, ii), rid("yo") + ii)
        for dd in BOTH:
            arrived(OUT1.at[:, f_block(TWO * gn + ii, dd)], rid("k1u") + dd * TWO + ii)
        arrived(OUT1.at[:, f_block(TWO * g + ii, e)], rid("k1d") + ii)
        arrived(out2_at(e, ii), rid("k2") + ii)
    for t in pending:
        for j in range(t.n):
            t.desc(j).wait_send()
    assert tuple(counts) == SEMS, counts


SEMS = (143, 143)


def solution(mesh):
    nr, nc, nd = mesh.shape["row"], mesh.shape["col"], mesh.shape["dep"]
    assert nr == 4 and nc == 4 and nd == 2
    tok_spec = P(("part", "row", "col"), "dep")
    vec_dep = P("dep")
    part_dep = P(("part", "dep"))
    in_specs = (tok_spec, vec_dep, vec_dep, P(("dep", "row"), "col"), P("col"), P(("col", "row"), "dep"), vec_dep, tok_spec)
    out_specs = (tok_spec, tok_spec, P(("part", "dep", "row"), "col"), P(("part", "col")), P(("part", "col", "row"), "dep"), part_dep, part_dep, part_dep)

    def local_step(x_in, ln_scale, ln_shift, w_up, b_up, w_down, b_down, y_grad):
        d = lax.axis_index("dep")
        th, dhalf = x_in.shape[0] // 2, x_in.shape[1]
        ds_, fb = w_up.shape[0], w_up.shape[1] // 8
        vec = jnp.stack([ln_scale, ln_shift, b_down.astype(F32)] + [jnp.zeros_like(ln_scale)] * 5)
        b3 = lax.dynamic_index_in_dim(b_up.reshape(4, 2, fb), d, 1, keepdims=False).astype(F32)
        bup = jnp.concatenate([b3[k] for k in (0, 3, 1, 2)]).reshape(1, 4 * fb)

        cfg = (th, 2 * dhalf, ds_, fb)
        outs = pl.pallas_call(
            functools.partial(kernel, cfg),
            name="mlp_layer",
            out_shape=buffers(*cfg),
            in_specs=[pl.BlockSpec(memory_space=pl.ANY)] * 5 + [pl.BlockSpec(memory_space=pltpu.VMEM)],
            out_specs=[pl.BlockSpec(memory_space=pl.ANY)] * len(NAMES),
            scratch_shapes=[dma(SEMS[0]), dma(SEMS[1]), fl(STAGES + 1, 8, dhalf), fl(STAGES, 8, dhalf), fl(3, 8, 4 * fb), fl(2, 8, 4 * fb)],
            compiler_params=pltpu.CompilerParams(collective_id=0, has_side_effects=True, vmem_limit_bytes=62 * 1024 * 1024),
        )(x_in, y_grad, w_up, w_down, vec, bup)
        o = dict(zip(NAMES, outs))
        db = o["BG"][:, 0].reshape(2, 4, fb)
        b_up_grad = jnp.stack([db[:, k] for k in (0, 2, 3, 1)]).reshape(8 * fb)
        return (o["OUTY"], o["OUTX"], o["OUT1"], b_up_grad, o["OUT2"], o["SO"][2], o["SO"][0], o["SO"][1])

    return jax.shard_map(local_step, mesh=mesh, in_specs=in_specs, out_specs=out_specs, check_vma=False)
```

```python
import functools

import jax
import jax.numpy as jnp
from jax import lax
from jax.experimental import pallas as pl
from jax.experimental.pallas import tpu as pltpu
from jax.sharding import PartitionSpec as P

LN_EPS = 1e-5
GELU_K = 0.7978845608028654
GELU_C = 0.044715
F32 = jnp.float32
BF16 = jnp.bfloat16
MESH = pl.DeviceIdType.MESH

NAMES = ("A", "G", "W1", "W2", "HP", "HQ", "CP", "CQ", "DB",
         "PY", "RY", "YQ1", "YQ2", "YRF", "YRX", "PD", "RD", "DQ1", "DQ2", "DRF", "DRX",
         "S1", "R1", "S2", "R2", "K1", "K2", "OUT1", "OUT2", "XF", "GF", "PV", "YO", "XO", "OUTY", "OUTX", "BG", "SO")
TWO, RING, STAGES, MANY = 2, 4, 5, 16
BOTH, SLOTS = (0, 1), (2,)
NT = (((1,), (1,)), ((), ()))
TN = (((0,), (0,)), ((), ()))


def flip(x):
    return 1 - x


def low(x):
    return x % 2


def high(x):
    return x // 2


def buffers(TH, DM, DS, FB):
    F2, FC, T2 = 2 * FB, 4 * FB, 2 * TH
    pair = (TWO, TWO)
    shapes = {
        "A": ((TWO, RING, T2, DM), BF16), "W1": ((DM, FC), BF16), "W2": ((FC, DM), BF16),
        "HP": (SLOTS + pair + (T2, F2), BF16), "HQ": (pair + (T2, F2), BF16), "DB": ((8, FC), F32),
        "S1": ((RING, DS, F2), F32), "S2": ((FB, DM), F32),
        "K1": ((RING, DS, F2), BF16), "K2": ((RING, FB, high(DM) // TWO), BF16),
        "OUT1": ((DS, 8 * FB), BF16), "OUT2": ((F2, high(DM)), BF16),
        "XF": ((TH, DM), BF16), "GF": ((TH, DM), BF16), "PV": ((8, DM), F32), "YO": ((RING, TH, high(DM) // TWO), BF16),
        "XO": ((TH, high(DM)), BF16), "OUTY": ((T2, high(DM)), BF16), "OUTX": ((T2, high(DM)), BF16),
        "BG": (SLOTS + (8, FC), F32), "SO": ((8, high(DM)), F32),
    }
    for new, old in (("G", "A"), ("CP", "HP"), ("CQ", "HQ"), ("R1", "S1"), ("R2", "S2")):
        shapes[new] = shapes[old]
    for p, s in (("PY", "Y"), ("PD", "D")):
        shapes[p] = shapes["R" + s] = (pair + (TH, DM), F32)
        for q in ("Q1", "Q2", "RX"):
            shapes[s + q] = (SLOTS + (TH, DM), F32)
        shapes[s + "RF"] = (SLOTS + (high(TH), DM), F32)
    return [jax.ShapeDtypeStruct(*shapes[n]) for n in NAMES]


def mul(x, n):
    return x * n if isinstance(x, int) else pl.multiple_of(x * n, n)


def cp(src, dst, sem):
    return pltpu.make_async_copy(src, dst, sem)


def parts(src, dst):
    rows = dst.shape[0]
    n = rows if rows == TWO and len(dst.shape) > RING - 1 else RING if rows % (8 * RING) == 0 else 1
    m = rows // n
    return [(src.at[pl.ds(i * m, m)], dst.at[pl.ds(i * m, m)]) for i in range(n)] if n > 1 else [(src, dst)]


def batch(sem, *pairs):
    return [cp(src, dst, sem.at[i]) for i, (src, dst) in enumerate(t for pair in pairs for t in parts(*pair))]


def start(copies):
    for t in copies:
        t.start()


def wait(copies):
    for t in copies:
        t.wait()


def move(copies):
    start(copies)
    wait(copies)


def dma(*shape):
    return pltpu.SemaphoreType.DMA(shape)


def bf(*shape):
    return pltpu.VMEM(shape, BF16)


def fl(*shape):
    return pltpu.VMEM(shape, F32)


def when(cond):
    def deco(fn):
        pl.when(cond)(fn)
    return deco


def run(n, ins, outs, isem, osem, work, done=None, posts=None, late=()):
    posts = posts or {}

    def fetch(k, s):
        return batch(isem.at[s], *ins(k, s))

    def back(k, s):
        return batch(osem.at[s], *outs(k, s))

    start(fetch(0, 0))

    def step(k, _):
        s, nxt = low(k), k + 1
        is_late = functools.reduce(jnp.logical_or, [nxt == t for t in late], False)
        more = nxt < n
        wait(fetch(k, s))

        @when(jnp.logical_and(more, jnp.logical_not(is_late)))
        def _():
            start(fetch(nxt, flip(s)))
        if done is None:
            @when(k >= TWO)
            def _():
                wait(back(k, s))
        work(k, s)
        start(back(k, s))
        for t, fn in posts.items():
            when(k == t)(fn)
        if late:
            @when(is_late)
            def _():
                start(fetch(nxt, flip(s)))
        if done is not None:
            @when(k == 0)
            def _():
                wait(back(k, s))
                done(k, s)

            @when(k >= TWO)
            def _():
                wait(back(k - 1, flip(s)))
                done(k - 1, flip(s))
        return 0

    lax.fori_loop(0, n, step, 0)
    last = n - 1
    if done is None:
        wait(back(last - 1, flip(low(last))))
    wait(back(last, low(last)))
    if done is not None:
        done(last, low(last))


def kernel(cfg, x_in, g_in, w1, w2, vec, bup, *refs):
    TH, DM, DS, FB = cfg
    o = dict(zip(NAMES, refs[:len(NAMES)]))
    ssem, rsem, sums, sums_in, db, db_in = refs[len(NAMES):]
    DH, F2, FC, HT, T2 = high(DM), TWO * FB, RING * FB, high(TH), TWO * TH
    BN, ALLT = high(DH), TWO * RING * T2
    A, G, W1, W2 = o["A"], o["G"], o["W1"], o["W2"]
    r, c, d = lax.axis_index("row"), lax.axis_index("col"), lax.axis_index("dep")
    hp, hi = low(r), high(r)
    hn, e = flip(hi), flip(d)
    g = low(r + hi)
    gn = flip(g)
    u, v, q = r + 1 - TWO * hp, RING - 1 - r, (r + TWO) % RING
    R, L, far = (c + 1) % RING, (c + RING - 1) % RING, (c + TWO) % RING
    pos_r, pos_v, pos_u, pos_q = TWO * g + hi, TWO * g + hn, TWO * gn + hi, TWO * gn + hn
    c_lo, c_hi = low(c), high(c)

    ids, counts = {}, [0, 0]

    def name(key, n=1):
        ids[key] = counts[0]
        counts[0] += n

    def rid(key):
        return ids[key]

    for nm in "AG":
        for w in ("xr1", "xl1", "fr0", "fl0", "fr1", "fl1"):
            name(nm + w)
        for w in ("xr0", "xl0", "u"):
            name(nm + w, TWO)
        for t in "01":
            for w in "cLRxy":
                name(nm + "d" + t + w, TWO)
    for s in "uv":
        name("w1" + s, TWO * RING)
        name("w2" + s, TWO)
        name("f1" + s, RING)
        name("f2" + s)
    for s in ("w2d", "xf", "gf", "pv", "xo", "bg"):
        name(s)
    name("yo", TWO)
    name("bf", TWO)
    name("sum", STAGES)
    for s in ("w1d", "s1", "s2", "k1u"):
        name(s, RING)
    name("k1d", TWO)
    name("k2", TWO)
    for s in "YD":
        for w in ("p", "r", "l", "pr", "pl"):
            name(s + w, RING)

    pending = []
    dev_e, dev_R, dev_L = {"dep": e}, {"col": R}, {"col": L}

    def dev(row, core):
        return {"row": row, "dep": core}

    class Send:
        def __init__(self, fn, n=1):
            self.fn, self.n, self.sid = fn, n, counts[1]
            counts[1] += n
            pending.append(self)

        def desc(self, j=0):
            src, dst, rsid, device = self.fn(j)
            return pltpu.make_async_remote_copy(src_ref=src, dst_ref=dst, send_sem=ssem.at[self.sid + j], recv_sem=rsem.at[rsid],
                                                device_id=device, device_id_type=MESH)

        def start(self, j=0):
            self.desc(j).start()

        def all(self):
            for j in range(self.n):
                self.start(j)

    def same(ref, rsid, device):
        return Send(lambda j: (ref, ref, rsid, device))

    def arrived(dst, rsid):
        pltpu.make_async_remote_copy(src_ref=dst, dst_ref=dst, send_sem=ssem.at[0], recv_sem=rsem.at[rsid],
                                     device_id=dev_e, device_id_type=MESH).wait_recv()

    barrier = pltpu.get_barrier_semaphore()
    peers = [dev_e, dev_R, dev_L] + [dev(t, k) for t in (u, v) for k in BOTH]
    for p in peers:
        pl.semaphore_signal(barrier, inc=1, device_id=p, device_id_type=MESH)
    pl.semaphore_wait(barrier, len(peers))

    ARR = (("A", A), ("G", G))
    ROW = (hp, flip(hp))

    def ch(X, t, col, core, part=None):
        if part is None:
            return X.at[ROW[t], col, pl.ds(mul(core, TH), TH)]
        return X.at[ROW[t], col, pl.ds(pl.multiple_of(core * TH + part * HT, HT), HT)]

    def blk(k, n):
        return pl.ds(mul(k, n), n)

    def f_block(pos, core):
        gg, ii = high(pos), low(pos)
        return blk((flip(gg) * (RING - 1) * ii + gg * (1 + ii)) * TWO + core, FB)

    def w1_src(pos, core):
        return w1.at[:, f_block(pos, core)]

    def w1_dst(dd, row, pos):
        return W1.at[blk(dd * RING + row, DS), blk(pos, FB)]

    def send_w1(tag, row, *positions):
        for pos in positions:
            for core in BOTH:
                Send(lambda j, pos=pos, core=core: (w1_src(pos, core), w1_dst(d, r, pos), rid("w1" + tag) + d * RING + pos, dev(row, core))).start()

    def w2_part(pos, half):
        return W2.at[blk(pos, FB), blk(half, DH)]

    def send_w2(tag, row):
        for core in BOTH:
            Send(lambda j, core=core: (w2.at[blk(core, FB), :], w2_part(pos_r, d), rid("w2" + tag) + d, dev(row, core))).start()

    def wait_w2(tag, pos):
        for dd in BOTH:
            arrived(w2_part(pos, dd), rid("w2" + tag) + dd)

    XF, GF, PV = o["XF"], o["GF"], o["PV"]
    Send(lambda j: (g_in.at[blk(e, TH), :], GF.at[:, blk(d, DH)], rid("gf"), dev_e)).start()
    Send(lambda j: (x_in.at[blk(e, TH), :], XF.at[:, blk(d, DH)], rid("xf"), dev_e)).start()
    Send(lambda j: (vec, PV.at[:, blk(d, DH)], rid("pv"), dev_e)).start()
    OWN_TO = (("xr0", dev_R), ("xl0", dev_L), ("u", dev(u, d)), ("d0c", dev_e))
    send_w1("v", v, pos_v, pos_r)
    send_w1("u", u, pos_u, pos_q)
    for w, dv in OWN_TO:
        Send(lambda j, w=w, dv=dv: (g_in.at[blk(d, TH), :], G.at[hp, c, blk(d, TH), blk(d, DH)], rid("G" + w), dv)).start()

    RL = min(8 * RING, TH)

    def stats(x):
        mean = jnp.sum(x, axis=1, keepdims=True) / DM
        var = jnp.sum(x * x, axis=1, keepdims=True) / DM - mean * mean
        inv_std = lax.rsqrt(var + LN_EPS)
        return inv_std, (x - mean) * inv_std


    def own_part(xb, gb, ab, vb, b2, b3, sems, sems2):
        mine, other = blk(d, DH), blk(e, DH)
        ld = batch(sems, (g_in.at[blk(d, TH), :], gb.at[:, mine]), (x_in.at[blk(d, TH), :], xb.at[:, mine]), (vec, vb.at[:, mine]))
        start(ld)
        wait(ld)
        got = batch(sems, (GF.at[:, other], gb.at[:, other]), (XF.at[:, other], xb.at[:, other]), (PV.at[:, other], vb.at[:, other]))
        for ref, w in ((GF, "gf"), (XF, "xf"), (PV, "pv")):
            arrived(ref.at[:, other], rid(w))
            if ref is GF:
                for w, dv in OWN_TO:
                    Send(lambda j, w=w, dv=dv: (GF.at[:, blk(e, DH)], G.at[hp, c, blk(d, TH), blk(e, DH)], rid("G" + w) + 1, dv)).start()
        move(got)
        start(batch(sems2, (gb, ch(G, 0, c, d))))
        keep = batch(sems, (xb.at[:, mine], XF.at[:, mine]), (vb.at[:, mine], PV.at[:, mine]))
        start(keep)
        scale, shift = vb[0:1, :], vb[1:TWO, :]

        def rows(m, _):
            sl = blk(m, RL)
            ab[sl, :] = (stats(xb[sl, :].astype(F32))[1] * scale + shift).astype(BF16)
            return 0

        lax.fori_loop(0, TH // RL, rows, 0)
        wait(keep)
        move(batch(sems, (ab, ch(A, 0, c, d))))
        for w, dv in OWN_TO:
            Send(lambda j, w=w, dv=dv: (ch(A, 0, c, d), ch(A, 0, c, d), rid("A" + w), dv)).start()
        send_w2("u", u)
        send_w1("u", u, pos_r, pos_v)
        wait(batch(sems2, (gb, ch(G, 0, c, d))))
        wl = batch(sems, (w2.at[blk(d, FB), :], b3), (w1_src(0, d), b2.at[:, blk(0, FB)]))
        move(wl)
        move(batch(sems, *[(w1_src(pos, d), b2.at[:, blk(pos, FB)]) for pos in range(1, RING)]))
        move(batch(sems, (b3, w2_part(pos_r, d)), (b2, W1.at[blk(d * RING + r, DS), :])))

    pl.run_scoped(own_part, bf(TH, DM), bf(TH, DM), bf(TH, DM), fl(8, DM), bf(DS, FC), bf(FB, DH), dma(MANY), dma(MANY))
    for pos in range(RING):
        Send(lambda j, pos=pos: (w1_src(pos, e), w1_dst(d, r, pos), rid("w1d") + pos, dev_e)).start()
    Send(lambda j: (w2.at[blk(e, FB), :], w2_part(pos_r, d), rid("w2d"), dev_e)).start()

    fwd, par = {}, {}
    for nm, X in ARR:
        for t in BOTH:
            b = nm + "d" + str(t)
            fwd[nm, t] = [same(ch(X, t, L, d, 0), rid(nm + "fr" + str(t)), dev_R), same(ch(X, t, R, d, 1), rid(nm + "fl" + str(t)), dev_L),
                          same(ch(X, t, L, d), rid(b + "L"), dev_e), same(ch(X, t, R, d), rid(b + "R"), dev_e),
                          same(ch(X, t, far, d, 0), rid(b + "x"), dev_e), same(ch(X, t, far, d, 1), rid(b + "y"), dev_e)]
        par[nm] = [same(ch(X, 1, c, d), rid(nm + w), dv) for w, dv in (("xr1", dev_R), ("xl1", dev_L), ("d1c", dev_e))]

    def own_in(nm, X, t, col, w, core=d):
        if nm + w in ("Gxr0", "Gxl0", "Gu", "Gd0c"):
            for half, i in ((core, 0), (flip(core), 1)):
                arrived(X.at[ROW[t], col, blk(core, TH), blk(half, DH)], rid(nm + w) + i)
        else:
            arrived(ch(X, t, col, core), rid(nm + w))

    def pass_on(nm, X, t):
        to_r, to_l, d_l, d_r = fwd[nm, t][:RING]
        own_in(nm, X, t, L, "xr" + str(t))
        to_r.start()
        own_in(nm, X, t, R, "xl" + str(t))
        to_l.start()
        d_l.start()
        d_r.start()

    def from_u(nm, X):
        own_in(nm, X, 1, c, "u")
        for t in par[nm]:
            t.start()

    def far_in(nm, X, t):
        for part, w in zip(BOTH, ("fr", "fl")):
            arrived(ch(X, t, far, d, part), rid(nm + w + str(t)))
            fwd[nm, t][RING + part].start()

    def other_core(t, *which):
        for nm, X in ARR:
            b = nm + "d" + str(t)
            for w in which:
                if w == "far":
                    for part, z in zip(BOTH, "xy"):
                        arrived(ch(X, t, far, e, part), rid(b + z))
                else:
                    own_in(nm, X, t, {"c": c, "L": L, "R": R}[w], b[1:] + w, e)

    def hop(tag, row, device, *positions):
        out = []
        for pos in positions:
            out.append(Send(lambda j, pos=pos: (w1_dst(j, row, pos), w1_dst(j, row, pos), rid(tag) + low(pos) * TWO + j, device), TWO))
        return out

    f1v = hop("f1v", u, dev(v, d), pos_v, pos_r)
    f1u = hop("f1u", v, dev(u, d), pos_r, pos_v)
    q0, q1 = pl.ds(0, BN), pl.ds(BN, DM - BN)
    f2u = same(W2.at[blk(pos_v, FB), q0], rid("f2u"), dev(u, d))
    f2v = same(W2.at[blk(pos_u, FB), q1], rid("f2v"), dev(v, d))

    def w1_in(tag, row, pos):
        for dd in BOTH:
            arrived(w1_dst(dd, row, pos), rid("w1" + tag) + dd * RING + pos)

    def w1_rest(pos, tag):
        arrived(w1_dst(e, r, pos), rid("w1d") + pos)
        for j in BOTH:
            arrived(w1_dst(j, q, pos), rid(tag) + low(pos) * TWO + j)

    for pos in (pos_r, pos_v):
        w1_in("u", u, pos)
    for t in f1v:
        t.all()
    send_w2("v", v)
    send_w1("v", v, pos_q, pos_u)
    pass_on("G", G, 0)
    for pos in (pos_r, pos_v):
        w1_in("v", v, pos)
    for t in f1u:
        t.all()
    other_core(0, "c")
    arrived(w2_part(pos_r, e), rid("w2d"))
    w1_rest(pos_r, "f1v")

    RC = min(8 * RING, TH)

    def cd_block(a, gr, w1b, w2b, bias, cbuf, gbuf, h_out, dc_out, db, count_db):
        cbuf[:] = jnp.dot(a, w1b, preferred_element_type=F32)
        gbuf[:] = lax.dot_general(gr, w2b, NT, preferred_element_type=F32)

        def rows(m, acc):
            sl = blk(m, RC)
            pre = cbuf[sl, :] + bias
            sq = pre * pre
            th = jnp.tanh(GELU_K * (pre + GELU_C * pre * sq))
            half = 0.5 * (1.0 + th)
            slope = half + 0.5 * pre * (1.0 - th * th) * GELU_K * (1.0 + 3.0 * GELU_C * sq)
            dc = gbuf[sl, :] * slope
            h_out[sl, :] = (pre * half).astype(BF16)
            dc_out[sl, :] = dc.astype(BF16)
            return acc + jnp.sum(dc.reshape(RC // 8, 8, FB), axis=0)

        acc = lax.fori_loop(0, T2 // RC, rows, jnp.zeros((8, FB), F32))

        @when(count_db)
        def _():
            db[:] += acc

    def hidden(n, place, block, need, first, posts, late):
        def body(ab, gb, w1b, w2b, cbuf, gbuf, hb, cb, dbs, isem, osem, wsem):
            def weights(b):
                pos = block(b * first)[1]
                return batch(wsem.at[b], (W1.at[:, blk(pos, FB)], w1b.at[b]), (W2.at[blk(pos, FB), :], w2b.at[b]))

            def load(b):
                need(b)
                start(weights(b))

            load(0)
            dbs[:] = jnp.zeros_like(dbs)

            def ins(k, s):
                row, col, _ = place(k)
                return (A.at[row, col], ab.at[s]), (G.at[row, col], gb.at[s])

            def outs(k, s):
                row, col, _ = place(k)
                to_p, cols = block(k)[TWO:]
                at = (high(col), low(col), slice(None), cols)
                H, C = (o["HP"].at[row], o["CP"].at[row]) if to_p else (o["HQ"], o["CQ"])
                return (hb.at[s], H.at[at]), (cb.at[s], C.at[at])

            def work(k, s):
                b, pos = block(k)[:TWO]
                for t in BOTH:
                    @when(k == t * first)
                    def _():
                        wait(weights(t))
                cd_block(ab[s], gb[s], w1b[b], w2b[b], bup[:, blk(pos, FB)], cbuf, gbuf, hb.at[s], cb.at[s], dbs.at[b], place(k)[TWO])

            run(n, ins, outs, isem, osem, work, posts={k: functools.partial(fn, load) for k, fn in posts.items()}, late=late)
            move(batch(wsem.at[0], *[(dbs.at[b], o["DB"].at[:, blk(block(b * first)[1], FB)]) for b in BOTH]))

        pl.run_scoped(body, bf(TWO, T2, DM), bf(TWO, T2, DM), bf(TWO, DM, FB), bf(TWO, FB, DM), fl(T2, FB), fl(T2, FB),
                      bf(TWO, T2, FB), bf(TWO, T2, FB), fl(TWO, 8, FB), dma(TWO, MANY), dma(TWO, MANY), dma(TWO, MANY))

    five, ten = RING + 1, TWO * RING + TWO

    def place1(k):
        early = k < ten
        k5, k2 = k % five, high(k - ten) + 1
        mine = jnp.logical_and(early, k5 < RING)
        m = jnp.where(early, k5 % RING, k2)
        return jnp.where(mine, hp, flip(hp)), (c + m + high(m) * (five - TWO * m)) % RING, mine

    def block1(k):
        b = jnp.where(k < ten, k // five % TWO, low(k))
        ii = jnp.where(b == 0, hi, hn)
        return b, TWO * g + ii, True, blk(ii, FB)

    def need1(b):
        if b:
            wait_w2("v", pos_v)
            f2u.start()
            w1_rest(pos_v, "f1v")

    def post0(load):
        pass_on("A", A, 0)
        from_u("G", G)
        other_core(0, "L", "R")

    def post2(load):
        far_in("G", G, 0)
        from_u("A", A)
        far_in("A", A, 0)
        other_core(0, "far")

    def post9(load):
        pass_on("A", A, 1)
        wait_w2("u", pos_u)
        f2v.start()
        other_core(1, "L", "R")

    def post13(load):
        far_in("G", G, 1)
        far_in("A", A, 1)
        other_core(1, "far")

    posts1 = {0: post0, TWO: post2, RING - 1: lambda load: other_core(1, "c"), RING: lambda load: load(1),
              five: lambda load: pass_on("G", G, 1), ten - 1: post9, ten + RING - 1: post13}
    hidden(ten + RING + TWO, place1, block1, need1, five, posts1, (1, RING - 1, RING, ten, ten + RING))

    S1, R1, S2, R2, K1, K2, OUT1, OUT2 = [o[t] for t in ("S1", "R1", "S2", "R2", "K1", "K2", "OUT1", "OUT2")]
    s1 = Send(lambda j: (S1.at[j], R1.at[j], rid("s1") + j, dev(v, d)), RING)
    s2 = Send(lambda j: (S2.at[:, blk(j, BN)], R2.at[:, blk(j, BN)], rid("s2") + j, dev(v, d)), RING)

    def dw1_cols(k, pair, first):
        j = first + (1 - TWO * first) * high(k)
        return blk(low(k) * RING + TWO * pair + j, DS)

    def grad(left, right, left_shape, right_shape, resident, out_shape, outs, done, recv=None, posts=None):
        rows, width = out_shape

        def body(lb, rb, acc, ob, nb, isem, osem, wsem):
            stay = batch(wsem, resident((lb, rb)))
            start(stay)

            def ins(k, s):
                return (left(k), lb.at[s]) if right is None else (right(k), rb.at[s]),

            def work(k, s):
                @when(k == 0)
                def _():
                    wait(stay)
                x, y = (lb[s], rb[:]) if right is None else (lb[:], rb[s])
                val = lax.dot_general(x.reshape(ALLT, rows), y.reshape(ALLT, width), TN, preferred_element_type=F32)
                if recv is None:
                    ob[s] = val
                else:
                    acc[:] = val
                    ref, rsid = recv(k)
                    arrived(ref, rsid)
                    move(batch(wsem, (ref, nb)))
                    ob[s] = (acc[:] + nb[:]).astype(BF16)

            run(RING, ins, lambda k, s: ((ob.at[s], outs(k)),), isem, osem, work, done=lambda k, s: done(k, ob.at[s], wsem), posts=posts)

        extra = out_shape if recv else (8, BN)
        pl.run_scoped(body, bf(*left_shape), bf(*right_shape), fl(*extra), pltpu.VMEM(SLOTS + out_shape, BF16 if recv else F32), fl(*extra),
                      dma(TWO, MANY), dma(TWO, MANY), dma(MANY))

    PT, PTS = (TWO, RING, T2), (TWO, TWO, TWO, T2)

    def grad1(pair, first, outs, done, recv=None):
        grad(lambda k: A.at[:, :, :, dw1_cols(k, pair, first)], None, SLOTS + PT + (DS,), PTS + (F2,), lambda b: (o["CP"], b[1]),
             (DS, F2), outs, done, recv)

    def grad2(pair, outs, done, recv=None, posts=None):
        grad(None, lambda k: G.at[:, :, :, blk(k, BN)], PTS + (FB,), SLOTS + PT + (BN,), lambda b: (o["HP"].at[:, :, :, :, blk(pair, FB)], b[0]),
             (FB, BN), outs, done, recv, posts)

    grad1(hn, hp, lambda k: S1.at[k], lambda k, ob, sem: s1.start(k))

    def block2(k):
        b = k // RING
        ii = jnp.where(b == 0, hi, hn)
        return b, TWO * gn + ii, False, blk(ii, FB)

    def need2(b):
        pos = pos_q if b else pos_u
        w1_in("u", u, pos)
        w1_in("v", v, pos)
        w1_rest(pos, "f1u")
        if b:
            arrived(W2.at[blk(pos_q, FB), q1], rid("f2v"))
            arrived(W2.at[blk(pos_q, FB), q0], rid("f2u"))

    hidden(TWO * RING, lambda k: (hp, k % RING, k >= 0), block2, need2, RING, {TWO: lambda load: load(1)}, ())

    LAG = 2

    def region(s, nt, XP, XQ, PX, RX):
        Q1, Q2, RF, RR = [o[s + t] for t in ("Q1", "Q2", "RF", "RX")]
        ex = Send(lambda j: (PX.at[:, :, :, blk(j, BN)], RX.at[:, :, :, blk(j, BN)], rid(s + "p") + j, dev_e), RING)
        away = flip(c_hi)
        far_r = Send(lambda j: (Q1.at[away, blk(0, HT), blk(j, BN)], RF.at[away, :, blk(j, BN)], rid(s + "r") + j, dev_R), RING)
        far_l = Send(lambda j: (Q1.at[away, blk(1, HT), blk(j, BN)], RF.at[away, :, blk(j, BN)], rid(s + "l") + j, dev_L), RING)
        pm_r = Send(lambda j: (Q2.at[high(R), :, blk(j, BN)], RR.at[0, :, blk(j, BN)], rid(s + "pr") + j, dev_R), RING)
        pm_l = Send(lambda j: (Q2.at[high(L), :, blk(j, BN)], RR.at[1, :, blk(j, BN)], rid(s + "pl") + j, dev_L), RING)
        wshape = (BN, FC) if nt else (FC, BN)
        mine, other = blk(d, TH), blk(e, TH)

        def wsrc(j):
            return W1.at[blk(j, BN), :] if nt else W2.at[:, blk(j, BN)]

        def wdot(p_ref, q_ref, wref, shape):
            total = 0.0
            for ref, half in ((p_ref, g), (q_ref, gn)):
                x, sel = ref[:].reshape(-1, F2), blk(half, F2)
                if nt:
                    total += lax.dot_general(x, wref[:, sel], NT, preferred_element_type=F32)
                else:
                    total += jnp.dot(x, wref[sel, :], preferred_element_type=F32)
            return total.reshape(shape)

        def first(lop, loq, lfp, lfq, wb, ob, ab, qb, wsem, lsem, osem):
            lds = batch(lsem, (XP.at[hp, :, :, other], lop), (XQ.at[:, :, other], loq), (XP.at[hp, :, c_lo, mine], lfp), (XQ.at[:, c_lo, mine], lfq))

            def wcp(j):
                return batch(wsem.at[j % RING], (wsrc(j), wb.at[j % RING]))

            start(wcp(0) + lds)
            wait(lds)

            def step(j, _):
                o1 = batch(osem, (ob, PX.at[:, :, :, blk(j, BN)]))

                @when(j < RING)
                def _():
                    wait(wcp(j))

                    @when(j < RING - 1)
                    def _():
                        start(wcp(j + 1))
                    ob[:] = wdot(lop, loq, wb.at[j % RING], (TWO, TWO, TH, BN))
                    start(o1)

                @when(j >= LAG)
                def _():
                    k = j - LAG
                    arrived(RX.at[:, :, :, blk(k, BN)], rid(s + "p") + k)
                    add = batch(lsem, (RX.at[:, c_lo, :, blk(k, BN)], ab))
                    start(add)
                    qb[:] = wdot(lfp, lfq, wb.at[k % RING], (TWO, TH, BN))
                    wait(add)
                    qb[:] += ab[:]

                @when(j < RING)
                def _():
                    wait(o1)
                    ex.start(j)

                @when(j >= LAG)
                def _():
                    k = j - LAG
                    move(batch(lsem, (qb, Q1.at[:, :, blk(k, BN)])))
                    far_r.start(k)
                    far_l.start(k)
                return 0

            lax.fori_loop(0, RING + LAG, step, 0)

        def second(lp, lq, wb, ab, fb, ob, lsem, isem, osem):
            lds = batch(lsem, (XP.at[hp, :, flip(c_lo), mine], lp), (XQ.at[:, flip(c_lo), mine], lq))
            start(lds)

            def need(k):
                arrived(RF.at[high(R), :, blk(k, BN)], rid(s + "r") + k)
                arrived(RF.at[high(L), :, blk(k, BN)], rid(s + "l") + k)

            for k in range(RING):
                need(k)
            wait(lds)

            def ins(k, sl):
                return (wsrc(k), wb.at[sl]), (RX.at[:, flip(c_lo), :, blk(k, BN)], ab.at[sl]), (RF.at[:, :, blk(k, BN)], fb.at[sl])

            def work(k, sl):
                ob[sl] = wdot(lp, lq, wb.at[sl], (TWO, TH, BN)) + ab[sl]
                for col, part in ((R, 0), (L, 1)):
                    ob[sl, high(col), part * HT:(part + 1) * HT, :] += fb[sl, high(col)]

            def done(k, sl):
                pm_r.start(k)
                pm_l.start(k)

            run(RING, ins, lambda k, sl: ((ob.at[sl], Q2.at[:, :, blk(k, BN)]),), isem, osem, work, done=done)

        def run_first():
            pl.run_scoped(first, bf(TWO, TWO, TH, F2), bf(TWO, TWO, TH, F2), bf(TWO, TH, F2), bf(TWO, TH, F2), bf(RING, *wshape),
                          fl(TWO, TWO, TH, BN), fl(TWO, TH, BN), fl(TWO, TH, BN), dma(RING, RING), dma(MANY), dma(MANY))

        def run_second():
            pl.run_scoped(second, bf(TWO, TH, F2), bf(TWO, TH, F2), bf(TWO, *wshape), fl(TWO, TWO, TH, BN), fl(TWO, TWO, HT, BN),
                          fl(TWO, TWO, TH, BN), dma(MANY), dma(TWO, MANY), dma(TWO, MANY))

        def come(j):
            arrived(RR.at[0, :, blk(j, BN)], rid(s + "pr") + j)
            arrived(RR.at[1, :, blk(j, BN)], rid(s + "pl") + j)
        return run_first, run_second, come

    y1, y2, y_come = region("Y", False, o["HP"], o["HQ"], o["PY"], o["RY"])
    d1, d2, d_come = region("D", True, o["CP"], o["CQ"], o["PD"], o["RD"])
    d1()
    y1()
    d2()
    grad2(hn, lambda k: S2.at[:, blk(k, BN)], lambda k, ob, sem: s2.start(k))
    y2()

    def piece(ii):
        return slice(ii * FB, (ii + 1) * FB)

    k1u = [Send(lambda m, ii=ii: (K1.at[m, :, piece(ii)], OUT1.at[:, f_block(TWO * g + ii, d)], rid("k1u") + d * TWO + ii, dev(u, m)), TWO)
           for ii in BOTH]
    k1d = [Send(lambda m, ii=ii: (K1.at[TWO + e, :, piece(ii)], OUT1.at[:, f_block(TWO * g + ii, d)], rid("k1d") + ii, dev_e)) for ii in BOTH]

    def done1(k, ob, sem):
        @when(k < TWO)
        def _():
            for t in k1u:
                t.start(k)

        @when(k == TWO + e)
        def _():
            for t in k1d:
                t.start()

        @when(k == TWO + d)
        def _():
            move(batch(sem, *[(ob.at[:, piece(ii)], OUT1.at[:, f_block(TWO * g + ii, d)]) for ii in BOTH]))

    def out2_at(core, jj):
        return OUT2.at[blk(core, FB), blk(jj, BN)]

    k2 = Send(lambda jj: (K2.at[TWO * e + jj], out2_at(d, jj), rid("k2") + jj, dev_e), TWO)

    def done2(k, ob, sem):
        @when(high(k) == d)
        def _():
            move(batch(sem, (ob, out2_at(d, low(k)))))

        @when(high(k) == e)
        def _():
            k2.start(low(k))

    grad1(hi, flip(hp), lambda k: K1.at[k], done1, lambda k: (R1.at[k], rid("s1") + k))

    RX_, OUTX, XO, OUTY, YO, BG, SO = [o[t] for t in ("DRX", "OUTX", "XO", "OUTY", "YO", "BG", "SO")]
    xo = Send(lambda j: (XO, OUTX.at[blk(d, TH), :], rid("xo"), dev_e))
    stages = [dev_e, dev(u, d), dev(v, d), {"col": c + 1 - TWO * c_lo}, {"col": RING - 1 - c}]
    assert len(stages) == STAGES
    sum_send = [Send(lambda j, k=k, dv=dv: (sums.at[k], sums_in.at[k], rid("sum") + k, dv))
                for k, dv in enumerate(stages)]
    bsend = [Send(lambda j, k=k, dv=dv: (db.at[k], db_in.at[k], rid("bf") + k, dv)) for k, dv in enumerate((dev(u, d), dev(v, d)))]
    bg = Send(lambda j: (BG.at[d], BG.at[d], rid("bg"), dev_e))

    def finish_dx(q1b, rlb, rrb, xb, gb, vb, xob, acc, dbb, isem, osem, wsem):
        RB = min(8 * RING, high(TH))
        par_ = batch(wsem, (PV, vb), (o["DB"], dbb))
        start(par_)
        for j in range(RING):
            d_come(j)
        acc[:] = jnp.zeros_like(acc)

        def ins(k, s):
            rows = blk(k, RB)
            return ((o["DQ1"].at[c_hi, rows], q1b.at[s]), (RX_.at[0, rows], rlb.at[s]), (RX_.at[1, rows], rrb.at[s]), (XF.at[rows, :], xb.at[s]),
                    (G.at[hp, c, pl.ds(pl.multiple_of(d * TH + k * RB, RB), RB), :], gb.at[s]))

        def outs(k, s):
            return ((xob.at[s, :, blk(d, DH)], OUTX.at[pl.ds(pl.multiple_of(d * TH + k * RB, RB), RB), :]),
                    (xob.at[s, :, blk(e, DH)], XO.at[blk(k, RB), :]))

        def fold(x):
            return jnp.sum(x.reshape(RB // 8, 8, DM), axis=0)

        def work(k, s):
            @when(k == 0)
            def _():
                wait(par_)
            da = q1b[s] + rlb[s] + rrb[s]
            inv_std, xhat = stats(xb[s].astype(F32))
            gr = gb[s].astype(F32)
            val = da * vb[0:1, :]
            m1 = jnp.sum(val, axis=1, keepdims=True) / DM
            m2 = jnp.sum(val * xhat, axis=1, keepdims=True) / DM
            xob[s] = (gr + inv_std * (val - m1 - xhat * m2)).astype(BF16)
            for i, t in enumerate((da * xhat, da, gr)):
                acc[i] += fold(t)

        run(TH // RB, ins, outs, isem, osem, work)
        xo.start()
        for i in range(RING - 1):
            row = jnp.sum(acc[i], axis=0, keepdims=True)
            acc[i, 0:1, :] = row
        for i in range(RING - 1):
            sums[STAGES, i:i + 1, :] = acc[i, 0:1, blk(d, DH)]
            sums[0, i:i + 1, :] = acc[i, 0:1, blk(e, DH)]
        db[0, 0:1, :] = jnp.sum(dbb[:], axis=0, keepdims=True)
        sum_send[0].start()

    def stage(k):
        arrived(sums_in.at[k], rid("sum") + k)
        sums[STAGES] += sums_in[k]
        if k in (1, TWO):
            arrived(db_in.at[k - 1], rid("bf") + k - 1)
            db[k] = db[k - 1] + db_in[k - 1]
        if k < STAGES - 1:
            sums[k + 1] = sums[STAGES]
            sum_send[k + 1].start()
        if k < TWO:
            bsend[k].start()

    def sums_out(wsem):
        stage(STAGES - 1)
        move(batch(wsem, (sums.at[STAGES], SO), (db.at[TWO], BG.at[d])))
        bg.start()

    def dx_all():
        RB = min(8 * RING, high(TH))
        pl.run_scoped(finish_dx, fl(TWO, RB, DM), fl(TWO, RB, DM), fl(TWO, RB, DM), bf(TWO, RB, DM), bf(TWO, RB, DM), fl(8, DM),
                      bf(TWO, RB, DM), fl(RING - 1, 8, DM), fl(8, FC), dma(TWO, MANY + RING), dma(TWO, MANY), dma(MANY))

    dx_all()
    grad2(hi, lambda k: K2.at[k], done2, lambda k: (R2.at[:, blk(k, BN)], rid("s2") + k), {k: functools.partial(stage, k) for k in range(RING)})

    def outy_at(core, jj):
        return OUTY.at[blk(core, TH), blk(jj, BN)]

    yo = Send(lambda jj: (YO.at[TWO * e + jj], outy_at(d, jj), rid("yo") + jj, dev_e), TWO)

    def finish_y(q1b, xb, vb, rxb, yb, isem, osem, wsem):
        def ins(k, s):
            cols = blk(k, BN)
            return (o["YQ1"].at[c_hi, :, cols], q1b.at[s]), (XF.at[:, cols], xb.at[s]), (PV.at[:, cols], vb.at[s])

        def work(k, s):
            arr = batch(wsem, (o["YRX"].at[:, :, blk(k, BN)], rxb))
            for j in range(RING):
                @when(k == j)
                def _():
                    y_come(j)
            move(arr)
            yb[s] = (xb[s].astype(F32) + (q1b[s] + rxb[0] + rxb[1]) + vb[s, TWO:TWO + 1, :]).astype(BF16)

        def done(k, s):
            @when(high(k) == d)
            def _():
                move(batch(wsem, (yb.at[s], outy_at(d, low(k)))))

            @when(high(k) == e)
            def _():
                yo.start(low(k))

        sums_out(wsem)
        run(RING, ins, lambda k, s: ((yb.at[s], YO.at[k]),), isem, osem, work, done=done)

    pl.run_scoped(finish_y, fl(TWO, TH, BN), bf(TWO, TH, BN), fl(TWO, 8, BN), fl(TWO, TH, BN), bf(TWO, TH, BN), dma(TWO, MANY), dma(TWO, MANY), dma(MANY))

    arrived(OUTX.at[blk(e, TH), :], rid("xo"))
    arrived(BG.at[e], rid("bg"))
    for ii in BOTH:
        arrived(outy_at(e, ii), rid("yo") + ii)
        for dd in BOTH:
            arrived(OUT1.at[:, f_block(TWO * gn + ii, dd)], rid("k1u") + dd * TWO + ii)
        arrived(OUT1.at[:, f_block(TWO * g + ii, e)], rid("k1d") + ii)
        arrived(out2_at(e, ii), rid("k2") + ii)
    for t in pending:
        for j in range(t.n):
            t.desc(j).wait_send()
    assert tuple(counts) == SEMS, counts


SEMS = (169, 147)


def solution(mesh):
    nr, nc, nd = mesh.shape["row"], mesh.shape["col"], mesh.shape["dep"]
    assert nr == 4 and nc == 4 and nd == 2
    tok_spec = P(("part", "row", "col"), "dep")
    vec_dep = P("dep")
    part_dep = P(("part", "dep"))
    in_specs = (tok_spec, vec_dep, vec_dep, P(("dep", "row"), "col"), P("col"), P(("col", "row"), "dep"), vec_dep, tok_spec)
    out_specs = (tok_spec, tok_spec, P(("part", "dep", "row"), "col"), P(("part", "col")), P(("part", "col", "row"), "dep"), part_dep, part_dep, part_dep)

    def local_step(x_in, ln_scale, ln_shift, w_up, b_up, w_down, b_down, y_grad):
        d = lax.axis_index("dep")
        th, dhalf = x_in.shape[0] // 2, x_in.shape[1]
        ds_, fb = w_up.shape[0], w_up.shape[1] // 8
        vec = jnp.stack([ln_scale, ln_shift, b_down.astype(F32)] + [jnp.zeros_like(ln_scale)] * 5)
        b3 = lax.dynamic_index_in_dim(b_up.reshape(4, 2, fb), d, 1, keepdims=False).astype(F32)
        bup = jnp.concatenate([b3[k] for k in (0, 3, 1, 2)]).reshape(1, 4 * fb)

        cfg = (th, 2 * dhalf, ds_, fb)
        outs = pl.pallas_call(
            functools.partial(kernel, cfg),
            name="mlp_layer",
            out_shape=buffers(*cfg),
            in_specs=[pl.BlockSpec(memory_space=pl.ANY)] * 5 + [pl.BlockSpec(memory_space=pltpu.VMEM)],
            out_specs=[pl.BlockSpec(memory_space=pl.ANY)] * len(NAMES),
            scratch_shapes=[dma(SEMS[1]), dma(SEMS[0]), fl(STAGES + 1, 8, dhalf), fl(STAGES, 8, dhalf), fl(3, 8, 4 * fb), fl(2, 8, 4 * fb)],
            compiler_params=pltpu.CompilerParams(collective_id=0, has_side_effects=True, vmem_limit_bytes=62 * 1024 * 1024),
        )(x_in, y_grad, w_up, w_down, vec, bup)
        o = dict(zip(NAMES, outs))
        db = o["BG"][:, 0].reshape(2, 4, fb)
        b_up_grad = jnp.stack([db[:, k] for k in (0, 2, 3, 1)]).reshape(8 * fb)
        return (o["OUTY"], o["OUTX"], o["OUT1"], b_up_grad, o["OUT2"], o["SO"][2], o["SO"][0], o["SO"][1])

    return jax.shard_map(local_step, mesh=mesh, in_specs=in_specs, out_specs=out_specs, check_vma=False)
```

```python
import functools

import jax
import jax.numpy as jnp
from jax import lax
from jax.experimental import pallas as pl
from jax.experimental.pallas import tpu as pltpu
from jax.sharding import PartitionSpec as P

LN_EPS = 1e-5
GELU_K = 0.7978845608028654
GELU_C = 0.044715
F32 = jnp.float32
BF16 = jnp.bfloat16
MESH = pl.DeviceIdType.MESH

NAMES = ("A", "G", "W1", "W2", "HP", "HQ", "CP", "CQ", "DB",
         "PY", "RY", "YQ1", "YQ2", "YRF", "YRX", "PD", "RD", "DQ1", "DQ2", "DRF", "DRX",
         "S1", "R1", "S2", "R2", "K1", "K2", "OUT1", "OUT2", "XF", "GF", "PV", "YO", "XO", "OUTY", "OUTX", "BG", "SO")
TWO, RING, STAGES, MANY = 2, 4, 5, 16
BOTH, SLOTS = (0, 1), (2,)
NT = (((1,), (1,)), ((), ()))
TN = (((0,), (0,)), ((), ()))


def flip(x):
    return 1 - x


def low(x):
    return x % 2


def high(x):
    return x // 2


def buffers(TH, DM, DS, FB):
    F2, FC, T2 = 2 * FB, 4 * FB, 2 * TH
    pair = (TWO, TWO)
    shapes = {
        "A": ((TWO, RING, T2, DM), BF16), "W1": ((DM, FC), BF16), "W2": ((FC, DM), BF16),
        "HP": (SLOTS + pair + (T2, F2), BF16), "HQ": (pair + (T2, F2), BF16), "DB": ((8, FC), F32),
        "S1": ((RING, DS, F2), F32), "S2": ((FB, DM), F32),
        "K1": ((RING, DS, F2), BF16), "K2": ((RING, FB, high(DM) // TWO), BF16),
        "OUT1": ((DS, 8 * FB), BF16), "OUT2": ((F2, high(DM)), BF16),
        "XF": ((TH, DM), BF16), "GF": ((TH, DM), BF16), "PV": ((8, DM), F32), "YO": ((RING, TH, high(DM) // TWO), BF16),
        "XO": ((TH, high(DM)), BF16), "OUTY": ((T2, high(DM)), BF16), "OUTX": ((T2, high(DM)), BF16),
        "BG": (SLOTS + (8, FC), F32), "SO": ((8, high(DM)), F32),
    }
    for new, old in (("G", "A"), ("CP", "HP"), ("CQ", "HQ"), ("R1", "S1"), ("R2", "S2")):
        shapes[new] = shapes[old]
    for p, s in (("PY", "Y"), ("PD", "D")):
        shapes[p] = shapes["R" + s] = (pair + (TH, DM), F32)
        for q in ("Q1", "Q2", "RX"):
            shapes[s + q] = (SLOTS + (TH, DM), F32)
        shapes[s + "RF"] = (SLOTS + (high(TH), DM), F32)
    return [jax.ShapeDtypeStruct(*shapes[n]) for n in NAMES]


def mul(x, n):
    return x * n if isinstance(x, int) else pl.multiple_of(x * n, n)


def cp(src, dst, sem):
    return pltpu.make_async_copy(src, dst, sem)


def parts(src, dst):
    rows = dst.shape[0]
    n = rows if rows == TWO and len(dst.shape) > RING - 1 else RING if rows % (8 * RING) == 0 else 1
    m = rows // n
    return [(src.at[pl.ds(i * m, m)], dst.at[pl.ds(i * m, m)]) for i in range(n)] if n > 1 else [(src, dst)]


def batch(sem, *pairs):
    return [cp(src, dst, sem.at[i]) for i, (src, dst) in enumerate(t for pair in pairs for t in parts(*pair))]


def start(copies):
    for t in copies:
        t.start()


def wait(copies):
    for t in copies:
        t.wait()


def move(copies):
    start(copies)
    wait(copies)


def dma(*shape):
    return pltpu.SemaphoreType.DMA(shape)


def bf(*shape):
    return pltpu.VMEM(shape, BF16)


def fl(*shape):
    return pltpu.VMEM(shape, F32)


def when(cond):
    def deco(fn):
        pl.when(cond)(fn)
    return deco


def run(n, ins, outs, isem, osem, work, done=None, posts=None, late=()):
    posts = posts or {}

    def fetch(k, s):
        return batch(isem.at[s], *ins(k, s))

    def back(k, s):
        return batch(osem.at[s], *outs(k, s))

    start(fetch(0, 0))

    def step(k, _):
        s, nxt = low(k), k + 1
        is_late = functools.reduce(jnp.logical_or, [nxt == t for t in late], False)
        more = nxt < n
        wait(fetch(k, s))

        @when(jnp.logical_and(more, jnp.logical_not(is_late)))
        def _():
            start(fetch(nxt, flip(s)))
        if done is None:
            @when(k >= TWO)
            def _():
                wait(back(k, s))
        work(k, s)
        start(back(k, s))
        for t, fn in posts.items():
            when(k == t)(fn)
        if late:
            @when(is_late)
            def _():
                start(fetch(nxt, flip(s)))
        if done is not None:
            @when(k == 0)
            def _():
                wait(back(k, s))
                done(k, s)

            @when(k >= TWO)
            def _():
                wait(back(k - 1, flip(s)))
                done(k - 1, flip(s))
        return 0

    lax.fori_loop(0, n, step, 0)
    last = n - 1
    if done is None:
        wait(back(last - 1, flip(low(last))))
    wait(back(last, low(last)))
    if done is not None:
        done(last, low(last))


def kernel(cfg, x_in, g_in, w1, w2, vec, bup, *refs):
    TH, DM, DS, FB = cfg
    o = dict(zip(NAMES, refs[:len(NAMES)]))
    ssem, rsem, sums, sums_in, db, db_in = refs[len(NAMES):]
    DH, F2, FC, HT, T2 = high(DM), TWO * FB, RING * FB, high(TH), TWO * TH
    BN, ALLT = high(DH), TWO * RING * T2
    A, G, W1, W2 = o["A"], o["G"], o["W1"], o["W2"]
    r, c, d = lax.axis_index("row"), lax.axis_index("col"), lax.axis_index("dep")
    hp, hi = low(r), high(r)
    hn, e = flip(hi), flip(d)
    g = low(r + hi)
    gn = flip(g)
    u, v, q = r + 1 - TWO * hp, RING - 1 - r, (r + TWO) % RING
    R, L, far = (c + 1) % RING, (c + RING - 1) % RING, (c + TWO) % RING
    pos_r, pos_v, pos_u, pos_q = TWO * g + hi, TWO * g + hn, TWO * gn + hi, TWO * gn + hn
    c_lo, c_hi = low(c), high(c)

    ids, counts = {}, [0, 0]

    def name(key, n=1):
        ids[key] = counts[0]
        counts[0] += n

    def rid(key):
        return ids[key]

    for nm in "AG":
        for w in ("xr1", "xl1", "fr0", "fl0", "fr1", "fl1"):
            name(nm + w)
        for w in ("xr0", "xl0", "u"):
            name(nm + w, TWO)
        for t in "01":
            for w in "cLRxy":
                name(nm + "d" + t + w, TWO)
    for s in "uv":
        name("w1" + s, TWO * RING)
        name("w2" + s, TWO)
        name("f1" + s, RING)
        name("f2" + s)
    for s in ("w2d", "xf", "gf", "pv", "xo", "bg"):
        name(s)
    name("yo", TWO)
    name("bf", TWO)
    name("sum", STAGES)
    for s in ("w1d", "s1", "s2", "k1u"):
        name(s, RING)
    name("k1d", TWO)
    name("k2", TWO)
    for s in "YD":
        for w in ("p", "r", "l", "pr", "pl"):
            name(s + w, RING)

    pending = []
    dev_e, dev_R, dev_L = {"dep": e}, {"col": R}, {"col": L}

    def dev(row, core):
        return {"row": row, "dep": core}

    class Send:
        def __init__(self, fn, n=1):
            self.fn, self.n, self.sid = fn, n, counts[1]
            counts[1] += n
            pending.append(self)

        def desc(self, j=0):
            src, dst, rsid, device = self.fn(j)
            return pltpu.make_async_remote_copy(src_ref=src, dst_ref=dst, send_sem=ssem.at[self.sid + j], recv_sem=rsem.at[rsid],
                                                device_id=device, device_id_type=MESH)

        def start(self, j=0):
            self.desc(j).start()

        def all(self):
            for j in range(self.n):
                self.start(j)

    def same(ref, rsid, device):
        return Send(lambda j: (ref, ref, rsid, device))

    def arrived(dst, rsid):
        pltpu.make_async_remote_copy(src_ref=dst, dst_ref=dst, send_sem=ssem.at[0], recv_sem=rsem.at[rsid],
                                     device_id=dev_e, device_id_type=MESH).wait_recv()

    barrier = pltpu.get_barrier_semaphore()
    peers = [dev_e, dev_R, dev_L] + [dev(t, k) for t in (u, v) for k in BOTH]
    for p in peers:
        pl.semaphore_signal(barrier, inc=1, device_id=p, device_id_type=MESH)
    pl.semaphore_wait(barrier, len(peers))

    ARR = (("A", A), ("G", G))
    ROW = (hp, flip(hp))

    def ch(X, t, col, core, part=None):
        if part is None:
            return X.at[ROW[t], col, pl.ds(mul(core, TH), TH)]
        return X.at[ROW[t], col, pl.ds(pl.multiple_of(core * TH + part * HT, HT), HT)]

    def blk(k, n):
        return pl.ds(mul(k, n), n)

    def f_block(pos, core):
        gg, ii = high(pos), low(pos)
        return blk((flip(gg) * (RING - 1) * ii + gg * (1 + ii)) * TWO + core, FB)

    def w1_src(pos, core):
        return w1.at[:, f_block(pos, core)]

    def w1_dst(dd, row, pos):
        return W1.at[blk(dd * RING + row, DS), blk(pos, FB)]

    def send_w1(tag, row, *positions):
        for pos in positions:
            for core in BOTH:
                Send(lambda j, pos=pos, core=core: (w1_src(pos, core), w1_dst(d, r, pos), rid("w1" + tag) + d * RING + pos, dev(row, core))).start()

    def w2_part(pos, half):
        return W2.at[blk(pos, FB), blk(half, DH)]

    def send_w2(tag, row):
        for core in BOTH:
            Send(lambda j, core=core: (w2.at[blk(core, FB), :], w2_part(pos_r, d), rid("w2" + tag) + d, dev(row, core))).start()

    def wait_w2(tag, pos):
        for dd in BOTH:
            arrived(w2_part(pos, dd), rid("w2" + tag) + dd)

    XF, GF, PV = o["XF"], o["GF"], o["PV"]
    Send(lambda j: (g_in.at[blk(e, TH), :], GF.at[:, blk(d, DH)], rid("gf"), dev_e)).start()
    Send(lambda j: (x_in.at[blk(e, TH), :], XF.at[:, blk(d, DH)], rid("xf"), dev_e)).start()
    Send(lambda j: (vec, PV.at[:, blk(d, DH)], rid("pv"), dev_e)).start()
    OWN_TO = (("xr0", dev_R), ("xl0", dev_L), ("u", dev(u, d)), ("d0c", dev_e))
    send_w1("v", v, pos_v, pos_r)
    send_w1("u", u, pos_u, pos_q)
    for w, dv in OWN_TO:
        Send(lambda j, w=w, dv=dv: (g_in.at[blk(d, TH), :], G.at[hp, c, blk(d, TH), blk(d, DH)], rid("G" + w), dv)).start()

    RL = min(8 * RING, TH)

    def stats(x):
        mean = jnp.sum(x, axis=1, keepdims=True) / DM
        var = jnp.sum(x * x, axis=1, keepdims=True) / DM - mean * mean
        inv_std = lax.rsqrt(var + LN_EPS)
        return inv_std, (x - mean) * inv_std


    def own_part(xb, gb, ab, vb, b2, b3, sems, sems2):
        mine, other = blk(d, DH), blk(e, DH)
        ld = batch(sems, (g_in.at[blk(d, TH), :], gb.at[:, mine]), (x_in.at[blk(d, TH), :], xb.at[:, mine]), (vec, vb.at[:, mine]))
        start(ld)
        wait(ld)
        got = batch(sems, (GF.at[:, other], gb.at[:, other]), (XF.at[:, other], xb.at[:, other]), (PV.at[:, other], vb.at[:, other]))
        for ref, w in ((GF, "gf"), (XF, "xf"), (PV, "pv")):
            arrived(ref.at[:, other], rid(w))
            if ref is GF:
                for w, dv in OWN_TO:
                    Send(lambda j, w=w, dv=dv: (GF.at[:, blk(e, DH)], G.at[hp, c, blk(d, TH), blk(e, DH)], rid("G" + w) + 1, dv)).start()
        move(got)
        start(batch(sems2, (gb, ch(G, 0, c, d))))
        keep = batch(sems, (xb.at[:, mine], XF.at[:, mine]), (vb.at[:, mine], PV.at[:, mine]))
        start(keep)
        scale, shift = vb[0:1, :], vb[1:TWO, :]

        def rows(m, _):
            sl = blk(m, RL)
            ab[sl, :] = (stats(xb[sl, :].astype(F32))[1] * scale + shift).astype(BF16)
            return 0

        lax.fori_loop(0, TH // RL, rows, 0)
        wait(keep)
        move(batch(sems, (ab, ch(A, 0, c, d))))
        for w, dv in OWN_TO:
            Send(lambda j, w=w, dv=dv: (ch(A, 0, c, d), ch(A, 0, c, d), rid("A" + w), dv)).start()
        send_w2("u", u)
        send_w1("u", u, pos_r, pos_v)
        wait(batch(sems2, (gb, ch(G, 0, c, d))))
        wl = batch(sems, (w2.at[blk(d, FB), :], b3), (w1_src(0, d), b2.at[:, blk(0, FB)]))
        move(wl)
        move(batch(sems, *[(w1_src(pos, d), b2.at[:, blk(pos, FB)]) for pos in range(1, RING)]))
        move(batch(sems, (b3, w2_part(pos_r, d)), (b2, W1.at[blk(d * RING + r, DS), :])))

    pl.run_scoped(own_part, bf(TH, DM), bf(TH, DM), bf(TH, DM), fl(8, DM), bf(DS, FC), bf(FB, DH), dma(MANY), dma(MANY))
    for pos in range(RING):
        Send(lambda j, pos=pos: (w1_src(pos, e), w1_dst(d, r, pos), rid("w1d") + pos, dev_e)).start()
    Send(lambda j: (w2.at[blk(e, FB), :], w2_part(pos_r, d), rid("w2d"), dev_e)).start()

    fwd, par = {}, {}
    for nm, X in ARR:
        for t in BOTH:
            b = nm + "d" + str(t)
            fwd[nm, t] = [same(ch(X, t, L, d, 0), rid(nm + "fr" + str(t)), dev_R), same(ch(X, t, R, d, 1), rid(nm + "fl" + str(t)), dev_L),
                          same(ch(X, t, L, d), rid(b + "L"), dev_e), same(ch(X, t, R, d), rid(b + "R"), dev_e),
                          same(ch(X, t, far, d, 0), rid(b + "x"), dev_e), same(ch(X, t, far, d, 1), rid(b + "y"), dev_e)]
        par[nm] = [same(ch(X, 1, c, d), rid(nm + w), dv) for w, dv in (("xr1", dev_R), ("xl1", dev_L), ("d1c", dev_e))]

    def own_in(nm, X, t, col, w, core=d):
        if nm + w in ("Gxr0", "Gxl0", "Gu", "Gd0c"):
            for half, i in ((core, 0), (flip(core), 1)):
                arrived(X.at[ROW[t], col, blk(core, TH), blk(half, DH)], rid(nm + w) + i)
        else:
            arrived(ch(X, t, col, core), rid(nm + w))

    def pass_on(nm, X, t):
        to_r, to_l, d_l, d_r = fwd[nm, t][:RING]
        own_in(nm, X, t, L, "xr" + str(t))
        to_r.start()
        own_in(nm, X, t, R, "xl" + str(t))
        to_l.start()
        d_l.start()
        d_r.start()

    def from_u(nm, X):
        own_in(nm, X, 1, c, "u")
        for t in par[nm]:
            t.start()

    def far_in(nm, X, t):
        for part, w in zip(BOTH, ("fr", "fl")):
            arrived(ch(X, t, far, d, part), rid(nm + w + str(t)))
            fwd[nm, t][RING + part].start()

    def other_core(t, *which):
        for nm, X in ARR:
            b = nm + "d" + str(t)
            for w in which:
                if w == "far":
                    for part, z in zip(BOTH, "xy"):
                        arrived(ch(X, t, far, e, part), rid(b + z))
                else:
                    own_in(nm, X, t, {"c": c, "L": L, "R": R}[w], b[1:] + w, e)

    def hop(tag, row, device, *positions):
        out = []
        for pos in positions:
            out.append(Send(lambda j, pos=pos: (w1_dst(j, row, pos), w1_dst(j, row, pos), rid(tag) + low(pos) * TWO + j, device), TWO))
        return out

    f1v = hop("f1v", u, dev(v, d), pos_v, pos_r)
    f1u = hop("f1u", v, dev(u, d), pos_r, pos_v)
    q0, q1 = pl.ds(0, BN), pl.ds(BN, DM - BN)
    f2u = same(W2.at[blk(pos_v, FB), q0], rid("f2u"), dev(u, d))
    f2v = same(W2.at[blk(pos_u, FB), q1], rid("f2v"), dev(v, d))

    def w1_in(tag, row, pos):
        for dd in BOTH:
            arrived(w1_dst(dd, row, pos), rid("w1" + tag) + dd * RING + pos)

    def w1_rest(pos, tag):
        arrived(w1_dst(e, r, pos), rid("w1d") + pos)
        for j in BOTH:
            arrived(w1_dst(j, q, pos), rid(tag) + low(pos) * TWO + j)

    for pos in (pos_r, pos_v):
        w1_in("u", u, pos)
    for t in f1v:
        t.all()
    send_w2("v", v)
    send_w1("v", v, pos_q, pos_u)
    pass_on("G", G, 0)
    for pos in (pos_r, pos_v):
        w1_in("v", v, pos)
    for t in f1u:
        t.all()
    other_core(0, "c")
    arrived(w2_part(pos_r, e), rid("w2d"))
    w1_rest(pos_r, "f1v")

    RC = min(8 * RING, TH)

    def cd_block(a, gr, w1b, w2b, bias, cbuf, gbuf, h_out, dc_out, db, count_db):
        cbuf[:] = jnp.dot(a, w1b, preferred_element_type=F32)
        gbuf[:] = lax.dot_general(gr, w2b, NT, preferred_element_type=F32)

        def rows(m, acc):
            sl = blk(m, RC)
            pre = cbuf[sl, :] + bias
            sq = pre * pre
            th = jnp.tanh(GELU_K * (pre + GELU_C * pre * sq))
            half = 0.5 * (1.0 + th)
            slope = half + 0.5 * pre * (1.0 - th * th) * GELU_K * (1.0 + 3.0 * GELU_C * sq)
            dc = gbuf[sl, :] * slope
            h_out[sl, :] = (pre * half).astype(BF16)
            dc_out[sl, :] = dc.astype(BF16)
            return acc + jnp.sum(dc.reshape(RC // 8, 8, FB), axis=0)

        acc = lax.fori_loop(0, T2 // RC, rows, jnp.zeros((8, FB), F32))

        @when(count_db)
        def _():
            db[:] += acc

    def hidden(n, place, block, need, first, posts, late):
        def body(ab, gb, w1b, w2b, cbuf, gbuf, hb, cb, dbs, isem, osem, wsem):
            def weights(b):
                pos = block(b * first)[1]
                return batch(wsem.at[b], (W1.at[:, blk(pos, FB)], w1b.at[b]), (W2.at[blk(pos, FB), :], w2b.at[b]))

            def load(b):
                need(b)
                start(weights(b))

            load(0)
            dbs[:] = jnp.zeros_like(dbs)

            def ins(k, s):
                row, col, _ = place(k)
                return (A.at[row, col], ab.at[s]), (G.at[row, col], gb.at[s])

            def outs(k, s):
                row, col, _ = place(k)
                to_p, cols = block(k)[TWO:]
                at = (high(col), low(col), slice(None), cols)
                H, C = (o["HP"].at[row], o["CP"].at[row]) if to_p else (o["HQ"], o["CQ"])
                return (hb.at[s], H.at[at]), (cb.at[s], C.at[at])

            def work(k, s):
                b, pos = block(k)[:TWO]
                for t in BOTH:
                    @when(k == t * first)
                    def _():
                        wait(weights(t))
                cd_block(ab[s], gb[s], w1b[b], w2b[b], bup[:, f_block(pos, d)].astype(F32), cbuf, gbuf, hb.at[s], cb.at[s], dbs.at[b], place(k)[TWO])

            run(n, ins, outs, isem, osem, work, posts={k: functools.partial(fn, load) for k, fn in posts.items()}, late=late)
            move(batch(wsem.at[0], *[(dbs.at[b], o["DB"].at[:, blk(block(b * first)[1], FB)]) for b in BOTH]))

        pl.run_scoped(body, bf(TWO, T2, DM), bf(TWO, T2, DM), bf(TWO, DM, FB), bf(TWO, FB, DM), fl(T2, FB), fl(T2, FB),
                      bf(TWO, T2, FB), bf(TWO, T2, FB), fl(TWO, 8, FB), dma(TWO, MANY), dma(TWO, MANY), dma(TWO, MANY))

    five, ten = RING + 1, TWO * RING + TWO

    def place1(k):
        early = k < ten
        k5, k2 = k % five, high(k - ten) + 1
        mine = jnp.logical_and(early, k5 < RING)
        m = jnp.where(early, k5 % RING, k2)
        return jnp.where(mine, hp, flip(hp)), (c + m + high(m) * (five - TWO * m)) % RING, mine

    def block1(k):
        b = jnp.where(k < ten, k // five % TWO, low(k))
        ii = jnp.where(b == 0, hi, hn)
        return b, TWO * g + ii, True, blk(ii, FB)

    def need1(b):
        if b:
            wait_w2("v", pos_v)
            f2u.start()
            w1_rest(pos_v, "f1v")

    def post0(load):
        pass_on("A", A, 0)
        from_u("G", G)
        other_core(0, "L", "R")

    def post2(load):
        far_in("G", G, 0)
        from_u("A", A)
        far_in("A", A, 0)
        other_core(0, "far")

    def post9(load):
        pass_on("A", A, 1)
        wait_w2("u", pos_u)
        f2v.start()
        other_core(1, "L", "R")

    def post13(load):
        start(early())
        far_in("G", G, 1)
        far_in("A", A, 1)
        other_core(1, "far")

    ahead = []

    def early():
        rb, sem = ahead
        return batch(sem, (o["CP"].at[hp], rb.at[hp]),
                     *[(o["CP"].at[flip(hp), high(t), low(t)], rb.at[flip(hp), high(t), low(t)]) for t in (c, R)])

    def rest():
        rb, sem = ahead
        return batch(sem.at[pl.ds(MANY, MANY)], *[(o["CP"].at[flip(hp), high(t), low(t)], rb.at[flip(hp), high(t), low(t)]) for t in (L, far)])

    posts1 = {0: post0, TWO: post2, RING - 1: lambda load: other_core(1, "c"), RING: lambda load: load(1),
              five: lambda load: pass_on("G", G, 1), ten - 1: post9, ten + RING - 1: post13}

    S1, R1, S2, R2, K1, K2, OUT1, OUT2 = [o[t] for t in ("S1", "R1", "S2", "R2", "K1", "K2", "OUT1", "OUT2")]
    s1 = Send(lambda j: (S1.at[j], R1.at[j], rid("s1") + j, dev(v, d)), RING)
    s2 = Send(lambda j: (S2.at[:, blk(j, BN)], R2.at[:, blk(j, BN)], rid("s2") + j, dev(v, d)), RING)

    def dw1_cols(k, pair, first):
        j = first + (1 - TWO * first) * high(k)
        return blk(low(k) * RING + TWO * pair + j, DS)

    def grad(left, right, left_shape, right_shape, resident, out_shape, outs, done, recv=None, posts=None, mid=None, pre=None):
        rows, width = out_shape

        def body(acc, ob, nb, isem, osem, wsem, lb, rb):
            if pre is not None:
                stay = early() + rest()
            else:
                stay = batch(wsem, resident((lb, rb)))
                start(stay)

            def ins(k, s):
                return (left(k), lb.at[s]) if right is None else (right(k), rb.at[s]),

            def work(k, s):
                @when(k == 0)
                def _():
                    wait(stay)
                x, y = (lb[s], rb[:]) if right is None else (lb[:], rb[s])
                val = lax.dot_general(x.reshape(ALLT, rows), y.reshape(ALLT, width), TN, preferred_element_type=F32)
                if recv is None:
                    ob[s] = val
                else:
                    acc[:] = val
                    if mid:
                        when(k == RING - 1)(mid)
                    ref, rsid = recv(k)
                    arrived(ref, rsid)
                    move(batch(wsem, (ref, nb)))
                    ob[s] = (acc[:] + nb[:]).astype(BF16)

            run(RING, ins, lambda k, s: ((ob.at[s], outs(k)),), isem, osem, work, done=lambda k, s: done(k, ob.at[s], wsem), posts=posts)

        extra = out_shape if recv else (8, BN)
        kinds = [fl(*extra), pltpu.VMEM(SLOTS + out_shape, BF16 if recv else F32), fl(*extra), dma(TWO, MANY), dma(TWO, MANY), dma(MANY)]
        if pre is not None:
            pl.run_scoped(lambda *bufs: body(*bufs, pre), *kinds, bf(*left_shape))
        else:
            pl.run_scoped(body, *kinds, bf(*left_shape), bf(*right_shape))

    PT, PTS = (TWO, RING, T2), (TWO, TWO, TWO, T2)

    def grad1(pair, first, outs, done, recv=None, pre=None):
        grad(lambda k: A.at[:, :, :, dw1_cols(k, pair, first)], None, SLOTS + PT + (DS,), PTS + (F2,), lambda b: (o["CP"], b[1]),
             (DS, F2), outs, done, recv, pre=pre)

    def grad2(pair, outs, done, recv=None, posts=None, mid=None):
        grad(None, lambda k: G.at[:, :, :, blk(k, BN)], PTS + (FB,), SLOTS + PT + (BN,), lambda b: (o["HP"].at[:, :, :, :, blk(pair, FB)], b[0]),
             (FB, BN), outs, done, recv, posts, mid)

    def phase1(rb, sem):
        ahead.extend((rb, sem))
        hidden(ten + RING + TWO, place1, block1, need1, five, posts1, (1, RING - 1, RING, ten, ten + RING))
        start(rest())
        grad1(hn, hp, lambda k: S1.at[k], lambda k, ob, sem: s1.start(k), pre=rb)

    pl.run_scoped(phase1, bf(*PTS, F2), dma(TWO * MANY))

    def block2(k):
        b = k // RING
        ii = jnp.where(b == 0, hi, hn)
        return b, TWO * gn + ii, False, blk(ii, FB)

    def need2(b):
        pos = pos_q if b else pos_u
        w1_in("u", u, pos)
        w1_in("v", v, pos)
        w1_rest(pos, "f1u")
        if b:
            arrived(W2.at[blk(pos_q, FB), q1], rid("f2v"))
            arrived(W2.at[blk(pos_q, FB), q0], rid("f2u"))

    hidden(TWO * RING, lambda k: (hp, k % RING, k >= 0), block2, need2, RING, {TWO: lambda load: load(1)}, ())

    def region(s, nt, XP, XQ, PX, RX):
        Q1, Q2, RF, RR = [o[s + t] for t in ("Q1", "Q2", "RF", "RX")]
        ex = Send(lambda j: (PX.at[:, :, :, blk(j, BN)], RX.at[:, :, :, blk(j, BN)], rid(s + "p") + j, dev_e), RING)
        away = flip(c_hi)
        far_r = Send(lambda j: (Q1.at[away, blk(0, HT), blk(j, BN)], RF.at[away, :, blk(j, BN)], rid(s + "r") + j, dev_R), RING)
        far_l = Send(lambda j: (Q1.at[away, blk(1, HT), blk(j, BN)], RF.at[away, :, blk(j, BN)], rid(s + "l") + j, dev_L), RING)
        pm_r = Send(lambda j: (Q2.at[high(R), :, blk(j, BN)], RR.at[0, :, blk(j, BN)], rid(s + "pr") + j, dev_R), RING)
        pm_l = Send(lambda j: (Q2.at[high(L), :, blk(j, BN)], RR.at[1, :, blk(j, BN)], rid(s + "pl") + j, dev_L), RING)
        wshape = (BN, FC) if nt else (FC, BN)
        mine, other = blk(d, TH), blk(e, TH)

        def wsrc(j):
            return W1.at[blk(j, BN), :] if nt else W2.at[:, blk(j, BN)]

        def wdot(out, p_ref, q_ref, wref):
            for ref, half in ((p_ref, g), (q_ref, gn)):
                x, sel = ref[:].reshape(-1, F2), blk(half, F2)
                if nt:
                    val = lax.dot_general(x, wref[:, sel], NT, preferred_element_type=F32)
                else:
                    val = jnp.dot(x, wref[sel, :], preferred_element_type=F32)
                val = val.reshape(out.shape)
                out[:] = val if ref is p_ref else out[:] + val

        def first(lop, loq, lfp, lfq, wb, ob, ab, qb, wsem, lsem, osem, asem):
            def wcp(j):
                return batch(wsem.at[low(j)], (wsrc(j), wb.at[low(j)]))

            lds = batch(lsem, (XP.at[hp, :, :, other], lop), (XQ.at[:, :, other], loq), (XP.at[hp, :, c_lo, mine], lfp), (XQ.at[:, c_lo, mine], lfq))
            start(wcp(0) + lds)
            wait(lds)

            def step(j, _):
                o1 = batch(osem, (ob, PX.at[:, :, :, blk(j, BN)]))

                @when(j < RING)
                def _():
                    wait(wcp(j))

                    @when(j < RING - 1)
                    def _():
                        start(wcp(j + 1))
                    wdot(ob, lop, loq, wb.at[low(j)])
                    start(o1)

                @when(j >= 1)
                def _():
                    k = j - 1
                    arrived(RX.at[:, :, :, blk(k, BN)], rid(s + "p") + k)
                    start(batch(asem, (RX.at[:, c_lo, :, blk(k, BN)], ab)))

                @when(j < RING)
                def _():
                    wait(o1)
                    ex.start(j)

                @when(j >= 1)
                def _():
                    k = j - 1
                    wait(batch(asem, (RX.at[:, c_lo, :, blk(k, BN)], ab)))
                    qb[:] += ab[:]
                    move(batch(lsem, (qb, Q1.at[:, :, blk(k, BN)])))
                    far_r.start(k)
                    far_l.start(k)

                @when(j < RING)
                def _():
                    wdot(qb, lfp, lfq, wb.at[low(j)])
                return 0

            lax.fori_loop(0, RING + 1, step, 0)

        def second(lp, lq, wb, ab, fb, ob, lsem, isem, osem):
            lds = batch(lsem, (XP.at[hp, :, flip(c_lo), mine], lp), (XQ.at[:, flip(c_lo), mine], lq))
            start(lds)

            def need(k):
                arrived(RF.at[high(R), :, blk(k, BN)], rid(s + "r") + k)
                arrived(RF.at[high(L), :, blk(k, BN)], rid(s + "l") + k)

            for k in range(RING):
                need(k)
            wait(lds)

            def ins(k, sl):
                return (wsrc(k), wb.at[sl]), (RX.at[:, flip(c_lo), :, blk(k, BN)], ab.at[sl]), (RF.at[:, :, blk(k, BN)], fb.at[sl])

            def work(k, sl):
                wdot(ob.at[sl], lp, lq, wb.at[sl])
                ob[sl] += ab[sl]
                for col, part in ((R, 0), (L, 1)):
                    ob[sl, high(col), part * HT:(part + 1) * HT, :] += fb[sl, high(col)]

            def done(k, sl):
                pm_r.start(k)
                pm_l.start(k)

            run(RING, ins, lambda k, sl: ((ob.at[sl], Q2.at[:, :, blk(k, BN)]),), isem, osem, work, done=done)

        def run_first():
            pl.run_scoped(first, bf(TWO, TWO, TH, F2), bf(TWO, TWO, TH, F2), bf(TWO, TH, F2), bf(TWO, TH, F2), bf(TWO, *wshape),
                          fl(TWO, TWO, TH, BN), fl(TWO, TH, BN), fl(TWO, TH, BN), dma(TWO, RING), dma(MANY), dma(MANY), dma(MANY))

        def run_second():
            pl.run_scoped(second, bf(TWO, TH, F2), bf(TWO, TH, F2), bf(TWO, *wshape), fl(TWO, TWO, TH, BN), fl(TWO, TWO, HT, BN),
                          fl(TWO, TWO, TH, BN), dma(MANY), dma(TWO, MANY), dma(TWO, MANY))

        def come(j):
            arrived(RR.at[0, :, blk(j, BN)], rid(s + "pr") + j)
            arrived(RR.at[1, :, blk(j, BN)], rid(s + "pl") + j)
        return run_first, run_second, come

    y1, y2, y_come = region("Y", False, o["HP"], o["HQ"], o["PY"], o["RY"])
    d1, d2, d_come = region("D", True, o["CP"], o["CQ"], o["PD"], o["RD"])
    d1()
    y1()
    d2()
    grad2(hn, lambda k: S2.at[:, blk(k, BN)], lambda k, ob, sem: s2.start(k))
    y2()

    def piece(ii):
        return slice(ii * FB, (ii + 1) * FB)

    k1u = [Send(lambda m, ii=ii: (K1.at[m, :, piece(ii)], OUT1.at[:, f_block(TWO * g + ii, d)], rid("k1u") + d * TWO + ii, dev(u, m)), TWO)
           for ii in BOTH]
    k1d = [Send(lambda m, ii=ii: (K1.at[TWO + e, :, piece(ii)], OUT1.at[:, f_block(TWO * g + ii, d)], rid("k1d") + ii, dev_e)) for ii in BOTH]

    def done1(k, ob, sem):
        @when(k < TWO)
        def _():
            for t in k1u:
                t.start(k)

        @when(k == TWO + e)
        def _():
            for t in k1d:
                t.start()

        @when(k == TWO + d)
        def _():
            move(batch(sem, *[(ob.at[:, piece(ii)], OUT1.at[:, f_block(TWO * g + ii, d)]) for ii in BOTH]))

    def out2_at(core, jj):
        return OUT2.at[blk(core, FB), blk(jj, BN)]

    k2 = Send(lambda jj: (K2.at[TWO * e + jj], out2_at(d, jj), rid("k2") + jj, dev_e), TWO)

    def done2(k, ob, sem):
        @when(high(k) == d)
        def _():
            move(batch(sem, (ob, out2_at(d, low(k)))))

        @when(high(k) == e)
        def _():
            k2.start(low(k))

    grad1(hi, flip(hp), lambda k: K1.at[k], done1, lambda k: (R1.at[k], rid("s1") + k))

    RX_, OUTX, XO, OUTY, YO, BG, SO = [o[t] for t in ("DRX", "OUTX", "XO", "OUTY", "YO", "BG", "SO")]
    xo = Send(lambda j: (XO, OUTX.at[blk(d, TH), :], rid("xo"), dev_e))
    stages = [dev_e, dev(u, d), dev(v, d), {"col": c + 1 - TWO * c_lo}, {"col": RING - 1 - c}]
    assert len(stages) == STAGES
    sum_send = [Send(lambda j, k=k, dv=dv: (sums.at[k], sums_in.at[k], rid("sum") + k, dv))
                for k, dv in enumerate(stages)]
    bsend = [Send(lambda j, k=k, dv=dv: (db.at[k], db_in.at[k], rid("bf") + k, dv)) for k, dv in enumerate((dev(u, d), dev(v, d)))]
    bg = Send(lambda j: (BG.at[d], BG.at[d], rid("bg"), dev_e))

    def finish_dx(q1b, rlb, rrb, xb, gb, vb, xob, acc, dbb, isem, osem, wsem):
        RB = min(8 * RING, high(TH))
        par_ = batch(wsem, (PV, vb), (o["DB"], dbb))
        start(par_)
        for j in range(RING):
            d_come(j)
        acc[:] = jnp.zeros_like(acc)

        def ins(k, s):
            rows = blk(k, RB)
            return ((o["DQ1"].at[c_hi, rows], q1b.at[s]), (RX_.at[0, rows], rlb.at[s]), (RX_.at[1, rows], rrb.at[s]), (XF.at[rows, :], xb.at[s]),
                    (G.at[hp, c, pl.ds(pl.multiple_of(d * TH + k * RB, RB), RB), :], gb.at[s]))

        def outs(k, s):
            return ((xob.at[s, :, blk(d, DH)], OUTX.at[pl.ds(pl.multiple_of(d * TH + k * RB, RB), RB), :]),
                    (xob.at[s, :, blk(e, DH)], XO.at[blk(k, RB), :]))

        def fold(x):
            return jnp.sum(x.reshape(RB // 8, 8, DM), axis=0)

        def work(k, s):
            @when(k == 0)
            def _():
                wait(par_)
            da = q1b[s] + rlb[s] + rrb[s]
            inv_std, xhat = stats(xb[s].astype(F32))
            gr = gb[s].astype(F32)
            val = da * vb[0:1, :]
            m1 = jnp.sum(val, axis=1, keepdims=True) / DM
            m2 = jnp.sum(val * xhat, axis=1, keepdims=True) / DM
            xob[s] = (gr + inv_std * (val - m1 - xhat * m2)).astype(BF16)
            for i, t in enumerate((da * xhat, da, gr)):
                acc[i] += fold(t)

        run(TH // RB, ins, outs, isem, osem, work)
        xo.start()
        for i in range(RING - 1):
            row = jnp.sum(acc[i], axis=0, keepdims=True)
            acc[i, 0:1, :] = row
        for i in range(RING - 1):
            sums[STAGES, i:i + 1, :] = acc[i, 0:1, blk(d, DH)]
            sums[0, i:i + 1, :] = acc[i, 0:1, blk(e, DH)]
        db[0, 0:1, :] = jnp.sum(dbb[:], axis=0, keepdims=True)
        sum_send[0].start()

    def stage(k):
        arrived(sums_in.at[k], rid("sum") + k)
        sums[STAGES] += sums_in[k]
        if k in (1, TWO):
            arrived(db_in.at[k - 1], rid("bf") + k - 1)
            db[k] = db[k - 1] + db_in[k - 1]
        if k < STAGES - 1:
            sums[k + 1] = sums[STAGES]
            sum_send[k + 1].start()
        if k < TWO:
            bsend[k].start()

    def sums_out(wsem):
        stage(STAGES - 1)
        move(batch(wsem, (sums.at[STAGES], SO), (db.at[TWO], BG.at[d])))
        bg.start()

    def dx_all():
        RB = min(8 * RING, high(TH))
        pl.run_scoped(finish_dx, fl(TWO, RB, DM), fl(TWO, RB, DM), fl(TWO, RB, DM), bf(TWO, RB, DM), bf(TWO, RB, DM), fl(8, DM),
                      bf(TWO, RB, DM), fl(RING - 1, 8, DM), fl(8, FC), dma(TWO, MANY + RING), dma(TWO, MANY), dma(MANY))

    dx_all()

    def outy_at(core, jj):
        return OUTY.at[blk(core, TH), blk(jj, BN)]

    yo = Send(lambda jj: (YO.at[TWO * e + jj], outy_at(d, jj), rid("yo") + jj, dev_e), TWO)

    def last_part(q1b, xb, vb, rxb, yb, sem, sem2):
        def finish_y(k):
            cols = blk(k, BN)
            here = batch(sem, (o["YQ1"].at[c_hi, :, cols], q1b), (XF.at[:, cols], xb), (PV.at[:, cols], vb))
            start(here)
            y_come(k)
            move(batch(sem2, (o["YRX"].at[:, :, cols], rxb)))
            wait(here)
            yb[:] = (xb[:].astype(F32) + (q1b[:] + rxb[0] + rxb[1]) + vb[TWO:TWO + 1, :]).astype(BF16)

            @when(d == high(k))
            def _():
                move(batch(sem, (yb, outy_at(high(k), low(k)))))

            @when(e == high(k))
            def _():
                move(batch(sem, (yb, YO.at[k])))
                yo.start(low(k))

        def third():
            stage(TWO)
            finish_y(0)
            stage(RING - 1)
            finish_y(1)
            finish_y(TWO)

        def mid():
            sums_out(sem)
            finish_y(RING - 1)

        posts = {k: functools.partial(stage, k) for k in BOTH}
        posts[TWO] = third
        grad2(hi, lambda k: K2.at[k], done2, lambda k: (R2.at[:, blk(k, BN)], rid("s2") + k), posts, mid)

    pl.run_scoped(last_part, fl(TH, BN), bf(TH, BN), fl(8, BN), fl(TWO, TH, BN), bf(TH, BN), dma(MANY), dma(MANY))

    arrived(OUTX.at[blk(e, TH), :], rid("xo"))
    arrived(BG.at[e], rid("bg"))
    for ii in BOTH:
        arrived(outy_at(e, ii), rid("yo") + ii)
        for dd in BOTH:
            arrived(OUT1.at[:, f_block(TWO * gn + ii, dd)], rid("k1u") + dd * TWO + ii)
        arrived(OUT1.at[:, f_block(TWO * g + ii, e)], rid("k1d") + ii)
        arrived(out2_at(e, ii), rid("k2") + ii)
    for t in pending:
        for j in range(t.n):
            t.desc(j).wait_send()
    assert tuple(counts) == SEMS, counts


SEMS = (169, 147)


def solution(mesh):
    nr, nc, nd = mesh.shape["row"], mesh.shape["col"], mesh.shape["dep"]
    assert nr == 4 and nc == 4 and nd == 2
    tok_spec = P(("part", "row", "col"), "dep")
    vec_dep = P("dep")
    part_dep = P(("part", "dep"))
    in_specs = (tok_spec, vec_dep, vec_dep, P(("dep", "row"), "col"), P("col"), P(("col", "row"), "dep"), vec_dep, tok_spec)
    out_specs = (tok_spec, tok_spec, P(("part", "dep", "row"), "col"), P(("part", "col")), P(("part", "col", "row"), "dep"), part_dep, part_dep, part_dep)

    def local_step(x_in, ln_scale, ln_shift, w_up, b_up, w_down, b_down, y_grad):
        th, dhalf = x_in.shape[0] // 2, x_in.shape[1]
        ds_, fb = w_up.shape[0], w_up.shape[1] // 8
        vec = jnp.stack([ln_scale, ln_shift, b_down.astype(F32)] + [jnp.zeros_like(ln_scale)] * 5)

        cfg = (th, 2 * dhalf, ds_, fb)
        outs = pl.pallas_call(
            functools.partial(kernel, cfg),
            name="mlp_layer",
            out_shape=buffers(*cfg),
            in_specs=[pl.BlockSpec(memory_space=pl.ANY)] * 5 + [pl.BlockSpec(memory_space=pltpu.VMEM)],
            out_specs=[pl.BlockSpec(memory_space=pl.ANY)] * len(NAMES),
            scratch_shapes=[dma(SEMS[1]), dma(SEMS[0]), fl(STAGES + 1, 8, dhalf), fl(STAGES, 8, dhalf), fl(3, 8, 4 * fb), fl(2, 8, 4 * fb)],
            compiler_params=pltpu.CompilerParams(collective_id=0, has_side_effects=True, vmem_limit_bytes=62 * 1024 * 1024),
        )(x_in, y_grad, w_up, w_down, vec, b_up.reshape(1, 8 * fb))
        o = dict(zip(NAMES, outs))
        db = o["BG"][:, 0].reshape(2, 4, fb)
        b_up_grad = jnp.stack([db[:, k] for k in (0, 2, 3, 1)]).reshape(8 * fb)
        return (o["OUTY"], o["OUTX"], o["OUT1"], b_up_grad, o["OUT2"], o["SO"][2], o["SO"][0], o["SO"][1])

    return jax.shard_map(local_step, mesh=mesh, in_specs=in_specs, out_specs=out_specs, check_vma=False)
```

```python
import functools

import jax
import jax.numpy as jnp
from jax import lax
from jax.experimental import pallas as pl
from jax.experimental.pallas import tpu as pltpu
from jax.sharding import PartitionSpec as P

LN_EPS = 1e-5
GELU_K = 0.7978845608028654
GELU_C = 0.044715
F32 = jnp.float32
BF16 = jnp.bfloat16
MESH = pl.DeviceIdType.MESH

NAMES = ("A", "G", "W1", "W2", "HP", "HQ", "CP", "CQ", "DB",
         "PY", "RY", "YQ1", "YQ2", "YRF", "YRX", "PD", "RD", "DQ1", "DQ2", "DRF", "DRX",
         "S1", "R1", "S2", "R2", "K1", "K2", "OUT1", "OUT2", "XF", "GF", "PV", "YO", "XO", "OUTY", "OUTX", "BG", "SO")
TWO, RING, STAGES, MANY = 2, 4, 5, 16
LAG = 2
BOTH, SLOTS = (0, 1), (2,)
NT = (((1,), (1,)), ((), ()))
TN = (((0,), (0,)), ((), ()))


def flip(x):
    return 1 - x


def low(x):
    return x % 2


def high(x):
    return x // 2


def buffers(TH, DM, DS, FB):
    F2, FC, T2 = 2 * FB, 4 * FB, 2 * TH
    pair = (TWO, TWO)
    shapes = {
        "A": ((TWO, RING, T2, DM), BF16), "W1": ((DM, FC), BF16), "W2": ((FC, DM), BF16),
        "HP": (SLOTS + pair + (T2, F2), BF16), "HQ": (pair + (T2, F2), BF16), "DB": ((8, FC), F32),
        "S1": ((RING, DS, F2), F32), "S2": ((FB, DM), F32),
        "K1": ((RING, DS, F2), BF16), "K2": ((RING, FB, high(DM) // TWO), BF16),
        "OUT1": ((DS, 8 * FB), BF16), "OUT2": ((F2, high(DM)), BF16),
        "XF": ((TH, DM), BF16), "GF": ((TH, DM), BF16), "PV": ((8, DM), F32), "YO": ((RING, TH, high(DM) // TWO), BF16),
        "XO": ((TH, high(DM)), BF16), "OUTY": ((T2, high(DM)), BF16), "OUTX": ((T2, high(DM)), BF16),
        "BG": (SLOTS + (8, FC), F32), "SO": ((8, high(DM)), F32),
    }
    for new, old in (("G", "A"), ("CP", "HP"), ("CQ", "HQ"), ("R1", "S1"), ("R2", "S2")):
        shapes[new] = shapes[old]
    for p, s in (("PY", "Y"), ("PD", "D")):
        shapes[p] = shapes["R" + s] = (pair + (TH, DM), F32)
        for q in ("Q1", "Q2", "RX"):
            shapes[s + q] = (SLOTS + (TH, DM), F32)
        shapes[s + "RF"] = (SLOTS + (high(TH), DM), F32)
    return [jax.ShapeDtypeStruct(*shapes[n]) for n in NAMES]


def mul(x, n):
    return x * n if isinstance(x, int) else pl.multiple_of(x * n, n)


def cp(src, dst, sem):
    return pltpu.make_async_copy(src, dst, sem)


def parts(src, dst):
    rows = dst.shape[0]
    n = rows if rows == TWO and len(dst.shape) > RING - 1 else RING if rows % (8 * RING) == 0 else 1
    m = rows // n
    return [(src.at[pl.ds(i * m, m)], dst.at[pl.ds(i * m, m)]) for i in range(n)] if n > 1 else [(src, dst)]


def batch(sem, *pairs):
    return [cp(src, dst, sem.at[i]) for i, (src, dst) in enumerate(t for pair in pairs for t in parts(*pair))]


def start(copies):
    for t in copies:
        t.start()


def wait(copies):
    for t in copies:
        t.wait()


def move(copies):
    start(copies)
    wait(copies)


def dma(*shape):
    return pltpu.SemaphoreType.DMA(shape)


def bf(*shape):
    return pltpu.VMEM(shape, BF16)


def fl(*shape):
    return pltpu.VMEM(shape, F32)


def when(cond):
    def deco(fn):
        pl.when(cond)(fn)
    return deco


def run(n, ins, outs, isem, osem, work, done=None, posts=None, late=()):
    posts = posts or {}

    def fetch(k, s):
        return batch(isem.at[s], *ins(k, s))

    def back(k, s):
        return batch(osem.at[s], *outs(k, s))

    start(fetch(0, 0))

    def step(k, _):
        s, nxt = low(k), k + 1
        is_late = functools.reduce(jnp.logical_or, [nxt == t for t in late], False)
        more = nxt < n
        wait(fetch(k, s))

        @when(jnp.logical_and(more, jnp.logical_not(is_late)))
        def _():
            start(fetch(nxt, flip(s)))
        if done is None:
            @when(k >= TWO)
            def _():
                wait(back(k, s))
        work(k, s)
        start(back(k, s))
        for t, fn in posts.items():
            when(k == t)(fn)
        if late:
            @when(is_late)
            def _():
                start(fetch(nxt, flip(s)))
        if done is not None:
            @when(k == 0)
            def _():
                wait(back(k, s))
                done(k, s)

            @when(k >= TWO)
            def _():
                wait(back(k - 1, flip(s)))
                done(k - 1, flip(s))
        return 0

    lax.fori_loop(0, n, step, 0)
    last = n - 1
    if done is None:
        wait(back(last - 1, flip(low(last))))
    wait(back(last, low(last)))
    if done is not None:
        done(last, low(last))


def kernel(cfg, x_in, g_in, w1, w2, vec, bup, *refs):
    TH, DM, DS, FB = cfg
    o = dict(zip(NAMES, refs[:len(NAMES)]))
    ssem, rsem, sums, sums_in, db, db_in = refs[len(NAMES):]
    DH, F2, FC, HT, T2 = high(DM), TWO * FB, RING * FB, high(TH), TWO * TH
    BN, ALLT = high(DH), TWO * RING * T2
    A, G, W1, W2 = o["A"], o["G"], o["W1"], o["W2"]
    r, c, d = lax.axis_index("row"), lax.axis_index("col"), lax.axis_index("dep")
    hp, hi = low(r), high(r)
    hn, e = flip(hi), flip(d)
    g = low(r + hi)
    gn = flip(g)
    u, v, q = r + 1 - TWO * hp, RING - 1 - r, (r + TWO) % RING
    R, L, far = (c + 1) % RING, (c + RING - 1) % RING, (c + TWO) % RING
    pos_r, pos_v, pos_u, pos_q = TWO * g + hi, TWO * g + hn, TWO * gn + hi, TWO * gn + hn
    c_lo, c_hi = low(c), high(c)

    ids, counts = {}, [0, 0]

    def name(key, n=1):
        ids[key] = counts[0]
        counts[0] += n

    def rid(key):
        return ids[key]

    for nm in "AG":
        for w in ("xr1", "xl1", "fr0", "fl0", "fr1", "fl1"):
            name(nm + w)
        for w in ("xr0", "xl0", "u"):
            name(nm + w, TWO)
        for t in "01":
            for w in "cLRxy":
                name(nm + "d" + t + w, TWO)
    for s in "uv":
        name("w1" + s, TWO * RING)
        name("w2" + s, TWO)
        name("f1" + s, RING)
        name("f2" + s)
    for s in ("w2d", "xf", "gf", "pv", "xo", "bg"):
        name(s)
    name("yo", TWO)
    name("bf", TWO)
    name("sum", STAGES)
    for s in ("w1d", "s1", "s2", "k1u"):
        name(s, RING)
    name("k1d", TWO)
    name("k2", TWO)
    for s in "YD":
        for w in ("p", "r", "l", "pr", "pl"):
            name(s + w, RING)

    pending = []
    dev_e, dev_R, dev_L = {"dep": e}, {"col": R}, {"col": L}

    def dev(row, core):
        return {"row": row, "dep": core}

    class Send:
        def __init__(self, fn, n=1):
            self.fn, self.n, self.sid = fn, n, counts[1]
            counts[1] += n
            pending.append(self)

        def desc(self, j=0):
            src, dst, rsid, device = self.fn(j)
            return pltpu.make_async_remote_copy(src_ref=src, dst_ref=dst, send_sem=ssem.at[self.sid + j], recv_sem=rsem.at[rsid],
                                                device_id=device, device_id_type=MESH)

        def start(self, j=0):
            self.desc(j).start()

        def all(self):
            for j in range(self.n):
                self.start(j)

    def same(ref, rsid, device):
        return Send(lambda j: (ref, ref, rsid, device))

    def arrived(dst, rsid):
        pltpu.make_async_remote_copy(src_ref=dst, dst_ref=dst, send_sem=ssem.at[0], recv_sem=rsem.at[rsid],
                                     device_id=dev_e, device_id_type=MESH).wait_recv()

    barrier = pltpu.get_barrier_semaphore()
    peers = [dev_e, dev_R, dev_L] + [dev(t, k) for t in (u, v) for k in BOTH]
    for p in peers:
        pl.semaphore_signal(barrier, inc=1, device_id=p, device_id_type=MESH)
    pl.semaphore_wait(barrier, len(peers))

    ARR = (("A", A), ("G", G))
    ROW = (hp, flip(hp))

    def ch(X, t, col, core, part=None):
        if part is None:
            return X.at[ROW[t], col, pl.ds(mul(core, TH), TH)]
        return X.at[ROW[t], col, pl.ds(pl.multiple_of(core * TH + part * HT, HT), HT)]

    def blk(k, n):
        return pl.ds(mul(k, n), n)

    def f_block(pos, core):
        gg, ii = high(pos), low(pos)
        return blk((flip(gg) * (RING - 1) * ii + gg * (1 + ii)) * TWO + core, FB)

    def w1_src(pos, core):
        return w1.at[:, f_block(pos, core)]

    def w1_dst(dd, row, pos):
        return W1.at[blk(dd * RING + row, DS), blk(pos, FB)]

    def send_w1(tag, row, *positions):
        for pos in positions:
            for core in BOTH:
                Send(lambda j, pos=pos, core=core: (w1_src(pos, core), w1_dst(d, r, pos), rid("w1" + tag) + d * RING + pos, dev(row, core))).start()

    def w2_part(pos, half):
        return W2.at[blk(pos, FB), blk(half, DH)]

    def send_w2(tag, row):
        for core in BOTH:
            Send(lambda j, core=core: (w2.at[blk(core, FB), :], w2_part(pos_r, d), rid("w2" + tag) + d, dev(row, core))).start()

    def wait_w2(tag, pos):
        for dd in BOTH:
            arrived(w2_part(pos, dd), rid("w2" + tag) + dd)

    XF, GF, PV = o["XF"], o["GF"], o["PV"]
    Send(lambda j: (g_in.at[blk(e, TH), :], GF.at[:, blk(d, DH)], rid("gf"), dev_e)).start()
    Send(lambda j: (x_in.at[blk(e, TH), :], XF.at[:, blk(d, DH)], rid("xf"), dev_e)).start()
    Send(lambda j: (vec, PV.at[:, blk(d, DH)], rid("pv"), dev_e)).start()
    OWN_TO = (("xr0", dev_R), ("xl0", dev_L), ("u", dev(u, d)), ("d0c", dev_e))
    send_w1("v", v, pos_v, pos_r)
    send_w1("u", u, pos_u, pos_q)
    for w, dv in OWN_TO:
        Send(lambda j, w=w, dv=dv: (g_in.at[blk(d, TH), :], G.at[hp, c, blk(d, TH), blk(d, DH)], rid("G" + w), dv)).start()

    RL = min(8 * RING, TH)

    def stats(x):
        mean = jnp.sum(x, axis=1, keepdims=True) / DM
        var = jnp.sum(x * x, axis=1, keepdims=True) / DM - mean * mean
        inv_std = lax.rsqrt(var + LN_EPS)
        return inv_std, (x - mean) * inv_std


    def own_part(xb, gb, ab, vb, b2, b3, sems, sems2):
        mine, other = blk(d, DH), blk(e, DH)
        ld = batch(sems, (g_in.at[blk(d, TH), :], gb.at[:, mine]), (x_in.at[blk(d, TH), :], xb.at[:, mine]), (vec, vb.at[:, mine]))
        start(ld)
        wait(ld)
        got = batch(sems, (GF.at[:, other], gb.at[:, other]), (XF.at[:, other], xb.at[:, other]), (PV.at[:, other], vb.at[:, other]))
        for ref, w in ((GF, "gf"), (XF, "xf"), (PV, "pv")):
            arrived(ref.at[:, other], rid(w))
            if ref is GF:
                for w, dv in OWN_TO:
                    Send(lambda j, w=w, dv=dv: (GF.at[:, blk(e, DH)], G.at[hp, c, blk(d, TH), blk(e, DH)], rid("G" + w) + 1, dv)).start()
        move(got)
        start(batch(sems2, (gb, ch(G, 0, c, d))))
        keep = batch(sems, (xb.at[:, mine], XF.at[:, mine]), (vb.at[:, mine], PV.at[:, mine]))
        start(keep)
        scale, shift = vb[0:1, :], vb[1:TWO, :]

        def rows(m, _):
            sl = blk(m, RL)
            ab[sl, :] = (stats(xb[sl, :].astype(F32))[1] * scale + shift).astype(BF16)
            return 0

        lax.fori_loop(0, TH // RL, rows, 0)
        wait(keep)
        move(batch(sems, (ab, ch(A, 0, c, d))))
        for w, dv in OWN_TO:
            Send(lambda j, w=w, dv=dv: (ch(A, 0, c, d), ch(A, 0, c, d), rid("A" + w), dv)).start()
        send_w2("u", u)
        send_w1("u", u, pos_r, pos_v)
        wait(batch(sems2, (gb, ch(G, 0, c, d))))
        wl = batch(sems, (w2.at[blk(d, FB), :], b3), (w1_src(0, d), b2.at[:, blk(0, FB)]))
        move(wl)
        move(batch(sems, *[(w1_src(pos, d), b2.at[:, blk(pos, FB)]) for pos in range(1, RING)]))
        move(batch(sems, (b3, w2_part(pos_r, d)), (b2, W1.at[blk(d * RING + r, DS), :])))

    pl.run_scoped(own_part, bf(TH, DM), bf(TH, DM), bf(TH, DM), fl(8, DM), bf(DS, FC), bf(FB, DH), dma(MANY), dma(MANY))
    for pos in range(RING):
        Send(lambda j, pos=pos: (w1_src(pos, e), w1_dst(d, r, pos), rid("w1d") + pos, dev_e)).start()
    Send(lambda j: (w2.at[blk(e, FB), :], w2_part(pos_r, d), rid("w2d"), dev_e)).start()

    fwd, par = {}, {}
    for nm, X in ARR:
        for t in BOTH:
            b = nm + "d" + str(t)
            fwd[nm, t] = [same(ch(X, t, L, d, 0), rid(nm + "fr" + str(t)), dev_R), same(ch(X, t, R, d, 1), rid(nm + "fl" + str(t)), dev_L),
                          same(ch(X, t, L, d), rid(b + "L"), dev_e), same(ch(X, t, R, d), rid(b + "R"), dev_e),
                          same(ch(X, t, far, d, 0), rid(b + "x"), dev_e), same(ch(X, t, far, d, 1), rid(b + "y"), dev_e)]
        par[nm] = [same(ch(X, 1, c, d), rid(nm + w), dv) for w, dv in (("xr1", dev_R), ("xl1", dev_L), ("d1c", dev_e))]

    def own_in(nm, X, t, col, w, core=d):
        if nm + w in ("Gxr0", "Gxl0", "Gu", "Gd0c"):
            for half, i in ((core, 0), (flip(core), 1)):
                arrived(X.at[ROW[t], col, blk(core, TH), blk(half, DH)], rid(nm + w) + i)
        else:
            arrived(ch(X, t, col, core), rid(nm + w))

    def pass_on(nm, X, t):
        to_r, to_l, d_l, d_r = fwd[nm, t][:RING]
        own_in(nm, X, t, L, "xr" + str(t))
        to_r.start()
        own_in(nm, X, t, R, "xl" + str(t))
        to_l.start()
        d_l.start()
        d_r.start()

    def from_u(nm, X):
        own_in(nm, X, 1, c, "u")
        for t in par[nm]:
            t.start()

    def far_in(nm, X, t):
        for part, w in zip(BOTH, ("fr", "fl")):
            arrived(ch(X, t, far, d, part), rid(nm + w + str(t)))
            fwd[nm, t][RING + part].start()

    def other_core(t, *which):
        for nm, X in ARR:
            b = nm + "d" + str(t)
            for w in which:
                if w == "far":
                    for part, z in zip(BOTH, "xy"):
                        arrived(ch(X, t, far, e, part), rid(b + z))
                else:
                    own_in(nm, X, t, {"c": c, "L": L, "R": R}[w], b[1:] + w, e)

    def hop(tag, row, device, *positions):
        out = []
        for pos in positions:
            out.append(Send(lambda j, pos=pos: (w1_dst(j, row, pos), w1_dst(j, row, pos), rid(tag) + low(pos) * TWO + j, device), TWO))
        return out

    f1v = hop("f1v", u, dev(v, d), pos_v, pos_r)
    f1u = hop("f1u", v, dev(u, d), pos_r, pos_v)
    q0, q1 = pl.ds(0, BN), pl.ds(BN, DM - BN)
    f2u = same(W2.at[blk(pos_v, FB), q0], rid("f2u"), dev(u, d))
    f2v = same(W2.at[blk(pos_u, FB), q1], rid("f2v"), dev(v, d))

    def w1_in(tag, row, pos):
        for dd in BOTH:
            arrived(w1_dst(dd, row, pos), rid("w1" + tag) + dd * RING + pos)

    def w1_rest(pos, tag):
        arrived(w1_dst(e, r, pos), rid("w1d") + pos)
        for j in BOTH:
            arrived(w1_dst(j, q, pos), rid(tag) + low(pos) * TWO + j)

    for pos in (pos_r, pos_v):
        w1_in("u", u, pos)
    for t in f1v:
        t.all()
    send_w2("v", v)
    send_w1("v", v, pos_q, pos_u)
    pass_on("G", G, 0)
    for pos in (pos_r, pos_v):
        w1_in("v", v, pos)
    for t in f1u:
        t.all()
    other_core(0, "c")
    arrived(w2_part(pos_r, e), rid("w2d"))
    w1_rest(pos_r, "f1v")

    RC = min(8 * RING, TH)

    def cd_block(a, gr, w1b, w2b, bias, cbuf, gbuf, h_out, dc_out, db, count_db):
        cbuf[:] = jnp.dot(a, w1b, preferred_element_type=F32)
        gbuf[:] = lax.dot_general(gr, w2b, NT, preferred_element_type=F32)

        def rows(m, acc):
            sl = blk(m, RC)
            pre = cbuf[sl, :] + bias
            sq = pre * pre
            th = jnp.tanh(GELU_K * (pre + GELU_C * pre * sq))
            half = 0.5 * (1.0 + th)
            slope = half + 0.5 * pre * (1.0 - th * th) * GELU_K * (1.0 + 3.0 * GELU_C * sq)
            dc = gbuf[sl, :] * slope
            h_out[sl, :] = (pre * half).astype(BF16)
            dc_out[sl, :] = dc.astype(BF16)
            return acc + jnp.sum(dc.reshape(RC // 8, 8, FB), axis=0)

        acc = lax.fori_loop(0, T2 // RC, rows, jnp.zeros((8, FB), F32))

        @when(count_db)
        def _():
            db[:] += acc

    def hidden(n, place, block, need, first, posts, late):
        def body(ab, gb, w1b, w2b, cbuf, gbuf, hb, cb, dbs, isem, osem, wsem):
            def weights(b):
                pos = block(b * first)[1]
                return batch(wsem.at[b], (W1.at[:, blk(pos, FB)], w1b.at[b]), (W2.at[blk(pos, FB), :], w2b.at[b]))

            def load(b):
                need(b)
                start(weights(b))

            load(0)
            dbs[:] = jnp.zeros_like(dbs)

            def ins(k, s):
                row, col, _ = place(k)
                return (A.at[row, col], ab.at[s]), (G.at[row, col], gb.at[s])

            def outs(k, s):
                row, col, _ = place(k)
                to_p, cols = block(k)[TWO:]
                at = (high(col), low(col), slice(None), cols)
                H, C = (o["HP"].at[row], o["CP"].at[row]) if to_p else (o["HQ"], o["CQ"])
                return (hb.at[s], H.at[at]), (cb.at[s], C.at[at])

            def work(k, s):
                b, pos = block(k)[:TWO]
                for t in BOTH:
                    @when(k == t * first)
                    def _():
                        wait(weights(t))
                cd_block(ab[s], gb[s], w1b[b], w2b[b], bup[:, f_block(pos, d)].astype(F32), cbuf, gbuf, hb.at[s], cb.at[s], dbs.at[b], place(k)[TWO])

            run(n, ins, outs, isem, osem, work, posts={k: functools.partial(fn, load) for k, fn in posts.items()}, late=late)
            move(batch(wsem.at[0], *[(dbs.at[b], o["DB"].at[:, blk(block(b * first)[1], FB)]) for b in BOTH]))

        pl.run_scoped(body, bf(TWO, T2, DM), bf(TWO, T2, DM), bf(TWO, DM, FB), bf(TWO, FB, DM), fl(T2, FB), fl(T2, FB),
                      bf(TWO, T2, FB), bf(TWO, T2, FB), fl(TWO, 8, FB), dma(TWO, MANY), dma(TWO, MANY), dma(TWO, MANY))

    five, ten = RING + 1, TWO * RING + TWO

    def place1(k):
        early = k < ten
        k5, k2 = k % five, high(k - ten) + 1
        mine = jnp.logical_and(early, k5 < RING)
        m = jnp.where(early, k5 % RING, k2)
        return jnp.where(mine, hp, flip(hp)), (c + m + high(m) * (five - TWO * m)) % RING, mine

    def block1(k):
        b = jnp.where(k < ten, k // five % TWO, low(k))
        ii = jnp.where(b == 0, hi, hn)
        return b, TWO * g + ii, True, blk(ii, FB)

    def need1(b):
        if b:
            wait_w2("v", pos_v)
            f2u.start()
            w1_rest(pos_v, "f1v")

    def post0(load):
        pass_on("A", A, 0)
        from_u("G", G)
        other_core(0, "L", "R")

    def post2(load):
        far_in("G", G, 0)
        from_u("A", A)
        far_in("A", A, 0)
        other_core(0, "far")

    def post9(load):
        pass_on("A", A, 1)
        wait_w2("u", pos_u)
        f2v.start()
        other_core(1, "L", "R")

    def post13(load):
        start(early())
        far_in("G", G, 1)
        far_in("A", A, 1)
        other_core(1, "far")

    ahead = []

    def early():
        rb, sem = ahead
        return batch(sem, (o["CP"].at[hp], rb.at[hp]),
                     *[(o["CP"].at[flip(hp), high(t), low(t)], rb.at[flip(hp), high(t), low(t)]) for t in (c, R)])

    def rest():
        rb, sem = ahead
        return batch(sem.at[pl.ds(MANY, MANY)], *[(o["CP"].at[flip(hp), high(t), low(t)], rb.at[flip(hp), high(t), low(t)]) for t in (L, far)])

    posts1 = {0: post0, TWO: post2, RING - 1: lambda load: other_core(1, "c"), RING: lambda load: load(1),
              five: lambda load: pass_on("G", G, 1), ten - 1: post9, ten + RING - 1: post13}

    S1, R1, S2, R2, K1, K2, OUT1, OUT2 = [o[t] for t in ("S1", "R1", "S2", "R2", "K1", "K2", "OUT1", "OUT2")]
    s1 = Send(lambda j: (S1.at[j], R1.at[j], rid("s1") + j, dev(v, d)), RING)
    s2 = Send(lambda j: (S2.at[:, blk(j, BN)], R2.at[:, blk(j, BN)], rid("s2") + j, dev(v, d)), RING)

    def dw1_cols(k, pair, first):
        j = first + (1 - TWO * first) * high(k)
        return blk(low(k) * RING + TWO * pair + j, DS)

    def grad(left, right, left_shape, right_shape, resident, out_shape, outs, done, recv=None, posts=None, mid=None, pre=None):
        rows, width = out_shape

        def body(acc, ob, nb, isem, osem, wsem, lb, rb):
            if pre is not None:
                stay = early() + rest()
            else:
                stay = batch(wsem, resident((lb, rb)))
                start(stay)

            def ins(k, s):
                return (left(k), lb.at[s]) if right is None else (right(k), rb.at[s]),

            def work(k, s):
                @when(k == 0)
                def _():
                    wait(stay)
                x, y = (lb[s], rb[:]) if right is None else (lb[:], rb[s])
                val = lax.dot_general(x.reshape(ALLT, rows), y.reshape(ALLT, width), TN, preferred_element_type=F32)
                if recv is None:
                    ob[s] = val
                else:
                    acc[:] = val
                    if mid:
                        when(k == RING - 1)(mid)
                    ref, rsid = recv(k)
                    arrived(ref, rsid)
                    move(batch(wsem, (ref, nb)))
                    ob[s] = (acc[:] + nb[:]).astype(BF16)

            run(RING, ins, lambda k, s: ((ob.at[s], outs(k)),), isem, osem, work, done=lambda k, s: done(k, ob.at[s], wsem), posts=posts)

        extra = out_shape if recv else (8, BN)
        kinds = [fl(*extra), pltpu.VMEM(SLOTS + out_shape, BF16 if recv else F32), fl(*extra), dma(TWO, MANY), dma(TWO, MANY), dma(MANY)]
        if pre is not None:
            pl.run_scoped(lambda *bufs: body(*bufs, pre), *kinds, bf(*left_shape))
        else:
            pl.run_scoped(body, *kinds, bf(*left_shape), bf(*right_shape))

    PT, PTS = (TWO, RING, T2), (TWO, TWO, TWO, T2)

    def grad1(pair, first, outs, done, recv=None, pre=None):
        grad(lambda k: A.at[:, :, :, dw1_cols(k, pair, first)], None, SLOTS + PT + (DS,), PTS + (F2,), lambda b: (o["CP"], b[1]),
             (DS, F2), outs, done, recv, pre=pre)

    def grad2(pair, outs, done, recv=None, posts=None, mid=None):
        grad(None, lambda k: G.at[:, :, :, blk(k, BN)], PTS + (FB,), SLOTS + PT + (BN,), lambda b: (o["HP"].at[:, :, :, :, blk(pair, FB)], b[0]),
             (FB, BN), outs, done, recv, posts, mid)

    def phase1(rb, sem):
        ahead.extend((rb, sem))
        hidden(ten + RING + TWO, place1, block1, need1, five, posts1, (1, RING - 1, RING, ten, ten + RING))
        start(rest())
        grad1(hn, hp, lambda k: S1.at[k], lambda k, ob, sem: s1.start(k), pre=rb)

    pl.run_scoped(phase1, bf(*PTS, F2), dma(TWO * MANY))

    def block2(k):
        b = k // RING
        ii = jnp.where(b == 0, hi, hn)
        return b, TWO * gn + ii, False, blk(ii, FB)

    def need2(b):
        pos = pos_q if b else pos_u
        w1_in("u", u, pos)
        w1_in("v", v, pos)
        w1_rest(pos, "f1u")
        if b:
            arrived(W2.at[blk(pos_q, FB), q1], rid("f2v"))
            arrived(W2.at[blk(pos_q, FB), q0], rid("f2u"))

    hidden(TWO * RING, lambda k: (hp, k % RING, k >= 0), block2, need2, RING, {TWO: lambda load: load(1)}, ())

    def region(s, nt, XP, XQ, PX, RX):
        Q1, Q2, RF, RR = [o[s + t] for t in ("Q1", "Q2", "RF", "RX")]
        ex = Send(lambda j: (PX.at[:, :, :, blk(j, BN)], RX.at[:, :, :, blk(j, BN)], rid(s + "p") + j, dev_e), RING)
        away = flip(c_hi)
        far_r = Send(lambda j: (Q1.at[away, blk(0, HT), blk(j, BN)], RF.at[away, :, blk(j, BN)], rid(s + "r") + j, dev_R), RING)
        far_l = Send(lambda j: (Q1.at[away, blk(1, HT), blk(j, BN)], RF.at[away, :, blk(j, BN)], rid(s + "l") + j, dev_L), RING)
        pm_r = Send(lambda j: (Q2.at[high(R), :, blk(j, BN)], RR.at[0, :, blk(j, BN)], rid(s + "pr") + j, dev_R), RING)
        pm_l = Send(lambda j: (Q2.at[high(L), :, blk(j, BN)], RR.at[1, :, blk(j, BN)], rid(s + "pl") + j, dev_L), RING)
        wshape = (BN, FC) if nt else (FC, BN)
        mine, other = blk(d, TH), blk(e, TH)

        def wsrc(j):
            return W1.at[blk(j, BN), :] if nt else W2.at[:, blk(j, BN)]

        def wdot(out, p_ref, q_ref, wref):
            for ref, half in ((p_ref, g), (q_ref, gn)):
                x, sel = ref[:].reshape(-1, F2), blk(half, F2)
                if nt:
                    val = lax.dot_general(x, wref[:, sel], NT, preferred_element_type=F32)
                else:
                    val = jnp.dot(x, wref[sel, :], preferred_element_type=F32)
                val = val.reshape(out.shape)
                out[:] = val if ref is p_ref else out[:] + val

        def first(lop, loq, lfp, lfq, wb, ob, ab, qb, wsem, lsem, osem, asem):
            def wcp(j):
                return batch(wsem.at[j % RING], (wsrc(j), wb.at[j % RING]))

            lds = batch(lsem, (XP.at[hp, :, :, other], lop), (XQ.at[:, :, other], loq), (XP.at[hp, :, c_lo, mine], lfp), (XQ.at[:, c_lo, mine], lfq))
            start(wcp(0) + lds)
            wait(lds)

            def step(j, _):
                o1 = batch(osem, (ob, PX.at[:, :, :, blk(j, BN)]))

                @when(j < RING)
                def _():
                    wait(wcp(j))

                    @when(j < RING - 1)
                    def _():
                        start(wcp(j + 1))
                    wdot(ob, lop, loq, wb.at[j % RING])
                    start(o1)

                @when(j >= LAG)
                def _():
                    k = j - LAG
                    arrived(RX.at[:, :, :, blk(k, BN)], rid(s + "p") + k)
                    add = batch(asem, (RX.at[:, c_lo, :, blk(k, BN)], ab))
                    start(add)
                    wdot(qb, lfp, lfq, wb.at[k % RING])
                    wait(add)
                    qb[:] += ab[:]
                    start(batch(lsem, (qb, Q1.at[:, :, blk(k, BN)])))

                @when(j < RING)
                def _():
                    wait(o1)
                    ex.start(j)

                @when(j >= LAG)
                def _():
                    k = j - LAG
                    wait(batch(lsem, (qb, Q1.at[:, :, blk(k, BN)])))
                    far_r.start(k)
                    far_l.start(k)
                return 0

            lax.fori_loop(0, RING + LAG, step, 0)

        def second(lp, lq, wb, ab, fb, ob, lsem, isem, osem):
            lds = batch(lsem, (XP.at[hp, :, flip(c_lo), mine], lp), (XQ.at[:, flip(c_lo), mine], lq))
            start(lds)

            def need(k):
                arrived(RF.at[high(R), :, blk(k, BN)], rid(s + "r") + k)
                arrived(RF.at[high(L), :, blk(k, BN)], rid(s + "l") + k)

            for k in range(RING):
                need(k)
            wait(lds)

            def ins(k, sl):
                return (wsrc(k), wb.at[sl]), (RX.at[:, flip(c_lo), :, blk(k, BN)], ab.at[sl]), (RF.at[:, :, blk(k, BN)], fb.at[sl])

            def work(k, sl):
                wdot(ob.at[sl], lp, lq, wb.at[sl])
                ob[sl] += ab[sl]
                for col, part in ((R, 0), (L, 1)):
                    ob[sl, high(col), part * HT:(part + 1) * HT, :] += fb[sl, high(col)]

            def done(k, sl):
                pm_r.start(k)
                pm_l.start(k)

            run(RING, ins, lambda k, sl: ((ob.at[sl], Q2.at[:, :, blk(k, BN)]),), isem, osem, work, done=done)

        def run_first():
            pl.run_scoped(first, bf(TWO, TWO, TH, F2), bf(TWO, TWO, TH, F2), bf(TWO, TH, F2), bf(TWO, TH, F2), bf(RING, *wshape),
                          fl(TWO, TWO, TH, BN), fl(TWO, TH, BN), fl(TWO, TH, BN), dma(RING, RING), dma(MANY), dma(MANY), dma(MANY))

        def run_second():
            pl.run_scoped(second, bf(TWO, TH, F2), bf(TWO, TH, F2), bf(TWO, *wshape), fl(TWO, TWO, TH, BN), fl(TWO, TWO, HT, BN),
                          fl(TWO, TWO, TH, BN), dma(MANY), dma(TWO, MANY), dma(TWO, MANY))

        def come(j):
            arrived(RR.at[0, :, blk(j, BN)], rid(s + "pr") + j)
            arrived(RR.at[1, :, blk(j, BN)], rid(s + "pl") + j)
        return run_first, run_second, come

    y1, y2, y_come = region("Y", False, o["HP"], o["HQ"], o["PY"], o["RY"])
    d1, d2, d_come = region("D", True, o["CP"], o["CQ"], o["PD"], o["RD"])
    d1()
    y1()
    d2()
    grad2(hn, lambda k: S2.at[:, blk(k, BN)], lambda k, ob, sem: s2.start(k))
    y2()

    def piece(ii):
        return slice(ii * FB, (ii + 1) * FB)

    k1u = [Send(lambda m, ii=ii: (K1.at[m, :, piece(ii)], OUT1.at[:, f_block(TWO * g + ii, d)], rid("k1u") + d * TWO + ii, dev(u, m)), TWO)
           for ii in BOTH]
    k1d = [Send(lambda m, ii=ii: (K1.at[TWO + e, :, piece(ii)], OUT1.at[:, f_block(TWO * g + ii, d)], rid("k1d") + ii, dev_e)) for ii in BOTH]

    def done1(k, ob, sem):
        @when(k < TWO)
        def _():
            for t in k1u:
                t.start(k)

        @when(k == TWO + e)
        def _():
            for t in k1d:
                t.start()

        @when(k == TWO + d)
        def _():
            move(batch(sem, *[(ob.at[:, piece(ii)], OUT1.at[:, f_block(TWO * g + ii, d)]) for ii in BOTH]))

    def out2_at(core, jj):
        return OUT2.at[blk(core, FB), blk(jj, BN)]

    k2 = Send(lambda jj: (K2.at[TWO * e + jj], out2_at(d, jj), rid("k2") + jj, dev_e), TWO)

    def done2(k, ob, sem):
        @when(high(k) == d)
        def _():
            move(batch(sem, (ob, out2_at(d, low(k)))))

        @when(high(k) == e)
        def _():
            k2.start(low(k))

    grad1(hi, flip(hp), lambda k: K1.at[k], done1, lambda k: (R1.at[k], rid("s1") + k))

    RX_, OUTX, XO, OUTY, YO, BG, SO = [o[t] for t in ("DRX", "OUTX", "XO", "OUTY", "YO", "BG", "SO")]
    xo = Send(lambda j: (XO, OUTX.at[blk(d, TH), :], rid("xo"), dev_e))
    stages = [dev_e, dev(u, d), dev(v, d), {"col": c + 1 - TWO * c_lo}, {"col": RING - 1 - c}]
    assert len(stages) == STAGES
    sum_send = [Send(lambda j, k=k, dv=dv: (sums.at[k], sums_in.at[k], rid("sum") + k, dv))
                for k, dv in enumerate(stages)]
    bsend = [Send(lambda j, k=k, dv=dv: (db.at[k], db_in.at[k], rid("bf") + k, dv)) for k, dv in enumerate((dev(u, d), dev(v, d)))]
    bg = Send(lambda j: (BG.at[d], BG.at[d], rid("bg"), dev_e))

    def finish_dx(q1b, rlb, rrb, xb, gb, vb, xob, acc, dbb, isem, osem, wsem):
        RB = min(8 * RING, high(TH))
        par_ = batch(wsem, (PV, vb), (o["DB"], dbb))
        start(par_)
        for j in range(RING):
            d_come(j)
        acc[:] = jnp.zeros_like(acc)

        def ins(k, s):
            rows = blk(k, RB)
            return ((o["DQ1"].at[c_hi, rows], q1b.at[s]), (RX_.at[0, rows], rlb.at[s]), (RX_.at[1, rows], rrb.at[s]), (XF.at[rows, :], xb.at[s]),
                    (G.at[hp, c, pl.ds(pl.multiple_of(d * TH + k * RB, RB), RB), :], gb.at[s]))

        def outs(k, s):
            return ((xob.at[s, :, blk(d, DH)], OUTX.at[pl.ds(pl.multiple_of(d * TH + k * RB, RB), RB), :]),
                    (xob.at[s, :, blk(e, DH)], XO.at[blk(k, RB), :]))

        def fold(x):
            return jnp.sum(x.reshape(RB // 8, 8, DM), axis=0)

        def work(k, s):
            @when(k == 0)
            def _():
                wait(par_)
            da = q1b[s] + rlb[s] + rrb[s]
            inv_std, xhat = stats(xb[s].astype(F32))
            gr = gb[s].astype(F32)
            val = da * vb[0:1, :]
            m1 = jnp.sum(val, axis=1, keepdims=True) / DM
            m2 = jnp.sum(val * xhat, axis=1, keepdims=True) / DM
            xob[s] = (gr + inv_std * (val - m1 - xhat * m2)).astype(BF16)
            for i, t in enumerate((da * xhat, da, gr)):
                acc[i] += fold(t)

        run(TH // RB, ins, outs, isem, osem, work)
        xo.start()
        for i in range(RING - 1):
            row = jnp.sum(acc[i], axis=0, keepdims=True)
            acc[i, 0:1, :] = row
        for i in range(RING - 1):
            sums[STAGES, i:i + 1, :] = acc[i, 0:1, blk(d, DH)]
            sums[0, i:i + 1, :] = acc[i, 0:1, blk(e, DH)]
        db[0, 0:1, :] = jnp.sum(dbb[:], axis=0, keepdims=True)
        sum_send[0].start()

    def stage(k):
        arrived(sums_in.at[k], rid("sum") + k)
        sums[STAGES] += sums_in[k]
        if k in (1, TWO):
            arrived(db_in.at[k - 1], rid("bf") + k - 1)
            db[k] = db[k - 1] + db_in[k - 1]
        if k < STAGES - 1:
            sums[k + 1] = sums[STAGES]
            sum_send[k + 1].start()
        if k < TWO:
            bsend[k].start()

    def sums_out(wsem):
        stage(STAGES - 1)
        move(batch(wsem, (sums.at[STAGES], SO), (db.at[TWO], BG.at[d])))
        bg.start()

    def dx_all():
        RB = min(8 * RING, high(TH))
        pl.run_scoped(finish_dx, fl(TWO, RB, DM), fl(TWO, RB, DM), fl(TWO, RB, DM), bf(TWO, RB, DM), bf(TWO, RB, DM), fl(8, DM),
                      bf(TWO, RB, DM), fl(RING - 1, 8, DM), fl(8, FC), dma(TWO, MANY + RING), dma(TWO, MANY), dma(MANY))

    dx_all()

    def outy_at(core, jj):
        return OUTY.at[blk(core, TH), blk(jj, BN)]

    yo = Send(lambda jj: (YO.at[TWO * e + jj], outy_at(d, jj), rid("yo") + jj, dev_e), TWO)

    def last_part(q1b, xb, vb, rxb, yb, sem, sem2):
        def finish_y(k):
            cols = blk(k, BN)
            here = batch(sem, (o["YQ1"].at[c_hi, :, cols], q1b), (XF.at[:, cols], xb), (PV.at[:, cols], vb))
            start(here)
            y_come(k)
            move(batch(sem2, (o["YRX"].at[:, :, cols], rxb)))
            wait(here)
            yb[:] = (xb[:].astype(F32) + (q1b[:] + rxb[0] + rxb[1]) + vb[TWO:TWO + 1, :]).astype(BF16)

            @when(d == high(k))
            def _():
                move(batch(sem, (yb, outy_at(high(k), low(k)))))

            @when(e == high(k))
            def _():
                move(batch(sem, (yb, YO.at[k])))
                yo.start(low(k))

        def third():
            stage(TWO)
            finish_y(0)
            stage(RING - 1)
            finish_y(1)
            finish_y(TWO)

        def mid():
            sums_out(sem)
            finish_y(RING - 1)

        posts = {k: functools.partial(stage, k) for k in BOTH}
        posts[TWO] = third
        grad2(hi, lambda k: K2.at[k], done2, lambda k: (R2.at[:, blk(k, BN)], rid("s2") + k), posts, mid)

    pl.run_scoped(last_part, fl(TH, BN), bf(TH, BN), fl(8, BN), fl(TWO, TH, BN), bf(TH, BN), dma(MANY), dma(MANY))

    arrived(OUTX.at[blk(e, TH), :], rid("xo"))
    arrived(BG.at[e], rid("bg"))
    for ii in BOTH:
        arrived(outy_at(e, ii), rid("yo") + ii)
        for dd in BOTH:
            arrived(OUT1.at[:, f_block(TWO * gn + ii, dd)], rid("k1u") + dd * TWO + ii)
        arrived(OUT1.at[:, f_block(TWO * g + ii, e)], rid("k1d") + ii)
        arrived(out2_at(e, ii), rid("k2") + ii)
    for t in pending:
        for j in range(t.n):
            t.desc(j).wait_send()
    assert tuple(counts) == SEMS, counts


SEMS = (169, 147)


def solution(mesh):
    nr, nc, nd = mesh.shape["row"], mesh.shape["col"], mesh.shape["dep"]
    assert nr == 4 and nc == 4 and nd == 2
    tok_spec = P(("part", "row", "col"), "dep")
    vec_dep = P("dep")
    part_dep = P(("part", "dep"))
    in_specs = (tok_spec, vec_dep, vec_dep, P(("dep", "row"), "col"), P("col"), P(("col", "row"), "dep"), vec_dep, tok_spec)
    out_specs = (tok_spec, tok_spec, P(("part", "dep", "row"), "col"), P(("part", "col")), P(("part", "col", "row"), "dep"), part_dep, part_dep, part_dep)

    def local_step(x_in, ln_scale, ln_shift, w_up, b_up, w_down, b_down, y_grad):
        th, dhalf = x_in.shape[0] // 2, x_in.shape[1]
        ds_, fb = w_up.shape[0], w_up.shape[1] // 8
        vec = jnp.stack([ln_scale, ln_shift, b_down.astype(F32)] + [jnp.zeros_like(ln_scale)] * 5)

        cfg = (th, 2 * dhalf, ds_, fb)
        outs = pl.pallas_call(
            functools.partial(kernel, cfg),
            name="mlp_layer",
            out_shape=buffers(*cfg),
            in_specs=[pl.BlockSpec(memory_space=pl.ANY)] * 5 + [pl.BlockSpec(memory_space=pltpu.VMEM)],
            out_specs=[pl.BlockSpec(memory_space=pl.ANY)] * len(NAMES),
            scratch_shapes=[dma(SEMS[1]), dma(SEMS[0]), fl(STAGES + 1, 8, dhalf), fl(STAGES, 8, dhalf), fl(3, 8, 4 * fb), fl(2, 8, 4 * fb)],
            compiler_params=pltpu.CompilerParams(collective_id=0, has_side_effects=True, vmem_limit_bytes=62 * 1024 * 1024),
        )(x_in, y_grad, w_up, w_down, vec, b_up.reshape(1, 8 * fb))
        o = dict(zip(NAMES, outs))
        db = o["BG"][:, 0].reshape(2, 4, fb)
        b_up_grad = jnp.stack([db[:, k] for k in (0, 2, 3, 1)]).reshape(8 * fb)
        return (o["OUTY"], o["OUTX"], o["OUT1"], b_up_grad, o["OUT2"], o["SO"][2], o["SO"][0], o["SO"][1])

    return jax.shard_map(local_step, mesh=mesh, in_specs=in_specs, out_specs=out_specs, check_vma=False)
```

```python
import functools

import jax
import jax.numpy as jnp
from jax import lax
from jax.experimental import pallas as pl
from jax.experimental.pallas import tpu as pltpu
from jax.sharding import PartitionSpec as P

LN_EPS = 1e-5
GELU_K = 0.7978845608028654
GELU_C = 0.044715
F32 = jnp.float32
BF16 = jnp.bfloat16
MESH = pl.DeviceIdType.MESH

NAMES = ("A", "G", "W1", "W2", "HP", "HQ", "CP", "CQ", "DB",
         "PY", "RY", "YQ1", "YQ2", "YRF", "YRX", "PD", "RD", "DQ1", "DQ2", "DRF", "DRX",
         "S1", "R1", "S2", "R2", "K1", "K2", "OUT1", "OUT2", "XF", "GF", "PV", "YO", "XO", "OUTY", "OUTX", "BG", "SO")
TWO, RING, STAGES, MANY = 2, 4, 5, 16
LAG = 2
BOTH, SLOTS = (0, 1), (2,)
NT = (((1,), (1,)), ((), ()))
TN = (((0,), (0,)), ((), ()))


def flip(x):
    return 1 - x


def low(x):
    return x % 2


def high(x):
    return x // 2


def buffers(TH, DM, DS, FB):
    F2, FC, T2 = 2 * FB, 4 * FB, 2 * TH
    pair = (TWO, TWO)
    shapes = {
        "A": ((TWO, RING, T2, DM), BF16), "W1": ((DM, FC), BF16), "W2": ((FC, DM), BF16),
        "HP": (SLOTS + pair + (T2, F2), BF16), "HQ": (pair + (T2, F2), BF16), "DB": ((8, FC), F32),
        "S1": ((RING, DS, F2), F32), "S2": ((FB, DM), F32),
        "K1": ((RING, DS, F2), BF16), "K2": ((RING, FB, high(DM) // TWO), BF16),
        "OUT1": ((DS, 8 * FB), BF16), "OUT2": ((F2, high(DM)), BF16),
        "XF": ((TH, DM), BF16), "GF": ((TH, DM), BF16), "PV": ((RING - 1, 1, DM), F32), "YO": ((RING, TH, high(DM) // TWO), BF16),
        "XO": ((TH, high(DM)), BF16), "OUTY": ((T2, high(DM)), BF16), "OUTX": ((T2, high(DM)), BF16),
        "BG": (SLOTS + (RING, 8, FB), F32), "SO": ((8, high(DM)), F32),
    }
    for new, old in (("G", "A"), ("CP", "HP"), ("CQ", "HQ"), ("R1", "S1"), ("R2", "S2")):
        shapes[new] = shapes[old]
    for p, s in (("PY", "Y"), ("PD", "D")):
        shapes[p] = shapes["R" + s] = (pair + (TH, DM), F32)
        for q in ("Q1", "Q2", "RX"):
            shapes[s + q] = (SLOTS + (TH, DM), F32)
        shapes[s + "RF"] = (SLOTS + (high(TH), DM), F32)
    return [jax.ShapeDtypeStruct(*shapes[n]) for n in NAMES]


def mul(x, n):
    return x * n if isinstance(x, int) else pl.multiple_of(x * n, n)


def cp(src, dst, sem):
    return pltpu.make_async_copy(src, dst, sem)


def parts(src, dst):
    rows = dst.shape[0]
    n = rows if rows == TWO and len(dst.shape) > RING - 1 else RING if rows % (8 * RING) == 0 else 1
    m = rows // n
    return [(src.at[pl.ds(i * m, m)], dst.at[pl.ds(i * m, m)]) for i in range(n)] if n > 1 else [(src, dst)]


def batch(sem, *pairs):
    return [cp(src, dst, sem.at[i]) for i, (src, dst) in enumerate(t for pair in pairs for t in parts(*pair))]


def start(copies):
    for t in copies:
        t.start()


def wait(copies):
    for t in copies:
        t.wait()


def move(copies):
    start(copies)
    wait(copies)


def dma(*shape):
    return pltpu.SemaphoreType.DMA(shape)


def bf(*shape):
    return pltpu.VMEM(shape, BF16)


def fl(*shape):
    return pltpu.VMEM(shape, F32)


def when(cond):
    def deco(fn):
        pl.when(cond)(fn)
    return deco


def run(n, ins, outs, isem, osem, work, done=None, posts=None, late=()):
    posts = posts or {}

    def fetch(k, s):
        return batch(isem.at[s], *ins(k, s))

    def back(k, s):
        return batch(osem.at[s], *outs(k, s))

    start(fetch(0, 0))

    def step(k, _):
        s, nxt = low(k), k + 1
        is_late = functools.reduce(jnp.logical_or, [nxt == t for t in late], False)
        more = nxt < n
        wait(fetch(k, s))

        @when(jnp.logical_and(more, jnp.logical_not(is_late)))
        def _():
            start(fetch(nxt, flip(s)))
        if done is None:
            @when(k >= TWO)
            def _():
                wait(back(k, s))
        work(k, s)
        start(back(k, s))
        for t, fn in posts.items():
            when(k == t)(fn)
        if late:
            @when(is_late)
            def _():
                start(fetch(nxt, flip(s)))
        if done is not None:
            @when(k == 0)
            def _():
                wait(back(k, s))
                done(k, s)

            @when(k >= TWO)
            def _():
                wait(back(k - 1, flip(s)))
                done(k - 1, flip(s))
        return 0

    lax.fori_loop(0, n, step, 0)
    last = n - 1
    if done is None:
        wait(back(last - 1, flip(low(last))))
    wait(back(last, low(last)))
    if done is not None:
        done(last, low(last))


def kernel(cfg, x_in, g_in, w1, w2, gam, bet, bdn, bup, *refs):
    TH, DM, DS, FB = cfg
    o = dict(zip(NAMES, refs[:len(NAMES)]))
    ssem, rsem, sums, sums_in, db, db_in = refs[len(NAMES):]
    DH, F2, FC, HT, T2 = high(DM), TWO * FB, RING * FB, high(TH), TWO * TH
    BN, ALLT = high(DH), TWO * RING * T2
    A, G, W1, W2 = o["A"], o["G"], o["W1"], o["W2"]
    r, c, d = lax.axis_index("row"), lax.axis_index("col"), lax.axis_index("dep")
    hp, hi = low(r), high(r)
    hn, e = flip(hi), flip(d)
    g = low(r + hi)
    gn = flip(g)
    u, v, q = r + 1 - TWO * hp, RING - 1 - r, (r + TWO) % RING
    R, L, far = (c + 1) % RING, (c + RING - 1) % RING, (c + TWO) % RING
    pos_r, pos_v, pos_u, pos_q = TWO * g + hi, TWO * g + hn, TWO * gn + hi, TWO * gn + hn
    c_lo, c_hi = low(c), high(c)

    ids, counts = {}, [0, 0]

    def name(key, n=1):
        ids[key] = counts[0]
        counts[0] += n

    def rid(key):
        return ids[key]

    for nm in "AG":
        for w in ("xr1", "xl1", "fr0", "fl0", "fr1", "fl1"):
            name(nm + w)
        for w in ("xr0", "xl0", "u"):
            name(nm + w, TWO)
        for t in "01":
            for w in "cLRxy":
                name(nm + "d" + t + w, TWO)
    for s in "uv":
        name("w1" + s, TWO * RING)
        name("w2" + s, TWO)
        name("f1" + s, RING)
        name("f2" + s)
    name("pv", RING - 1)
    for s in ("w2d", "xf", "gf", "xo", "bg"):
        name(s)
    name("yo", TWO)
    name("bf", TWO)
    name("sum", STAGES)
    for s in ("w1d", "s1", "s2", "k1u"):
        name(s, RING)
    name("k1d", TWO)
    name("k2", TWO)
    for s in "YD":
        for w in ("p", "r", "l", "pr", "pl"):
            name(s + w, RING)

    pending = []
    dev_e, dev_R, dev_L = {"dep": e}, {"col": R}, {"col": L}

    def dev(row, core):
        return {"row": row, "dep": core}

    class Send:
        def __init__(self, fn, n=1):
            self.fn, self.n, self.sid = fn, n, counts[1]
            counts[1] += n
            pending.append(self)

        def desc(self, j=0):
            src, dst, rsid, device = self.fn(j)
            return pltpu.make_async_remote_copy(src_ref=src, dst_ref=dst, send_sem=ssem.at[self.sid + j], recv_sem=rsem.at[rsid],
                                                device_id=device, device_id_type=MESH)

        def start(self, j=0):
            self.desc(j).start()

        def all(self):
            for j in range(self.n):
                self.start(j)

    def same(ref, rsid, device):
        return Send(lambda j: (ref, ref, rsid, device))

    def arrived(dst, rsid):
        pltpu.make_async_remote_copy(src_ref=dst, dst_ref=dst, send_sem=ssem.at[0], recv_sem=rsem.at[rsid],
                                     device_id=dev_e, device_id_type=MESH).wait_recv()

    barrier = pltpu.get_barrier_semaphore()
    peers = [dev_e, dev_R, dev_L] + [dev(t, k) for t in (u, v) for k in BOTH]
    for p in peers:
        pl.semaphore_signal(barrier, inc=1, device_id=p, device_id_type=MESH)
    pl.semaphore_wait(barrier, len(peers))

    ARR = (("A", A), ("G", G))
    ROW = (hp, flip(hp))

    def ch(X, t, col, core, part=None):
        if part is None:
            return X.at[ROW[t], col, pl.ds(mul(core, TH), TH)]
        return X.at[ROW[t], col, pl.ds(pl.multiple_of(core * TH + part * HT, HT), HT)]

    def blk(k, n):
        return pl.ds(mul(k, n), n)

    def f_block(pos, core):
        gg, ii = high(pos), low(pos)
        return blk((flip(gg) * (RING - 1) * ii + gg * (1 + ii)) * TWO + core, FB)

    def w1_src(pos, core):
        return w1.at[:, f_block(pos, core)]

    def w1_dst(dd, row, pos):
        return W1.at[blk(dd * RING + row, DS), blk(pos, FB)]

    def send_w1(tag, row, *positions):
        for pos in positions:
            for core in BOTH:
                Send(lambda j, pos=pos, core=core: (w1_src(pos, core), w1_dst(d, r, pos), rid("w1" + tag) + d * RING + pos, dev(row, core))).start()

    def w2_part(pos, half):
        return W2.at[blk(pos, FB), blk(half, DH)]

    def send_w2(tag, row):
        for core in BOTH:
            Send(lambda j, core=core: (w2.at[blk(core, FB), :], w2_part(pos_r, d), rid("w2" + tag) + d, dev(row, core))).start()

    def wait_w2(tag, pos):
        for dd in BOTH:
            arrived(w2_part(pos, dd), rid("w2" + tag) + dd)

    XF, GF, PV = o["XF"], o["GF"], o["PV"]
    Send(lambda j: (g_in.at[blk(e, TH), :], GF.at[:, blk(d, DH)], rid("gf"), dev_e)).start()
    Send(lambda j: (x_in.at[blk(e, TH), :], XF.at[:, blk(d, DH)], rid("xf"), dev_e)).start()
    VEC = (gam, bet, bdn)
    for i, ref in enumerate(VEC):
        Send(lambda j, i=i, ref=ref: (ref, PV.at[i, :, blk(d, DH)], rid("pv") + i, dev_e)).start()
    OWN_TO = (("xr0", dev_R), ("xl0", dev_L), ("u", dev(u, d)), ("d0c", dev_e))
    send_w1("v", v, pos_v, pos_r)
    send_w1("u", u, pos_u, pos_q)
    for w, dv in OWN_TO:
        Send(lambda j, w=w, dv=dv: (g_in.at[blk(d, TH), :], G.at[hp, c, blk(d, TH), blk(d, DH)], rid("G" + w), dv)).start()

    RL = min(8 * RING, TH)

    def stats(x):
        mean = jnp.sum(x, axis=1, keepdims=True) / DM
        var = jnp.sum(x * x, axis=1, keepdims=True) / DM - mean * mean
        inv_std = lax.rsqrt(var + LN_EPS)
        return inv_std, (x - mean) * inv_std


    def own_part(xb, gb, ab, vb, b2, b3, sems, sems2):
        mine, other = blk(d, DH), blk(e, DH)
        ld = batch(sems, (g_in.at[blk(d, TH), :], gb.at[:, mine]), (x_in.at[blk(d, TH), :], xb.at[:, mine]),
                   *[(ref, vb.at[i, :, mine]) for i, ref in enumerate(VEC)])
        start(ld)
        wait(ld)
        got = batch(sems, (GF.at[:, other], gb.at[:, other]), (XF.at[:, other], xb.at[:, other]),
                    *[(PV.at[i, :, other], vb.at[i, :, other]) for i in range(len(VEC))])
        for i in range(len(VEC)):
            arrived(PV.at[i, :, other], rid("pv") + i)
        for ref, w in ((GF, "gf"), (XF, "xf")):
            arrived(ref.at[:, other], rid(w))
            if ref is GF:
                for w, dv in OWN_TO:
                    Send(lambda j, w=w, dv=dv: (GF.at[:, blk(e, DH)], G.at[hp, c, blk(d, TH), blk(e, DH)], rid("G" + w) + 1, dv)).start()
        move(got)
        start(batch(sems2, (gb, ch(G, 0, c, d))))
        keep = batch(sems, (xb.at[:, mine], XF.at[:, mine]), *[(vb.at[i, :, mine], PV.at[i, :, mine]) for i in range(len(VEC))])
        start(keep)
        scale, shift = vb[0], vb[1]

        def rows(m, _):
            sl = blk(m, RL)
            ab[sl, :] = (stats(xb[sl, :].astype(F32))[1] * scale + shift).astype(BF16)
            return 0

        lax.fori_loop(0, TH // RL, rows, 0)
        wait(keep)
        move(batch(sems, (ab, ch(A, 0, c, d))))
        for w, dv in OWN_TO:
            Send(lambda j, w=w, dv=dv: (ch(A, 0, c, d), ch(A, 0, c, d), rid("A" + w), dv)).start()
        send_w2("u", u)
        send_w1("u", u, pos_r, pos_v)
        wait(batch(sems2, (gb, ch(G, 0, c, d))))
        wl = batch(sems, (w2.at[blk(d, FB), :], b3), (w1_src(0, d), b2.at[:, blk(0, FB)]))
        move(wl)
        move(batch(sems, *[(w1_src(pos, d), b2.at[:, blk(pos, FB)]) for pos in range(1, RING)]))
        move(batch(sems, (b3, w2_part(pos_r, d)), (b2, W1.at[blk(d * RING + r, DS), :])))

    pl.run_scoped(own_part, bf(TH, DM), bf(TH, DM), bf(TH, DM), fl(RING - 1, 1, DM), bf(DS, FC), bf(FB, DH), dma(MANY), dma(MANY))
    for pos in range(RING):
        Send(lambda j, pos=pos: (w1_src(pos, e), w1_dst(d, r, pos), rid("w1d") + pos, dev_e)).start()
    Send(lambda j: (w2.at[blk(e, FB), :], w2_part(pos_r, d), rid("w2d"), dev_e)).start()

    fwd, par = {}, {}
    for nm, X in ARR:
        for t in BOTH:
            b = nm + "d" + str(t)
            fwd[nm, t] = [same(ch(X, t, L, d, 0), rid(nm + "fr" + str(t)), dev_R), same(ch(X, t, R, d, 1), rid(nm + "fl" + str(t)), dev_L),
                          same(ch(X, t, L, d), rid(b + "L"), dev_e), same(ch(X, t, R, d), rid(b + "R"), dev_e),
                          same(ch(X, t, far, d, 0), rid(b + "x"), dev_e), same(ch(X, t, far, d, 1), rid(b + "y"), dev_e)]
        par[nm] = [same(ch(X, 1, c, d), rid(nm + w), dv) for w, dv in (("xr1", dev_R), ("xl1", dev_L), ("d1c", dev_e))]

    def own_in(nm, X, t, col, w, core=d):
        if nm + w in ("Gxr0", "Gxl0", "Gu", "Gd0c"):
            for half, i in ((core, 0), (flip(core), 1)):
                arrived(X.at[ROW[t], col, blk(core, TH), blk(half, DH)], rid(nm + w) + i)
        else:
            arrived(ch(X, t, col, core), rid(nm + w))

    def pass_on(nm, X, t):
        to_r, to_l, d_l, d_r = fwd[nm, t][:RING]
        own_in(nm, X, t, L, "xr" + str(t))
        to_r.start()
        own_in(nm, X, t, R, "xl" + str(t))
        to_l.start()
        d_l.start()
        d_r.start()

    def from_u(nm, X):
        own_in(nm, X, 1, c, "u")
        for t in par[nm]:
            t.start()

    def far_in(nm, X, t):
        for part, w in zip(BOTH, ("fr", "fl")):
            arrived(ch(X, t, far, d, part), rid(nm + w + str(t)))
            fwd[nm, t][RING + part].start()

    def other_core(t, *which):
        for nm, X in ARR:
            b = nm + "d" + str(t)
            for w in which:
                if w == "far":
                    for part, z in zip(BOTH, "xy"):
                        arrived(ch(X, t, far, e, part), rid(b + z))
                else:
                    own_in(nm, X, t, {"c": c, "L": L, "R": R}[w], b[1:] + w, e)

    def hop(tag, row, device, *positions):
        out = []
        for pos in positions:
            out.append(Send(lambda j, pos=pos: (w1_dst(j, row, pos), w1_dst(j, row, pos), rid(tag) + low(pos) * TWO + j, device), TWO))
        return out

    f1v = hop("f1v", u, dev(v, d), pos_v, pos_r)
    f1u = hop("f1u", v, dev(u, d), pos_r, pos_v)
    q0, q1 = pl.ds(0, BN), pl.ds(BN, DM - BN)
    f2u = same(W2.at[blk(pos_v, FB), q0], rid("f2u"), dev(u, d))
    f2v = same(W2.at[blk(pos_u, FB), q1], rid("f2v"), dev(v, d))

    def w1_in(tag, row, pos):
        for dd in BOTH:
            arrived(w1_dst(dd, row, pos), rid("w1" + tag) + dd * RING + pos)

    def w1_rest(pos, tag):
        arrived(w1_dst(e, r, pos), rid("w1d") + pos)
        for j in BOTH:
            arrived(w1_dst(j, q, pos), rid(tag) + low(pos) * TWO + j)

    for pos in (pos_r, pos_v):
        w1_in("u", u, pos)
    for t in f1v:
        t.all()
    send_w2("v", v)
    send_w1("v", v, pos_q, pos_u)
    pass_on("G", G, 0)
    for pos in (pos_r, pos_v):
        w1_in("v", v, pos)
    for t in f1u:
        t.all()
    other_core(0, "c")
    arrived(w2_part(pos_r, e), rid("w2d"))
    w1_rest(pos_r, "f1v")

    RC = min(8 * RING, TH)

    def cd_block(a, gr, w1b, w2b, bias, cbuf, gbuf, h_out, dc_out, db, count_db):
        cbuf[:] = jnp.dot(a, w1b, preferred_element_type=F32)
        gbuf[:] = lax.dot_general(gr, w2b, NT, preferred_element_type=F32)

        def rows(m, acc):
            sl = blk(m, RC)
            pre = cbuf[sl, :] + bias
            sq = pre * pre
            th = jnp.tanh(GELU_K * (pre + GELU_C * pre * sq))
            half = 0.5 * (1.0 + th)
            slope = half + 0.5 * pre * (1.0 - th * th) * GELU_K * (1.0 + 3.0 * GELU_C * sq)
            dc = gbuf[sl, :] * slope
            h_out[sl, :] = (pre * half).astype(BF16)
            dc_out[sl, :] = dc.astype(BF16)
            return acc + jnp.sum(dc.reshape(RC // 8, 8, FB), axis=0)

        acc = lax.fori_loop(0, T2 // RC, rows, jnp.zeros((8, FB), F32))

        @when(count_db)
        def _():
            db[:] += acc

    def hidden(n, place, block, need, first, posts, late):
        def body(ab, gb, w1b, w2b, cbuf, gbuf, hb, cb, dbs, isem, osem, wsem):
            def weights(b):
                pos = block(b * first)[1]
                return batch(wsem.at[b], (W1.at[:, blk(pos, FB)], w1b.at[b]), (W2.at[blk(pos, FB), :], w2b.at[b]))

            def load(b):
                need(b)
                start(weights(b))

            load(0)
            dbs[:] = jnp.zeros_like(dbs)

            def ins(k, s):
                row, col, _ = place(k)
                return (A.at[row, col], ab.at[s]), (G.at[row, col], gb.at[s])

            def outs(k, s):
                row, col, _ = place(k)
                to_p, cols = block(k)[TWO:]
                at = (high(col), low(col), slice(None), cols)
                H, C = (o["HP"].at[row], o["CP"].at[row]) if to_p else (o["HQ"], o["CQ"])
                return (hb.at[s], H.at[at]), (cb.at[s], C.at[at])

            def work(k, s):
                b, pos = block(k)[:TWO]
                for t in BOTH:
                    @when(k == t * first)
                    def _():
                        wait(weights(t))
                cd_block(ab[s], gb[s], w1b[b], w2b[b], bup[:, f_block(pos, d)], cbuf, gbuf, hb.at[s], cb.at[s], dbs.at[b], place(k)[TWO])

            run(n, ins, outs, isem, osem, work, posts={k: functools.partial(fn, load) for k, fn in posts.items()}, late=late)
            move(batch(wsem.at[0], *[(dbs.at[b], o["DB"].at[:, blk(block(b * first)[1], FB)]) for b in BOTH]))

        pl.run_scoped(body, bf(TWO, T2, DM), bf(TWO, T2, DM), bf(TWO, DM, FB), bf(TWO, FB, DM), fl(T2, FB), fl(T2, FB),
                      bf(TWO, T2, FB), bf(TWO, T2, FB), fl(TWO, 8, FB), dma(TWO, MANY), dma(TWO, MANY), dma(TWO, MANY))

    five, ten = RING + 1, TWO * RING + TWO

    def place1(k):
        early = k < ten
        k5, k2 = k % five, high(k - ten) + 1
        mine = jnp.logical_and(early, k5 < RING)
        m = jnp.where(early, k5 % RING, k2)
        return jnp.where(mine, hp, flip(hp)), (c + m + high(m) * (five - TWO * m)) % RING, mine

    def block1(k):
        b = jnp.where(k < ten, k // five % TWO, low(k))
        ii = jnp.where(b == 0, hi, hn)
        return b, TWO * g + ii, True, blk(ii, FB)

    def need1(b):
        if b:
            wait_w2("v", pos_v)
            f2u.start()
            w1_rest(pos_v, "f1v")

    def post0(load):
        pass_on("A", A, 0)
        from_u("G", G)
        other_core(0, "L", "R")

    def post2(load):
        far_in("G", G, 0)
        from_u("A", A)
        far_in("A", A, 0)
        other_core(0, "far")

    def post9(load):
        pass_on("A", A, 1)
        wait_w2("u", pos_u)
        f2v.start()
        other_core(1, "L", "R")

    def post13(load):
        start(early())
        far_in("G", G, 1)
        far_in("A", A, 1)
        other_core(1, "far")

    ahead = []

    def early():
        rb, sem = ahead
        return batch(sem, (o["CP"].at[hp], rb.at[hp]),
                     *[(o["CP"].at[flip(hp), high(t), low(t)], rb.at[flip(hp), high(t), low(t)]) for t in (c, R)])

    def rest():
        rb, sem = ahead
        return batch(sem.at[pl.ds(MANY, MANY)], *[(o["CP"].at[flip(hp), high(t), low(t)], rb.at[flip(hp), high(t), low(t)]) for t in (L, far)])

    posts1 = {0: post0, TWO: post2, RING - 1: lambda load: other_core(1, "c"), RING: lambda load: load(1),
              five: lambda load: pass_on("G", G, 1), ten - 1: post9, ten + RING - 1: post13}

    S1, R1, S2, R2, K1, K2, OUT1, OUT2 = [o[t] for t in ("S1", "R1", "S2", "R2", "K1", "K2", "OUT1", "OUT2")]
    s1 = Send(lambda j: (S1.at[j], R1.at[j], rid("s1") + j, dev(v, d)), RING)
    s2 = Send(lambda j: (S2.at[:, blk(j, BN)], R2.at[:, blk(j, BN)], rid("s2") + j, dev(v, d)), RING)

    def dw1_cols(k, pair, first):
        j = first + (1 - TWO * first) * high(k)
        return blk(low(k) * RING + TWO * pair + j, DS)

    def grad(left, right, left_shape, right_shape, resident, out_shape, outs, done, recv=None, posts=None, mid=None, pre=None):
        rows, width = out_shape

        def body(acc, ob, nb, isem, osem, wsem, lb, rb):
            if pre is not None:
                stay = early() + rest()
            else:
                stay = batch(wsem, resident((lb, rb)))
                start(stay)

            def ins(k, s):
                return (left(k), lb.at[s]) if right is None else (right(k), rb.at[s]),

            def work(k, s):
                @when(k == 0)
                def _():
                    wait(stay)
                x, y = (lb[s], rb[:]) if right is None else (lb[:], rb[s])
                val = lax.dot_general(x.reshape(ALLT, rows), y.reshape(ALLT, width), TN, preferred_element_type=F32)
                if recv is None:
                    ob[s] = val
                else:
                    acc[:] = val
                    ref, rsid = recv(k)
                    if mid:
                        for t, fn in enumerate(mid):
                            if t:
                                arrived(ref, rsid)
                                start(batch(wsem, (ref, nb)))
                            when(k == RING - 1)(fn)
                        wait(batch(wsem, (ref, nb)))
                    else:
                        arrived(ref, rsid)
                        move(batch(wsem, (ref, nb)))
                    ob[s] = (acc[:] + nb[:]).astype(BF16)

            run(RING, ins, lambda k, s: ((ob.at[s], outs(k)),), isem, osem, work, done=lambda k, s: done(k, ob.at[s], wsem), posts=posts)

        extra = out_shape if recv else (8, BN)
        kinds = [fl(*extra), pltpu.VMEM(SLOTS + out_shape, BF16 if recv else F32), fl(*extra), dma(TWO, MANY), dma(TWO, MANY), dma(MANY)]
        if pre is not None:
            pl.run_scoped(lambda *bufs: body(*bufs, pre), *kinds, bf(*left_shape))
        else:
            pl.run_scoped(body, *kinds, bf(*left_shape), bf(*right_shape))

    PT, PTS = (TWO, RING, T2), (TWO, TWO, TWO, T2)

    def grad1(pair, first, outs, done, recv=None, pre=None):
        grad(lambda k: A.at[:, :, :, dw1_cols(k, pair, first)], None, SLOTS + PT + (DS,), PTS + (F2,), lambda b: (o["CP"], b[1]),
             (DS, F2), outs, done, recv, pre=pre)

    def grad2(pair, outs, done, recv=None, posts=None, mid=None):
        grad(None, lambda k: G.at[:, :, :, blk(k, BN)], PTS + (FB,), SLOTS + PT + (BN,), lambda b: (o["HP"].at[:, :, :, :, blk(pair, FB)], b[0]),
             (FB, BN), outs, done, recv, posts, mid)

    def phase1(rb, sem):
        ahead.extend((rb, sem))
        hidden(ten + RING + TWO, place1, block1, need1, five, posts1, (1, RING - 1, RING, ten, ten + RING))
        start(rest())
        grad1(hn, hp, lambda k: S1.at[k], lambda k, ob, sem: s1.start(k), pre=rb)

    pl.run_scoped(phase1, bf(*PTS, F2), dma(TWO * MANY))

    def block2(k):
        b = k // RING
        ii = jnp.where(b == 0, hi, hn)
        return b, TWO * gn + ii, False, blk(ii, FB)

    def need2(b):
        pos = pos_q if b else pos_u
        w1_in("u", u, pos)
        w1_in("v", v, pos)
        w1_rest(pos, "f1u")
        if b:
            arrived(W2.at[blk(pos_q, FB), q1], rid("f2v"))
            arrived(W2.at[blk(pos_q, FB), q0], rid("f2u"))

    hidden(TWO * RING, lambda k: (hp, k % RING, k >= 0), block2, need2, RING, {TWO: lambda load: load(1)}, ())

    def region(s, nt, XP, XQ, PX, RX):
        Q1, Q2, RF, RR = [o[s + t] for t in ("Q1", "Q2", "RF", "RX")]
        ex = Send(lambda j: (PX.at[:, :, :, blk(j, BN)], RX.at[:, :, :, blk(j, BN)], rid(s + "p") + j, dev_e), RING)
        away = flip(c_hi)
        far_r = Send(lambda j: (Q1.at[away, blk(0, HT), blk(j, BN)], RF.at[away, :, blk(j, BN)], rid(s + "r") + j, dev_R), RING)
        far_l = Send(lambda j: (Q1.at[away, blk(1, HT), blk(j, BN)], RF.at[away, :, blk(j, BN)], rid(s + "l") + j, dev_L), RING)
        pm_r = Send(lambda j: (Q2.at[high(R), :, blk(j, BN)], RR.at[0, :, blk(j, BN)], rid(s + "pr") + j, dev_R), RING)
        pm_l = Send(lambda j: (Q2.at[high(L), :, blk(j, BN)], RR.at[1, :, blk(j, BN)], rid(s + "pl") + j, dev_L), RING)
        wshape = (BN, FC) if nt else (FC, BN)
        mine, other = blk(d, TH), blk(e, TH)

        def wsrc(j):
            return W1.at[blk(j, BN), :] if nt else W2.at[:, blk(j, BN)]

        def wdot(out, p_ref, q_ref, wref):
            for ref, half in ((p_ref, g), (q_ref, gn)):
                x, sel = ref[:].reshape(-1, F2), blk(half, F2)
                if nt:
                    val = lax.dot_general(x, wref[:, sel], NT, preferred_element_type=F32)
                else:
                    val = jnp.dot(x, wref[sel, :], preferred_element_type=F32)
                val = val.reshape(out.shape)
                out[:] = val if ref is p_ref else out[:] + val

        def first(lop, loq, lfp, lfq, wb, ob, ab, qb, wsem, lsem, osem, asem):
            def wcp(j):
                return batch(wsem.at[j % RING], (wsrc(j), wb.at[j % RING]))

            lds = batch(lsem, (XP.at[hp, :, :, other], lop), (XQ.at[:, :, other], loq), (XP.at[hp, :, c_lo, mine], lfp), (XQ.at[:, c_lo, mine], lfq))
            start(wcp(0) + lds)
            wait(lds)

            def step(j, _):
                o1 = batch(osem, (ob, PX.at[:, :, :, blk(j, BN)]))

                @when(j < RING)
                def _():
                    wait(wcp(j))

                    @when(j < RING - 1)
                    def _():
                        start(wcp(j + 1))
                    wdot(ob, lop, loq, wb.at[j % RING])
                    start(o1)

                @when(j >= LAG)
                def _():
                    k = j - LAG
                    arrived(RX.at[:, :, :, blk(k, BN)], rid(s + "p") + k)
                    add = batch(asem, (RX.at[:, c_lo, :, blk(k, BN)], ab))
                    start(add)
                    wdot(qb, lfp, lfq, wb.at[k % RING])
                    wait(add)
                    qb[:] += ab[:]
                    start(batch(lsem, (qb, Q1.at[:, :, blk(k, BN)])))

                @when(j < RING)
                def _():
                    wait(o1)
                    ex.start(j)

                @when(j >= LAG)
                def _():
                    k = j - LAG
                    wait(batch(lsem, (qb, Q1.at[:, :, blk(k, BN)])))
                    far_r.start(k)
                    far_l.start(k)
                return 0

            lax.fori_loop(0, RING + LAG, step, 0)

        def second(lp, lq, wb, ab, fb, ob, lsem, isem, osem):
            lds = batch(lsem, (XP.at[hp, :, flip(c_lo), mine], lp), (XQ.at[:, flip(c_lo), mine], lq))
            start(lds)

            def need(k):
                arrived(RF.at[high(R), :, blk(k, BN)], rid(s + "r") + k)
                arrived(RF.at[high(L), :, blk(k, BN)], rid(s + "l") + k)

            for k in range(RING):
                need(k)
            wait(lds)

            def ins(k, sl):
                return (wsrc(k), wb.at[sl]), (RX.at[:, flip(c_lo), :, blk(k, BN)], ab.at[sl]), (RF.at[:, :, blk(k, BN)], fb.at[sl])

            def work(k, sl):
                wdot(ob.at[sl], lp, lq, wb.at[sl])
                ob[sl] += ab[sl]
                for col, part in ((R, 0), (L, 1)):
                    ob[sl, high(col), part * HT:(part + 1) * HT, :] += fb[sl, high(col)]

            def done(k, sl):
                pm_r.start(k)
                pm_l.start(k)

            run(RING, ins, lambda k, sl: ((ob.at[sl], Q2.at[:, :, blk(k, BN)]),), isem, osem, work, done=done)

        def run_first():
            pl.run_scoped(first, bf(TWO, TWO, TH, F2), bf(TWO, TWO, TH, F2), bf(TWO, TH, F2), bf(TWO, TH, F2), bf(RING, *wshape),
                          fl(TWO, TWO, TH, BN), fl(TWO, TH, BN), fl(TWO, TH, BN), dma(RING, RING), dma(MANY), dma(MANY), dma(MANY))

        def run_second():
            pl.run_scoped(second, bf(TWO, TH, F2), bf(TWO, TH, F2), bf(TWO, *wshape), fl(TWO, TWO, TH, BN), fl(TWO, TWO, HT, BN),
                          fl(TWO, TWO, TH, BN), dma(MANY), dma(TWO, MANY), dma(TWO, MANY))

        def come(j):
            arrived(RR.at[0, :, blk(j, BN)], rid(s + "pr") + j)
            arrived(RR.at[1, :, blk(j, BN)], rid(s + "pl") + j)
        return run_first, run_second, come

    y1, y2, y_come = region("Y", False, o["HP"], o["HQ"], o["PY"], o["RY"])
    d1, d2, d_come = region("D", True, o["CP"], o["CQ"], o["PD"], o["RD"])
    d1()
    y1()
    d2()
    grad2(hn, lambda k: S2.at[:, blk(k, BN)], lambda k, ob, sem: s2.start(k))
    y2()

    def piece(ii):
        return slice(ii * FB, (ii + 1) * FB)

    k1u = [Send(lambda m, ii=ii: (K1.at[m, :, piece(ii)], OUT1.at[:, f_block(TWO * g + ii, d)], rid("k1u") + d * TWO + ii, dev(u, m)), TWO)
           for ii in BOTH]
    k1d = [Send(lambda m, ii=ii: (K1.at[TWO + e, :, piece(ii)], OUT1.at[:, f_block(TWO * g + ii, d)], rid("k1d") + ii, dev_e)) for ii in BOTH]

    def done1(k, ob, sem):
        @when(k < TWO)
        def _():
            for t in k1u:
                t.start(k)

        @when(k == TWO + e)
        def _():
            for t in k1d:
                t.start()

        @when(k == TWO + d)
        def _():
            move(batch(sem, *[(ob.at[:, piece(ii)], OUT1.at[:, f_block(TWO * g + ii, d)]) for ii in BOTH]))

    def out2_at(core, jj):
        return OUT2.at[blk(core, FB), blk(jj, BN)]

    k2 = Send(lambda jj: (K2.at[TWO * e + jj], out2_at(d, jj), rid("k2") + jj, dev_e), TWO)

    def done2(k, ob, sem):
        @when(high(k) == d)
        def _():
            move(batch(sem, (ob, out2_at(d, low(k)))))

        @when(high(k) == e)
        def _():
            k2.start(low(k))

    grad1(hi, flip(hp), lambda k: K1.at[k], done1, lambda k: (R1.at[k], rid("s1") + k))

    RX_, OUTX, XO, OUTY, YO, BG, SO = [o[t] for t in ("DRX", "OUTX", "XO", "OUTY", "YO", "BG", "SO")]
    xo = Send(lambda j: (XO, OUTX.at[blk(d, TH), :], rid("xo"), dev_e))
    stages = [dev_e, dev(u, d), dev(v, d), {"col": c + 1 - TWO * c_lo}, {"col": RING - 1 - c}]
    assert len(stages) == STAGES
    sum_send = [Send(lambda j, k=k, dv=dv: (sums.at[k], sums_in.at[k], rid("sum") + k, dv))
                for k, dv in enumerate(stages)]
    bsend = [Send(lambda j, k=k, dv=dv: (db.at[k], db_in.at[k], rid("bf") + k, dv)) for k, dv in enumerate((dev(u, d), dev(v, d)))]
    bg = Send(lambda j: (BG.at[d], BG.at[d], rid("bg"), dev_e))

    def finish_dx(q1b, rlb, rrb, xb, gb, vb, xob, acc, dbb, isem, osem, wsem):
        RB = min(8 * RING, high(TH))
        par_ = batch(wsem, (PV, vb), (o["DB"], dbb))
        start(par_)
        for j in range(RING):
            d_come(j)
        acc[:] = jnp.zeros_like(acc)

        def ins(k, s):
            rows = blk(k, RB)
            return ((o["DQ1"].at[c_hi, rows], q1b.at[s]), (RX_.at[0, rows], rlb.at[s]), (RX_.at[1, rows], rrb.at[s]), (XF.at[rows, :], xb.at[s]),
                    (G.at[hp, c, pl.ds(pl.multiple_of(d * TH + k * RB, RB), RB), :], gb.at[s]))

        def outs(k, s):
            return ((xob.at[s, :, blk(d, DH)], OUTX.at[pl.ds(pl.multiple_of(d * TH + k * RB, RB), RB), :]),
                    (xob.at[s, :, blk(e, DH)], XO.at[blk(k, RB), :]))

        def fold(x):
            return jnp.sum(x.reshape(RB // 8, 8, DM), axis=0)

        def work(k, s):
            @when(k == 0)
            def _():
                wait(par_)
            da = q1b[s] + rlb[s] + rrb[s]
            inv_std, xhat = stats(xb[s].astype(F32))
            gr = gb[s].astype(F32)
            val = da * vb[0]
            m1 = jnp.sum(val, axis=1, keepdims=True) / DM
            m2 = jnp.sum(val * xhat, axis=1, keepdims=True) / DM
            xob[s] = (gr + inv_std * (val - m1 - xhat * m2)).astype(BF16)
            for i, t in enumerate((da * xhat, da, gr)):
                acc[i] += fold(t)

        run(TH // RB, ins, outs, isem, osem, work)
        xo.start()
        for i in range(RING - 1):
            row = jnp.sum(acc[i], axis=0, keepdims=True)
            acc[i, 0:1, :] = row
        for i in range(RING - 1):
            sums[STAGES, i:i + 1, :] = acc[i, 0:1, blk(d, DH)]
            sums[0, i:i + 1, :] = acc[i, 0:1, blk(e, DH)]
        db[0, 0:1, :] = jnp.sum(dbb[:], axis=0, keepdims=True)
        sum_send[0].start()

    def stage(k):
        arrived(sums_in.at[k], rid("sum") + k)
        sums[STAGES] += sums_in[k]
        if k in (1, TWO):
            arrived(db_in.at[k - 1], rid("bf") + k - 1)
            db[k] = db[k - 1] + db_in[k - 1]
        if k < STAGES - 1:
            sums[k + 1] = sums[STAGES]
            sum_send[k + 1].start()
        if k < TWO:
            bsend[k].start()

    def sums_out(wsem):
        stage(STAGES - 1)
        move(batch(wsem, (sums.at[STAGES], SO), *[(db.at[TWO, :, blk(pos, FB)], BG.at[d, row]) for pos, row in enumerate((0, RING - 1, 1, TWO))]))
        bg.start()

    def dx_all():
        RB = min(8 * RING, high(TH))
        pl.run_scoped(finish_dx, fl(TWO, RB, DM), fl(TWO, RB, DM), fl(TWO, RB, DM), bf(TWO, RB, DM), bf(TWO, RB, DM), fl(RING - 1, 1, DM),
                      bf(TWO, RB, DM), fl(RING - 1, 8, DM), fl(8, FC), dma(TWO, MANY + RING), dma(TWO, MANY), dma(MANY))

    dx_all()

    def outy_at(core, jj):
        return OUTY.at[blk(core, TH), blk(jj, BN)]

    yo = Send(lambda jj: (YO.at[TWO * e + jj], outy_at(d, jj), rid("yo") + jj, dev_e), TWO)

    def last_part(q1b, xb, vb, rxb, yb, sem, sem2):
        def fetch_y(k):
            cols = blk(k, BN)
            start(batch(sem, (o["YQ1"].at[c_hi, :, cols], q1b), (XF.at[:, cols], xb), (PV.at[TWO, :, cols], vb)))
            y_come(k)
            start(batch(sem2, (o["YRX"].at[:, :, cols], rxb)))

        def finish_y(k):
            cols = blk(k, BN)
            here = batch(sem, (o["YQ1"].at[c_hi, :, cols], q1b), (XF.at[:, cols], xb), (PV.at[TWO, :, cols], vb))
            wait(here)
            wait(batch(sem2, (o["YRX"].at[:, :, cols], rxb)))
            yb[:] = (xb[:].astype(F32) + (q1b[:] + rxb[0] + rxb[1]) + vb[:]).astype(BF16)

            @when(d == high(k))
            def _():
                move(batch(sem, (yb, outy_at(high(k), low(k)))))

            @when(e == high(k))
            def _():
                move(batch(sem, (yb, YO.at[k])))
                yo.start(low(k))

        def third():
            stage(TWO)
            for k in range(RING - 1):
                fetch_y(k)
                finish_y(k)
                if k == 0:
                    stage(RING - 1)

        def before():
            sums_out(sem)
            fetch_y(RING - 1)

        mid = (before, lambda: finish_y(RING - 1))

        posts = {k: functools.partial(stage, k) for k in BOTH}
        posts[TWO] = third
        grad2(hi, lambda k: K2.at[k], done2, lambda k: (R2.at[:, blk(k, BN)], rid("s2") + k), posts, mid)

    pl.run_scoped(last_part, fl(TH, BN), bf(TH, BN), fl(1, BN), fl(TWO, TH, BN), bf(TH, BN), dma(MANY), dma(MANY))

    arrived(OUTX.at[blk(e, TH), :], rid("xo"))
    arrived(BG.at[e], rid("bg"))
    for ii in BOTH:
        arrived(outy_at(e, ii), rid("yo") + ii)
        for dd in BOTH:
            arrived(OUT1.at[:, f_block(TWO * gn + ii, dd)], rid("k1u") + dd * TWO + ii)
        arrived(OUT1.at[:, f_block(TWO * g + ii, e)], rid("k1d") + ii)
        arrived(out2_at(e, ii), rid("k2") + ii)
    for t in pending:
        for j in range(t.n):
            t.desc(j).wait_send()
    assert tuple(counts) == SEMS, counts


SEMS = (171, 149)


def solution(mesh):
    nr, nc, nd = mesh.shape["row"], mesh.shape["col"], mesh.shape["dep"]
    assert nr == 4 and nc == 4 and nd == 2
    tok_spec = P(("part", "row", "col"), "dep")
    vec_dep = P("dep")
    part_dep = P(("part", "dep"))
    in_specs = (tok_spec, vec_dep, vec_dep, P(("dep", "row"), "col"), P("col"), P(("col", "row"), "dep"), vec_dep, tok_spec)
    out_specs = (tok_spec, tok_spec, P(("part", "dep", "row"), "col"), P(("part", "col")), P(("part", "col", "row"), "dep"), part_dep, part_dep, part_dep)

    def local_step(x_in, ln_scale, ln_shift, w_up, b_up, w_down, b_down, y_grad):
        th, dhalf = x_in.shape[0] // 2, x_in.shape[1]
        ds_, fb = w_up.shape[0], w_up.shape[1] // 8
        rows = [t.astype(F32).reshape(1, -1) for t in (ln_scale, ln_shift, b_down, b_up)]

        cfg = (th, 2 * dhalf, ds_, fb)
        outs = pl.pallas_call(
            functools.partial(kernel, cfg),
            name="mlp_layer",
            out_shape=buffers(*cfg),
            in_specs=[pl.BlockSpec(memory_space=pl.ANY)] * 7 + [pl.BlockSpec(memory_space=pltpu.VMEM)],
            out_specs=[pl.BlockSpec(memory_space=pl.ANY)] * len(NAMES),
            scratch_shapes=[dma(SEMS[1]), dma(SEMS[0]), fl(STAGES + 1, 8, dhalf), fl(STAGES, 8, dhalf), fl(3, 8, 4 * fb), fl(2, 8, 4 * fb)],
            compiler_params=pltpu.CompilerParams(collective_id=0, has_side_effects=True, vmem_limit_bytes=62 * 1024 * 1024),
        )(x_in, y_grad, w_up, w_down, *rows)
        o = dict(zip(NAMES, outs))
        b_up_grad = o["BG"][:, :, 0].transpose(1, 0, 2).reshape(8 * fb)
        return (o["OUTY"], o["OUTX"], o["OUT1"], b_up_grad, o["OUT2"], o["SO"][2], o["SO"][0], o["SO"][1])

    return jax.shard_map(local_step, mesh=mesh, in_specs=in_specs, out_specs=out_specs, check_vma=False)
```

```python
import functools

import jax
import jax.numpy as jnp
from jax import lax
from jax.experimental import pallas as pl
from jax.experimental.pallas import tpu as pltpu
from jax.sharding import PartitionSpec as P

LN_EPS = 1e-5
GELU_K = 0.7978845608028654
GELU_C = 0.044715
F32 = jnp.float32
BF16 = jnp.bfloat16
MESH = pl.DeviceIdType.MESH

NAMES = ("A", "G", "W1", "W2", "HP", "HQ", "CP", "CQ", "DB",
         "PY", "RY", "YQ1", "YQ2", "YRF", "YRX", "PD", "RD", "DQ1", "DQ2", "DRF", "DRX",
         "S1", "R1", "S2", "R2", "K1", "K2", "OUT1", "OUT2", "XF", "GF", "PV", "YO", "XO", "OUTY", "OUTX", "BG", "SO")
TWO, RING, STAGES, MANY = 2, 4, 5, 16
LAG = 2
BOTH, SLOTS = (0, 1), (2,)
NT = (((1,), (1,)), ((), ()))
TN = (((0,), (0,)), ((), ()))


def flip(x):
    return 1 - x


def low(x):
    return x % 2


def high(x):
    return x // 2


def buffers(TH, DM, DS, FB):
    F2, FC, T2 = 2 * FB, 4 * FB, 2 * TH
    pair = (TWO, TWO)
    shapes = {
        "A": ((TWO, RING, T2, DM), BF16), "W1": ((DM, FC), BF16), "W2": ((FC, DM), BF16),
        "HP": (SLOTS + pair + (T2, F2), BF16), "HQ": (pair + (T2, F2), BF16), "DB": ((8, FC), F32),
        "S1": ((RING, DS, F2), F32), "S2": ((FB, DM), F32),
        "K1": ((RING, DS, F2), BF16), "K2": ((RING, FB, high(DM) // TWO), BF16),
        "OUT1": ((DS, 8 * FB), BF16), "OUT2": ((F2, high(DM)), BF16),
        "XF": ((TH, DM), BF16), "GF": ((TH, DM), BF16), "PV": ((RING - 1, 1, DM), F32), "YO": ((RING, TH, high(DM) // TWO), BF16),
        "XO": ((TH, high(DM)), BF16), "OUTY": ((T2, high(DM)), BF16), "OUTX": ((T2, high(DM)), BF16),
        "BG": (SLOTS + (RING, 8, FB), F32), "SO": ((8, high(DM)), F32),
    }
    for new, old in (("G", "A"), ("CP", "HP"), ("CQ", "HQ"), ("R1", "S1"), ("R2", "S2")):
        shapes[new] = shapes[old]
    for p, s in (("PY", "Y"), ("PD", "D")):
        shapes[p] = shapes["R" + s] = (pair + (TH, DM), F32)
        for q in ("Q1", "Q2", "RX"):
            shapes[s + q] = (SLOTS + (TH, DM), F32)
        shapes[s + "RF"] = (SLOTS + (high(TH), DM), F32)
    return [jax.ShapeDtypeStruct(*shapes[n]) for n in NAMES]


def mul(x, n):
    return x * n if isinstance(x, int) else pl.multiple_of(x * n, n)


def cp(src, dst, sem):
    return pltpu.make_async_copy(src, dst, sem)


def parts(src, dst):
    rows = dst.shape[0]
    n = rows if rows == TWO and len(dst.shape) > RING - 1 else RING if rows % (8 * RING) == 0 else 1
    m = rows // n
    return [(src.at[pl.ds(i * m, m)], dst.at[pl.ds(i * m, m)]) for i in range(n)] if n > 1 else [(src, dst)]


def batch(sem, *pairs):
    return [cp(src, dst, sem.at[i]) for i, (src, dst) in enumerate(t for pair in pairs for t in parts(*pair))]


def start(copies):
    for t in copies:
        t.start()


def wait(copies):
    for t in copies:
        t.wait()


def move(copies):
    start(copies)
    wait(copies)


def dma(*shape):
    return pltpu.SemaphoreType.DMA(shape)


def bf(*shape):
    return pltpu.VMEM(shape, BF16)


def fl(*shape):
    return pltpu.VMEM(shape, F32)


def when(cond):
    def deco(fn):
        pl.when(cond)(fn)
    return deco


def run(n, ins, outs, isem, osem, work, done=None, posts=None, late=()):
    posts = posts or {}

    def fetch(k, s):
        return batch(isem.at[s], *ins(k, s))

    def back(k, s):
        return batch(osem.at[s], *outs(k, s))

    start(fetch(0, 0))

    def step(k, _):
        s, nxt = low(k), k + 1
        is_late = functools.reduce(jnp.logical_or, [nxt == t for t in late], False)
        more = nxt < n
        wait(fetch(k, s))

        @when(jnp.logical_and(more, jnp.logical_not(is_late)))
        def _():
            start(fetch(nxt, flip(s)))
        if done is None:
            @when(k >= TWO)
            def _():
                wait(back(k, s))
        work(k, s)
        start(back(k, s))
        for t, fn in posts.items():
            when(k == t)(fn)
        if late:
            @when(is_late)
            def _():
                start(fetch(nxt, flip(s)))
        if done is not None:
            @when(k == 0)
            def _():
                wait(back(k, s))
                done(k, s)

            @when(k >= TWO)
            def _():
                wait(back(k - 1, flip(s)))
                done(k - 1, flip(s))
        return 0

    lax.fori_loop(0, n, step, 0)
    last = n - 1
    if done is None:
        wait(back(last - 1, flip(low(last))))
    wait(back(last, low(last)))
    if done is not None:
        done(last, low(last))


def kernel(cfg, x_in, g_in, w1, w2, gam, bet, bdn, bup, *refs):
    TH, DM, DS, FB = cfg
    o = dict(zip(NAMES, refs[:len(NAMES)]))
    ssem, rsem, sums, sums_in, db, db_in = refs[len(NAMES):]
    DH, F2, FC, HT, T2 = high(DM), TWO * FB, RING * FB, high(TH), TWO * TH
    BN, ALLT = high(DH), TWO * RING * T2
    A, G, W1, W2 = o["A"], o["G"], o["W1"], o["W2"]
    r, c, d = lax.axis_index("row"), lax.axis_index("col"), lax.axis_index("dep")
    hp, hi = low(r), high(r)
    hn, e = flip(hi), flip(d)
    g = low(r + hi)
    gn = flip(g)
    u, v, q = r + 1 - TWO * hp, RING - 1 - r, (r + TWO) % RING
    R, L, far = (c + 1) % RING, (c + RING - 1) % RING, (c + TWO) % RING
    pos_r, pos_v, pos_u, pos_q = TWO * g + hi, TWO * g + hn, TWO * gn + hi, TWO * gn + hn
    c_lo, c_hi = low(c), high(c)

    ids, counts = {}, [0, 0]

    def name(key, n=1):
        ids[key] = counts[0]
        counts[0] += n

    def rid(key):
        return ids[key]

    for nm in "AG":
        for w in ("xr1", "xl1", "fr0", "fl0", "fr1", "fl1"):
            name(nm + w)
        for w in ("xr0", "xl0", "u"):
            name(nm + w, TWO)
        for t in "01":
            for w in "cLRxy":
                name(nm + "d" + t + w, TWO)
    for s in "uv":
        name("w1" + s, TWO * RING)
        name("w2" + s, TWO)
        name("f1" + s, RING)
        name("f2" + s)
    name("pv", RING - 1)
    for s in ("w2d", "xf", "gf", "xo", "bg"):
        name(s)
    name("yo", TWO)
    name("bf", TWO)
    name("sum", STAGES)
    for s in ("w1d", "s1", "s2", "k1u"):
        name(s, RING)
    name("k1d", TWO)
    name("k2", TWO)
    for s in "YD":
        for w in ("p", "r", "l", "pr", "pl"):
            name(s + w, RING)

    pending = []
    dev_e, dev_R, dev_L = {"dep": e}, {"col": R}, {"col": L}

    def dev(row, core):
        return {"row": row, "dep": core}

    class Send:
        def __init__(self, fn, n=1):
            self.fn, self.n, self.sid = fn, n, counts[1]
            counts[1] += n
            pending.append(self)

        def desc(self, j=0):
            src, dst, rsid, device = self.fn(j)
            return pltpu.make_async_remote_copy(src_ref=src, dst_ref=dst, send_sem=ssem.at[self.sid + j], recv_sem=rsem.at[rsid],
                                                device_id=device, device_id_type=MESH)

        def start(self, j=0):
            self.desc(j).start()

        def all(self):
            for j in range(self.n):
                self.start(j)

    def same(ref, rsid, device):
        return Send(lambda j: (ref, ref, rsid, device))

    def arrived(dst, rsid):
        pltpu.make_async_remote_copy(src_ref=dst, dst_ref=dst, send_sem=ssem.at[0], recv_sem=rsem.at[rsid],
                                     device_id=dev_e, device_id_type=MESH).wait_recv()

    barrier = pltpu.get_barrier_semaphore()
    peers = [dev_e, dev_R, dev_L] + [dev(t, k) for t in (u, v) for k in BOTH]
    for p in peers:
        pl.semaphore_signal(barrier, inc=1, device_id=p, device_id_type=MESH)
    pl.semaphore_wait(barrier, len(peers))

    ARR = (("A", A), ("G", G))
    ROW = (hp, flip(hp))

    def ch(X, t, col, core, part=None):
        if part is None:
            return X.at[ROW[t], col, pl.ds(mul(core, TH), TH)]
        return X.at[ROW[t], col, pl.ds(pl.multiple_of(core * TH + part * HT, HT), HT)]

    def blk(k, n):
        return pl.ds(mul(k, n), n)

    def f_block(pos, core):
        gg, ii = high(pos), low(pos)
        return blk((flip(gg) * (RING - 1) * ii + gg * (1 + ii)) * TWO + core, FB)

    def w1_src(pos, core):
        return w1.at[:, f_block(pos, core)]

    def w1_dst(dd, row, pos):
        return W1.at[blk(dd * RING + row, DS), blk(pos, FB)]

    def send_w1(tag, row, *positions):
        for pos in positions:
            for core in BOTH:
                Send(lambda j, pos=pos, core=core: (w1_src(pos, core), w1_dst(d, r, pos), rid("w1" + tag) + d * RING + pos, dev(row, core))).start()

    def w2_part(pos, half):
        return W2.at[blk(pos, FB), blk(half, DH)]

    def send_w2(tag, row):
        for core in BOTH:
            Send(lambda j, core=core: (w2.at[blk(core, FB), :], w2_part(pos_r, d), rid("w2" + tag) + d, dev(row, core))).start()

    def wait_w2(tag, pos):
        for dd in BOTH:
            arrived(w2_part(pos, dd), rid("w2" + tag) + dd)

    XF, GF, PV = o["XF"], o["GF"], o["PV"]
    Send(lambda j: (g_in.at[blk(e, TH), :], GF.at[:, blk(d, DH)], rid("gf"), dev_e)).start()
    Send(lambda j: (x_in.at[blk(e, TH), :], XF.at[:, blk(d, DH)], rid("xf"), dev_e)).start()
    VEC = (gam, bet, bdn)
    for i, ref in enumerate(VEC):
        Send(lambda j, i=i, ref=ref: (ref, PV.at[i, :, blk(d, DH)], rid("pv") + i, dev_e)).start()
    OWN_TO = (("xr0", dev_R), ("xl0", dev_L), ("u", dev(u, d)), ("d0c", dev_e))
    send_w1("v", v, pos_v, pos_r)
    send_w1("u", u, pos_u, pos_q)
    for w, dv in OWN_TO:
        Send(lambda j, w=w, dv=dv: (g_in.at[blk(d, TH), :], G.at[hp, c, blk(d, TH), blk(d, DH)], rid("G" + w), dv)).start()

    RL = min(8 * RING, TH)

    def stats(x):
        mean = jnp.sum(x, axis=1, keepdims=True) / DM
        var = jnp.sum(x * x, axis=1, keepdims=True) / DM - mean * mean
        inv_std = lax.rsqrt(var + LN_EPS)
        return inv_std, (x - mean) * inv_std


    def own_part(xb, gb, ab, vb, b2, b3, sems, sems2):
        mine, other = blk(d, DH), blk(e, DH)
        ld = batch(sems, (g_in.at[blk(d, TH), :], gb.at[:, mine]), (x_in.at[blk(d, TH), :], xb.at[:, mine]),
                   *[(ref, vb.at[i, :, mine]) for i, ref in enumerate(VEC)])
        start(ld)
        wait(ld)
        got = batch(sems, (GF.at[:, other], gb.at[:, other]), (XF.at[:, other], xb.at[:, other]),
                    *[(PV.at[i, :, other], vb.at[i, :, other]) for i in range(len(VEC))])
        for i in range(len(VEC)):
            arrived(PV.at[i, :, other], rid("pv") + i)
        for ref, w in ((GF, "gf"), (XF, "xf")):
            arrived(ref.at[:, other], rid(w))
            if ref is GF:
                for w, dv in OWN_TO:
                    Send(lambda j, w=w, dv=dv: (GF.at[:, blk(e, DH)], G.at[hp, c, blk(d, TH), blk(e, DH)], rid("G" + w) + 1, dv)).start()
        move(got)
        start(batch(sems2, (gb, ch(G, 0, c, d))))
        keep = batch(sems, (xb.at[:, mine], XF.at[:, mine]), *[(vb.at[i, :, mine], PV.at[i, :, mine]) for i in range(len(VEC))])
        start(keep)
        scale, shift = vb[0], vb[1]

        def rows(m, _):
            sl = blk(m, RL)
            ab[sl, :] = (stats(xb[sl, :].astype(F32))[1] * scale + shift).astype(BF16)
            return 0

        lax.fori_loop(0, TH // RL, rows, 0)
        wait(keep)
        move(batch(sems, (ab, ch(A, 0, c, d))))
        for w, dv in OWN_TO:
            Send(lambda j, w=w, dv=dv: (ch(A, 0, c, d), ch(A, 0, c, d), rid("A" + w), dv)).start()
        send_w2("u", u)
        send_w1("u", u, pos_r)
        wait(batch(sems2, (gb, ch(G, 0, c, d))))
        wl = batch(sems, (w2.at[blk(d, FB), :], b3), (w1_src(0, d), b2.at[:, blk(0, FB)]))
        move(wl)
        move(batch(sems, *[(w1_src(pos, d), b2.at[:, blk(pos, FB)]) for pos in range(1, RING)]))
        move(batch(sems, (b3, w2_part(pos_r, d)), (b2, W1.at[blk(d * RING + r, DS), :])))

    pl.run_scoped(own_part, bf(TH, DM), bf(TH, DM), bf(TH, DM), fl(RING - 1, 1, DM), bf(DS, FC), bf(FB, DH), dma(MANY), dma(MANY))
    for pos in range(RING):
        Send(lambda j, pos=pos: (w1_src(pos, e), w1_dst(d, r, pos), rid("w1d") + pos, dev_e)).start()
    Send(lambda j: (w2.at[blk(e, FB), :], w2_part(pos_r, d), rid("w2d"), dev_e)).start()

    fwd, par = {}, {}
    for nm, X in ARR:
        for t in BOTH:
            b = nm + "d" + str(t)
            fwd[nm, t] = [same(ch(X, t, L, d, 0), rid(nm + "fr" + str(t)), dev_R), same(ch(X, t, R, d, 1), rid(nm + "fl" + str(t)), dev_L),
                          same(ch(X, t, L, d), rid(b + "L"), dev_e), same(ch(X, t, R, d), rid(b + "R"), dev_e),
                          same(ch(X, t, far, d, 0), rid(b + "x"), dev_e), same(ch(X, t, far, d, 1), rid(b + "y"), dev_e)]
        par[nm] = [same(ch(X, 1, c, d), rid(nm + w), dv) for w, dv in (("xr1", dev_R), ("xl1", dev_L), ("d1c", dev_e))]

    def own_in(nm, X, t, col, w, core=d):
        if nm + w in ("Gxr0", "Gxl0", "Gu", "Gd0c"):
            for half, i in ((core, 0), (flip(core), 1)):
                arrived(X.at[ROW[t], col, blk(core, TH), blk(half, DH)], rid(nm + w) + i)
        else:
            arrived(ch(X, t, col, core), rid(nm + w))

    def pass_on(nm, X, t):
        to_r, to_l, d_l, d_r = fwd[nm, t][:RING]
        own_in(nm, X, t, L, "xr" + str(t))
        to_r.start()
        own_in(nm, X, t, R, "xl" + str(t))
        to_l.start()
        d_l.start()
        d_r.start()

    def from_u(nm, X):
        own_in(nm, X, 1, c, "u")
        for t in par[nm]:
            t.start()

    def far_in(nm, X, t):
        for part, w in zip(BOTH, ("fr", "fl")):
            arrived(ch(X, t, far, d, part), rid(nm + w + str(t)))
            fwd[nm, t][RING + part].start()

    def other_core(t, *which):
        for nm, X in ARR:
            b = nm + "d" + str(t)
            for w in which:
                if w == "far":
                    for part, z in zip(BOTH, "xy"):
                        arrived(ch(X, t, far, e, part), rid(b + z))
                else:
                    own_in(nm, X, t, {"c": c, "L": L, "R": R}[w], b[1:] + w, e)

    def hop(tag, row, device, *positions):
        out = []
        for pos in positions:
            out.append(Send(lambda j, pos=pos: (w1_dst(j, row, pos), w1_dst(j, row, pos), rid(tag) + low(pos) * TWO + j, device), TWO))
        return out

    f1v = hop("f1v", u, dev(v, d), pos_v, pos_r)
    f1u = hop("f1u", v, dev(u, d), pos_r, pos_v)
    cut = BN - high(FB)
    q0, q1 = pl.ds(0, cut), pl.ds(cut, DM - cut)
    f2u = same(W2.at[blk(pos_v, FB), q0], rid("f2u"), dev(u, d))
    f2v = same(W2.at[blk(pos_u, FB), q1], rid("f2v"), dev(v, d))

    def w1_in(tag, row, pos):
        for dd in BOTH:
            arrived(w1_dst(dd, row, pos), rid("w1" + tag) + dd * RING + pos)

    def w1_rest(pos, tag):
        arrived(w1_dst(e, r, pos), rid("w1d") + pos)
        for j in BOTH:
            arrived(w1_dst(j, q, pos), rid(tag) + low(pos) * TWO + j)

    for pos in (pos_r, pos_v):
        w1_in("u", u, pos)
    for t in f1v:
        t.all()
    send_w2("v", v)
    send_w1("v", v, pos_q, pos_u)
    pass_on("G", G, 0)
    for pos in (pos_r, pos_v):
        w1_in("v", v, pos)
    f1u[0].all()
    send_w1("u", u, pos_v)
    f1u[1].all()
    other_core(0, "c")
    arrived(w2_part(pos_r, e), rid("w2d"))
    w1_rest(pos_r, "f1v")

    RC = min(8 * RING, TH)

    def cd_block(a, gr, w1b, w2b, bias, cbuf, gbuf, h_out, dc_out, db, count_db):
        cbuf[:] = jnp.dot(a, w1b, preferred_element_type=F32)
        gbuf[:] = lax.dot_general(gr, w2b, NT, preferred_element_type=F32)

        def rows(m, acc):
            sl = blk(m, RC)
            pre = cbuf[sl, :] + bias
            sq = pre * pre
            th = jnp.tanh(GELU_K * (pre + GELU_C * pre * sq))
            half = 0.5 * (1.0 + th)
            slope = half + 0.5 * pre * (1.0 - th * th) * GELU_K * (1.0 + 3.0 * GELU_C * sq)
            dc = gbuf[sl, :] * slope
            h_out[sl, :] = (pre * half).astype(BF16)
            dc_out[sl, :] = dc.astype(BF16)
            return acc + jnp.sum(dc.reshape(RC // 8, 8, FB), axis=0)

        acc = lax.fori_loop(0, T2 // RC, rows, jnp.zeros((8, FB), F32))

        @when(count_db)
        def _():
            db[:] += acc

    def hidden(n, place, block, need, first, posts, late):
        def body(ab, gb, w1b, w2b, cbuf, gbuf, hb, cb, dbs, isem, osem, wsem):
            def weights(b):
                pos = block(b * first)[1]
                return batch(wsem.at[b], (W1.at[:, blk(pos, FB)], w1b.at[b]), (W2.at[blk(pos, FB), :], w2b.at[b]))

            def load(b):
                need(b)
                start(weights(b))

            load(0)
            dbs[:] = jnp.zeros_like(dbs)

            def ins(k, s):
                row, col, _ = place(k)
                return (A.at[row, col], ab.at[s]), (G.at[row, col], gb.at[s])

            def outs(k, s):
                row, col, _ = place(k)
                to_p, cols = block(k)[TWO:]
                at = (high(col), low(col), slice(None), cols)
                H, C = (o["HP"].at[row], o["CP"].at[row]) if to_p else (o["HQ"], o["CQ"])
                return (hb.at[s], H.at[at]), (cb.at[s], C.at[at])

            def work(k, s):
                b, pos = block(k)[:TWO]
                for t in BOTH:
                    @when(k == t * first)
                    def _():
                        wait(weights(t))
                cd_block(ab[s], gb[s], w1b[b], w2b[b], bup[:, f_block(pos, d)], cbuf, gbuf, hb.at[s], cb.at[s], dbs.at[b], place(k)[TWO])

            run(n, ins, outs, isem, osem, work, posts={k: functools.partial(fn, load) for k, fn in posts.items()}, late=late)
            move(batch(wsem.at[0], *[(dbs.at[b], o["DB"].at[:, blk(block(b * first)[1], FB)]) for b in BOTH]))

        pl.run_scoped(body, bf(TWO, T2, DM), bf(TWO, T2, DM), bf(TWO, DM, FB), bf(TWO, FB, DM), fl(T2, FB), fl(T2, FB),
                      bf(TWO, T2, FB), bf(TWO, T2, FB), fl(TWO, 8, FB), dma(TWO, MANY), dma(TWO, MANY), dma(TWO, MANY))

    five, ten = RING + 1, TWO * RING + TWO

    def place1(k):
        early = k < ten
        k5, k2 = k % five, high(k - ten) + 1
        mine = jnp.logical_and(early, k5 < RING)
        m = jnp.where(early, k5 % RING, k2)
        return jnp.where(mine, hp, flip(hp)), (c + m + high(m) * (five - TWO * m)) % RING, mine

    def block1(k):
        b = jnp.where(k < ten, k // five % TWO, low(k))
        ii = jnp.where(b == 0, hi, hn)
        return b, TWO * g + ii, True, blk(ii, FB)

    def need1(b):
        if b:
            wait_w2("v", pos_v)
            f2u.start()
            w1_rest(pos_v, "f1v")

    def post0(load):
        pass_on("A", A, 0)
        from_u("G", G)
        other_core(0, "L", "R")

    def post2(load):
        far_in("G", G, 0)
        from_u("A", A)
        far_in("A", A, 0)
        other_core(0, "far")

    def post9(load):
        pass_on("A", A, 1)
        wait_w2("u", pos_u)
        f2v.start()
        other_core(1, "L", "R")

    def post13(load):
        start(early())
        far_in("G", G, 1)
        far_in("A", A, 1)
        other_core(1, "far")

    ahead = []

    def early():
        rb, sem = ahead
        return batch(sem, (o["CP"].at[hp], rb.at[hp]),
                     *[(o["CP"].at[flip(hp), high(t), low(t)], rb.at[flip(hp), high(t), low(t)]) for t in (c, R)])

    def rest():
        rb, sem = ahead
        return batch(sem.at[pl.ds(MANY, MANY)], *[(o["CP"].at[flip(hp), high(t), low(t)], rb.at[flip(hp), high(t), low(t)]) for t in (L, far)])

    posts1 = {0: post0, TWO: post2, RING - 1: lambda load: other_core(1, "c"), RING: lambda load: load(1),
              five: lambda load: pass_on("G", G, 1), ten - 1: post9, ten + RING - 1: post13}

    S1, R1, S2, R2, K1, K2, OUT1, OUT2 = [o[t] for t in ("S1", "R1", "S2", "R2", "K1", "K2", "OUT1", "OUT2")]
    s1 = Send(lambda j: (S1.at[j], R1.at[j], rid("s1") + j, dev(v, d)), RING)
    s2 = Send(lambda j: (S2.at[:, blk(j, BN)], R2.at[:, blk(j, BN)], rid("s2") + j, dev(v, d)), RING)

    def dw1_cols(k, pair, first):
        j = first + (1 - TWO * first) * high(k)
        return blk(low(k) * RING + TWO * pair + j, DS)

    def grad(left, right, left_shape, right_shape, resident, out_shape, outs, done, recv=None, posts=None, mid=None, pre=None):
        rows, width = out_shape

        def body(acc, ob, nb, isem, osem, wsem, lb, rb):
            if pre is not None:
                stay = early() + rest()
            else:
                stay = batch(wsem, resident((lb, rb)))
                start(stay)

            def ins(k, s):
                return (left(k), lb.at[s]) if right is None else (right(k), rb.at[s]),

            def work(k, s):
                @when(k == 0)
                def _():
                    wait(stay)
                x, y = (lb[s], rb[:]) if right is None else (lb[:], rb[s])
                val = lax.dot_general(x.reshape(ALLT, rows), y.reshape(ALLT, width), TN, preferred_element_type=F32)
                if recv is None:
                    ob[s] = val
                else:
                    acc[:] = val
                    ref, rsid = recv(k)
                    if mid:
                        for t, fn in enumerate(mid):
                            if t:
                                arrived(ref, rsid)
                                start(batch(wsem, (ref, nb)))
                            when(k == RING - 1)(fn)
                        wait(batch(wsem, (ref, nb)))
                    else:
                        arrived(ref, rsid)
                        move(batch(wsem, (ref, nb)))
                    ob[s] = (acc[:] + nb[:]).astype(BF16)

            run(RING, ins, lambda k, s: ((ob.at[s], outs(k)),), isem, osem, work, done=lambda k, s: done(k, ob.at[s], wsem), posts=posts)

        extra = out_shape if recv else (8, BN)
        kinds = [fl(*extra), pltpu.VMEM(SLOTS + out_shape, BF16 if recv else F32), fl(*extra), dma(TWO, MANY), dma(TWO, MANY), dma(MANY)]
        if pre is not None:
            pl.run_scoped(lambda *bufs: body(*bufs, pre), *kinds, bf(*left_shape))
        else:
            pl.run_scoped(body, *kinds, bf(*left_shape), bf(*right_shape))

    PT, PTS = (TWO, RING, T2), (TWO, TWO, TWO, T2)

    def grad1(pair, first, outs, done, recv=None, pre=None):
        grad(lambda k: A.at[:, :, :, dw1_cols(k, pair, first)], None, SLOTS + PT + (DS,), PTS + (F2,), lambda b: (o["CP"], b[1]),
             (DS, F2), outs, done, recv, pre=pre)

    def grad2(pair, outs, done, recv=None, posts=None, mid=None):
        grad(None, lambda k: G.at[:, :, :, blk(k, BN)], PTS + (FB,), SLOTS + PT + (BN,), lambda b: (o["HP"].at[:, :, :, :, blk(pair, FB)], b[0]),
             (FB, BN), outs, done, recv, posts, mid)

    def phase1(rb, sem):
        ahead.extend((rb, sem))
        hidden(ten + RING + TWO, place1, block1, need1, five, posts1, (1, RING - 1, RING, ten, ten + RING))
        start(rest())
        grad1(hn, hp, lambda k: S1.at[k], lambda k, ob, sem: s1.start(k), pre=rb)

    pl.run_scoped(phase1, bf(*PTS, F2), dma(TWO * MANY))

    def block2(k):
        b = k // RING
        ii = jnp.where(b == 0, hi, hn)
        return b, TWO * gn + ii, False, blk(ii, FB)

    def need2(b):
        pos = pos_q if b else pos_u
        w1_in("u", u, pos)
        w1_in("v", v, pos)
        w1_rest(pos, "f1u")
        if b:
            arrived(W2.at[blk(pos_q, FB), q1], rid("f2v"))
            arrived(W2.at[blk(pos_q, FB), q0], rid("f2u"))

    hidden(TWO * RING, lambda k: (hp, k % RING, k >= 0), block2, need2, RING, {TWO: lambda load: load(1)}, ())

    def region(s, nt, XP, XQ, PX, RX):
        Q1, Q2, RF, RR = [o[s + t] for t in ("Q1", "Q2", "RF", "RX")]
        ex = Send(lambda j: (PX.at[:, :, :, blk(j, BN)], RX.at[:, :, :, blk(j, BN)], rid(s + "p") + j, dev_e), RING)
        away = flip(c_hi)
        far_r = Send(lambda j: (Q1.at[away, blk(0, HT), blk(j, BN)], RF.at[away, :, blk(j, BN)], rid(s + "r") + j, dev_R), RING)
        far_l = Send(lambda j: (Q1.at[away, blk(1, HT), blk(j, BN)], RF.at[away, :, blk(j, BN)], rid(s + "l") + j, dev_L), RING)
        pm_r = Send(lambda j: (Q2.at[high(R), :, blk(j, BN)], RR.at[0, :, blk(j, BN)], rid(s + "pr") + j, dev_R), RING)
        pm_l = Send(lambda j: (Q2.at[high(L), :, blk(j, BN)], RR.at[1, :, blk(j, BN)], rid(s + "pl") + j, dev_L), RING)
        wshape = (BN, FC) if nt else (FC, BN)
        mine, other = blk(d, TH), blk(e, TH)

        def wsrc(j):
            return W1.at[blk(j, BN), :] if nt else W2.at[:, blk(j, BN)]

        def wdot(out, p_ref, q_ref, wref):
            for ref, half in ((p_ref, g), (q_ref, gn)):
                x, sel = ref[:].reshape(-1, F2), blk(half, F2)
                if nt:
                    val = lax.dot_general(x, wref[:, sel], NT, preferred_element_type=F32)
                else:
                    val = jnp.dot(x, wref[sel, :], preferred_element_type=F32)
                val = val.reshape(out.shape)
                out[:] = val if ref is p_ref else out[:] + val

        def first(lop, loq, lfp, lfq, wb, ob, ab, qb, wsem, lsem, osem, asem):
            def wcp(j):
                return batch(wsem.at[j % RING], (wsrc(j), wb.at[j % RING]))

            lds = batch(lsem, (XP.at[hp, :, :, other], lop), (XQ.at[:, :, other], loq), (XP.at[hp, :, c_lo, mine], lfp), (XQ.at[:, c_lo, mine], lfq))
            start(wcp(0) + lds)
            wait(lds)

            def step(j, _):
                o1 = batch(osem, (ob, PX.at[:, :, :, blk(j, BN)]))

                @when(j < RING)
                def _():
                    wait(wcp(j))

                    @when(j < RING - 1)
                    def _():
                        start(wcp(j + 1))
                    wdot(ob, lop, loq, wb.at[j % RING])
                    start(o1)

                @when(j >= LAG)
                def _():
                    k = j - LAG
                    arrived(RX.at[:, :, :, blk(k, BN)], rid(s + "p") + k)
                    add = batch(asem, (RX.at[:, c_lo, :, blk(k, BN)], ab))
                    start(add)
                    wdot(qb, lfp, lfq, wb.at[k % RING])
                    wait(add)
                    qb[:] += ab[:]
                    start(batch(lsem, (qb, Q1.at[:, :, blk(k, BN)])))

                @when(j < RING)
                def _():
                    wait(o1)
                    ex.start(j)

                @when(j >= LAG)
                def _():
                    k = j - LAG
                    wait(batch(lsem, (qb, Q1.at[:, :, blk(k, BN)])))
                    far_r.start(k)
                    far_l.start(k)
                return 0

            lax.fori_loop(0, RING + LAG, step, 0)

        def second(lp, lq, wb, ab, fb, ob, lsem, isem, osem):
            lds = batch(lsem, (XP.at[hp, :, flip(c_lo), mine], lp), (XQ.at[:, flip(c_lo), mine], lq))
            start(lds)

            def need(k):
                arrived(RF.at[high(R), :, blk(k, BN)], rid(s + "r") + k)
                arrived(RF.at[high(L), :, blk(k, BN)], rid(s + "l") + k)

            for k in range(RING):
                need(k)
            wait(lds)

            def ins(k, sl):
                return (wsrc(k), wb.at[sl]), (RX.at[:, flip(c_lo), :, blk(k, BN)], ab.at[sl]), (RF.at[:, :, blk(k, BN)], fb.at[sl])

            def work(k, sl):
                wdot(ob.at[sl], lp, lq, wb.at[sl])
                ob[sl] += ab[sl]
                for col, part in ((R, 0), (L, 1)):
                    ob[sl, high(col), part * HT:(part + 1) * HT, :] += fb[sl, high(col)]

            def done(k, sl):
                pm_r.start(k)
                pm_l.start(k)

            run(RING, ins, lambda k, sl: ((ob.at[sl], Q2.at[:, :, blk(k, BN)]),), isem, osem, work, done=done)

        def run_first():
            pl.run_scoped(first, bf(TWO, TWO, TH, F2), bf(TWO, TWO, TH, F2), bf(TWO, TH, F2), bf(TWO, TH, F2), bf(RING, *wshape),
                          fl(TWO, TWO, TH, BN), fl(TWO, TH, BN), fl(TWO, TH, BN), dma(RING, RING), dma(MANY), dma(MANY), dma(MANY))

        def run_second():
            pl.run_scoped(second, bf(TWO, TH, F2), bf(TWO, TH, F2), bf(TWO, *wshape), fl(TWO, TWO, TH, BN), fl(TWO, TWO, HT, BN),
                          fl(TWO, TWO, TH, BN), dma(MANY), dma(TWO, MANY), dma(TWO, MANY))

        def come(j):
            arrived(RR.at[0, :, blk(j, BN)], rid(s + "pr") + j)
            arrived(RR.at[1, :, blk(j, BN)], rid(s + "pl") + j)
        return run_first, run_second, come

    y1, y2, y_come = region("Y", False, o["HP"], o["HQ"], o["PY"], o["RY"])
    d1, d2, d_come = region("D", True, o["CP"], o["CQ"], o["PD"], o["RD"])
    d1()
    y1()
    d2()
    grad2(hn, lambda k: S2.at[:, blk(k, BN)], lambda k, ob, sem: s2.start(k))
    y2()

    def piece(ii):
        return slice(ii * FB, (ii + 1) * FB)

    k1u = [Send(lambda m, ii=ii: (K1.at[m, :, piece(ii)], OUT1.at[:, f_block(TWO * g + ii, d)], rid("k1u") + d * TWO + ii, dev(u, m)), TWO)
           for ii in BOTH]
    k1d = [Send(lambda m, ii=ii: (K1.at[TWO + e, :, piece(ii)], OUT1.at[:, f_block(TWO * g + ii, d)], rid("k1d") + ii, dev_e)) for ii in BOTH]

    def done1(k, ob, sem):
        @when(k < TWO)
        def _():
            for t in k1u:
                t.start(k)

        @when(k == TWO + e)
        def _():
            for t in k1d:
                t.start()

        @when(k == TWO + d)
        def _():
            move(batch(sem, *[(ob.at[:, piece(ii)], OUT1.at[:, f_block(TWO * g + ii, d)]) for ii in BOTH]))

    def out2_at(core, jj):
        return OUT2.at[blk(core, FB), blk(jj, BN)]

    k2 = Send(lambda jj: (K2.at[TWO * e + jj], out2_at(d, jj), rid("k2") + jj, dev_e), TWO)

    def done2(k, ob, sem):
        @when(high(k) == d)
        def _():
            move(batch(sem, (ob, out2_at(d, low(k)))))

        @when(high(k) == e)
        def _():
            k2.start(low(k))

    grad1(hi, flip(hp), lambda k: K1.at[k], done1, lambda k: (R1.at[k], rid("s1") + k))

    RX_, OUTX, XO, OUTY, YO, BG, SO = [o[t] for t in ("DRX", "OUTX", "XO", "OUTY", "YO", "BG", "SO")]
    xo = Send(lambda j: (XO, OUTX.at[blk(d, TH), :], rid("xo"), dev_e))
    stages = [dev_e, dev(u, d), dev(v, d), {"col": c + 1 - TWO * c_lo}, {"col": RING - 1 - c}]
    assert len(stages) == STAGES
    sum_send = [Send(lambda j, k=k, dv=dv: (sums.at[k], sums_in.at[k], rid("sum") + k, dv))
                for k, dv in enumerate(stages)]
    bsend = [Send(lambda j, k=k, dv=dv: (db.at[k], db_in.at[k], rid("bf") + k, dv)) for k, dv in enumerate((dev(u, d), dev(v, d)))]
    bg = Send(lambda j: (BG.at[d], BG.at[d], rid("bg"), dev_e))

    def finish_dx(q1b, rlb, rrb, xb, gb, vb, xob, acc, dbb, isem, osem, wsem):
        RB = min(8 * RING, high(TH))
        par_ = batch(wsem, (PV, vb), (o["DB"], dbb))
        start(par_)
        for j in range(RING):
            d_come(j)
        acc[:] = jnp.zeros_like(acc)

        def ins(k, s):
            rows = blk(k, RB)
            return ((o["DQ1"].at[c_hi, rows], q1b.at[s]), (RX_.at[0, rows], rlb.at[s]), (RX_.at[1, rows], rrb.at[s]), (XF.at[rows, :], xb.at[s]),
                    (G.at[hp, c, pl.ds(pl.multiple_of(d * TH + k * RB, RB), RB), :], gb.at[s]))

        def outs(k, s):
            return ((xob.at[s, :, blk(d, DH)], OUTX.at[pl.ds(pl.multiple_of(d * TH + k * RB, RB), RB), :]),
                    (xob.at[s, :, blk(e, DH)], XO.at[blk(k, RB), :]))

        def fold(x):
            return jnp.sum(x.reshape(RB // 8, 8, DM), axis=0)

        def work(k, s):
            @when(k == 0)
            def _():
                wait(par_)
            da = q1b[s] + rlb[s] + rrb[s]
            inv_std, xhat = stats(xb[s].astype(F32))
            gr = gb[s].astype(F32)
            val = da * vb[0]
            m1 = jnp.sum(val, axis=1, keepdims=True) / DM
            m2 = jnp.sum(val * xhat, axis=1, keepdims=True) / DM
            xob[s] = (gr + inv_std * (val - m1 - xhat * m2)).astype(BF16)
            for i, t in enumerate((da * xhat, da, gr)):
                acc[i] += fold(t)

        run(TH // RB, ins, outs, isem, osem, work)
        xo.start()
        for i in range(RING - 1):
            row = jnp.sum(acc[i], axis=0, keepdims=True)
            acc[i, 0:1, :] = row
        for i in range(RING - 1):
            sums[STAGES, i:i + 1, :] = acc[i, 0:1, blk(d, DH)]
            sums[0, i:i + 1, :] = acc[i, 0:1, blk(e, DH)]
        db[0, 0:1, :] = jnp.sum(dbb[:], axis=0, keepdims=True)
        sum_send[0].start()

    def stage(k):
        arrived(sums_in.at[k], rid("sum") + k)
        sums[STAGES] += sums_in[k]
        if k in (1, TWO):
            arrived(db_in.at[k - 1], rid("bf") + k - 1)
            db[k] = db[k - 1] + db_in[k - 1]
        if k < STAGES - 1:
            sums[k + 1] = sums[STAGES]
            sum_send[k + 1].start()
        if k < TWO:
            bsend[k].start()

    def sums_out(wsem):
        stage(STAGES - 1)
        move(batch(wsem, (sums.at[STAGES], SO), *[(db.at[TWO, :, blk(pos, FB)], BG.at[d, row]) for pos, row in enumerate((0, RING - 1, 1, TWO))]))
        bg.start()

    def dx_all():
        RB = min(8 * RING, high(TH))
        pl.run_scoped(finish_dx, fl(TWO, RB, DM), fl(TWO, RB, DM), fl(TWO, RB, DM), bf(TWO, RB, DM), bf(TWO, RB, DM), fl(RING - 1, 1, DM),
                      bf(TWO, RB, DM), fl(RING - 1, 8, DM), fl(8, FC), dma(TWO, MANY + RING), dma(TWO, MANY), dma(MANY))

    dx_all()

    def outy_at(core, jj):
        return OUTY.at[blk(core, TH), blk(jj, BN)]

    yo = Send(lambda jj: (YO.at[TWO * e + jj], outy_at(d, jj), rid("yo") + jj, dev_e), TWO)

    def last_part(q1b, xb, vb, rxb, yb, sem, sem2):
        def fetch_y(k):
            cols = blk(k, BN)
            start(batch(sem, (o["YQ1"].at[c_hi, :, cols], q1b), (XF.at[:, cols], xb), (PV.at[TWO, :, cols], vb)))
            y_come(k)
            start(batch(sem2, (o["YRX"].at[:, :, cols], rxb)))

        def finish_y(k):
            cols = blk(k, BN)
            here = batch(sem, (o["YQ1"].at[c_hi, :, cols], q1b), (XF.at[:, cols], xb), (PV.at[TWO, :, cols], vb))
            wait(here)
            wait(batch(sem2, (o["YRX"].at[:, :, cols], rxb)))
            yb[:] = (xb[:].astype(F32) + (q1b[:] + rxb[0] + rxb[1]) + vb[:]).astype(BF16)

            @when(d == high(k))
            def _():
                move(batch(sem, (yb, outy_at(high(k), low(k)))))

            @when(e == high(k))
            def _():
                move(batch(sem, (yb, YO.at[k])))
                yo.start(low(k))

        def third():
            stage(TWO)
            for k in range(RING - 1):
                fetch_y(k)
                finish_y(k)
                if k == 0:
                    stage(RING - 1)

        def before():
            sums_out(sem)
            fetch_y(RING - 1)

        mid = (before, lambda: finish_y(RING - 1))

        posts = {k: functools.partial(stage, k) for k in BOTH}
        posts[TWO] = third
        grad2(hi, lambda k: K2.at[k], done2, lambda k: (R2.at[:, blk(k, BN)], rid("s2") + k), posts, mid)

    pl.run_scoped(last_part, fl(TH, BN), bf(TH, BN), fl(1, BN), fl(TWO, TH, BN), bf(TH, BN), dma(MANY), dma(MANY))

    arrived(OUTX.at[blk(e, TH), :], rid("xo"))
    arrived(BG.at[e], rid("bg"))
    for ii in BOTH:
        arrived(outy_at(e, ii), rid("yo") + ii)
        for dd in BOTH:
            arrived(OUT1.at[:, f_block(TWO * gn + ii, dd)], rid("k1u") + dd * TWO + ii)
        arrived(OUT1.at[:, f_block(TWO * g + ii, e)], rid("k1d") + ii)
        arrived(out2_at(e, ii), rid("k2") + ii)
    for t in pending:
        for j in range(t.n):
            t.desc(j).wait_send()
    assert tuple(counts) == SEMS, counts


SEMS = (171, 149)


def solution(mesh):
    nr, nc, nd = mesh.shape["row"], mesh.shape["col"], mesh.shape["dep"]
    assert nr == 4 and nc == 4 and nd == 2
    tok_spec = P(("part", "row", "col"), "dep")
    vec_dep = P("dep")
    part_dep = P(("part", "dep"))
    in_specs = (tok_spec, vec_dep, vec_dep, P(("dep", "row"), "col"), P("col"), P(("col", "row"), "dep"), vec_dep, tok_spec)
    out_specs = (tok_spec, tok_spec, P(("part", "dep", "row"), "col"), P(("part", "col")), P(("part", "col", "row"), "dep"), part_dep, part_dep, part_dep)

    def local_step(x_in, ln_scale, ln_shift, w_up, b_up, w_down, b_down, y_grad):
        th, dhalf = x_in.shape[0] // 2, x_in.shape[1]
        ds_, fb = w_up.shape[0], w_up.shape[1] // 8
        rows = [t.astype(F32).reshape(1, -1) for t in (ln_scale, ln_shift, b_down, b_up)]

        cfg = (th, 2 * dhalf, ds_, fb)
        outs = pl.pallas_call(
            functools.partial(kernel, cfg),
            name="mlp_layer",
            out_shape=buffers(*cfg),
            in_specs=[pl.BlockSpec(memory_space=pl.ANY)] * 7 + [pl.BlockSpec(memory_space=pltpu.VMEM)],
            out_specs=[pl.BlockSpec(memory_space=pl.ANY)] * len(NAMES),
            scratch_shapes=[dma(SEMS[1]), dma(SEMS[0]), fl(STAGES + 1, 8, dhalf), fl(STAGES, 8, dhalf), fl(3, 8, 4 * fb), fl(2, 8, 4 * fb)],
            compiler_params=pltpu.CompilerParams(collective_id=0, has_side_effects=True, vmem_limit_bytes=62 * 1024 * 1024),
        )(x_in, y_grad, w_up, w_down, *rows)
        o = dict(zip(NAMES, outs))
        b_up_grad = o["BG"][:, :, 0].transpose(1, 0, 2).reshape(8 * fb)
        return (o["OUTY"], o["OUTX"], o["OUT1"], b_up_grad, o["OUT2"], o["SO"][2], o["SO"][0], o["SO"][1])

    return jax.shard_map(local_step, mesh=mesh, in_specs=in_specs, out_specs=out_specs, check_vma=False)
```
